256 devices in a mesh: sample: 16 (over y, x), sy: 4 (over z_lo, core), sz: 4 (over z_hi).
Axes of the slice: x: 4, y: 4, z: 8 (z_hi: 4, z_lo: 2; z = z_hi * 2 + z_lo), core: 2. Of those that a mesh axis runs over, the one named last changes fastest.
Arguments:
- volume: bfloat16 [16, 32, 16, 32, 128], P('sample', None, 'sz', 'sy'), may hold values from -22.5 to 22.5
- amax_history: float32 [4, 16], replicated, may hold values from 0.48 to 2.5
- conv_first: bfloat16 [27, 32, 32], replicated, may hold values from -0.21875 to 0.21875
- conv_second: bfloat16 [27, 32, 32], replicated, may hold values from -0.21875 to 0.21875
- conv_third: bfloat16 [27, 64, 32], P(None, 'sy'), may hold values from -0.21875 to 0.21875
- conv_fourth: bfloat16 [27, 64, 64], P(None, 'sy'), may hold values from -0.15625 to 0.15625
- gain_fine: float32 [2, 32], replicated, may hold values from 0.5 to 1.5
- shift_fine: float32 [2, 32], replicated, may hold values from -0.5 to 0.5
- gain_coarse: float32 [2, 64], P(None, 'sy'), may hold values from 0.5 to 1.5
- shift_coarse: float32 [2, 64], P(None, 'sy'), may hold values from -0.5 to 0.5
Outputs:
- skip_features: bfloat16 [16, 32, 16, 32, 128], P('sample', None, 'sz', 'sy')
- coarse_features: bfloat16 [16, 64, 8, 1024], P('sample', 'sy', 'sz')
- amax_now: float32 [4], replicated
The draws below stay inside these ranges and needn't reach their ends.
All inputs are finite; a program needn't handle non-finite values.
Results may differ from the reference program's by a relative error of at most 0.012.
Values may be sent and summed in bfloat16 or wider, within the bound.
A program may use at most 128 MiB of HBM per device.

```python
import jax
import jax.numpy as jnp
from jax import lax

C1 = 32
C2 = 64
NX = 128
HIST = 16
LAYERS = 4
SAMPLES = 16
NY = 32
NZ = 16


def draw_volume(key, part):
    shape_all = (SAMPLES, C1, NZ, NY, NX)
    sample_pos = lax.broadcasted_iota(jnp.float32, shape_all, 0) / max(SAMPLES - 1, 1)
    z_pos = lax.broadcasted_iota(jnp.float32, shape_all, 2) / NZ
    y_pos = lax.broadcasted_iota(jnp.float32, shape_all, 3) / NY
    scaling = (0.6 + 1.2 * sample_pos) * (0.5 + z_pos + y_pos)
    noise_part = jnp.clip(jax.random.normal(key, shape_all, jnp.float32), -5.0, 5.0)
    return (noise_part * scaling).astype(jnp.bfloat16)


def draw_amax_history(key, part):
    level_key = jax.random.fold_in(key, 11)
    entry_key = jax.random.fold_in(key, 12)
    level_log = jax.random.uniform(level_key, (LAYERS, 1), jnp.float32, jnp.log(0.8), jnp.log(2.5))
    entries = jax.random.uniform(entry_key, (LAYERS, HIST), jnp.float32, 0.6, 1.0)
    return jnp.exp(level_log) * entries


def level_of(stream_key, dims, cuts, least, largest):
    def one(position, shards_of):
        steps = jax.random.uniform(jax.random.fold_in(jax.random.fold_in(stream_key, 6), position), (shards_of,), jnp.float32, least / len(cuts), largest / len(cuts))
        return jnp.repeat(jnp.exp(steps), dims[position] // shards_of).reshape((-1,) + (1,) * (len(dims) - position - 1))

    factor_of = one(*cuts[0])
    for cut in cuts[1:]:
        factor_of = factor_of * one(*cut)
    return factor_of


def gaussian(own_key, shape, scale, most, cuts=(), held_as=jnp.bfloat16):
    values = scale * jax.random.normal(own_key, shape, jnp.float32)
    if cuts:
        values = values * level_of(own_key, shape, cuts, -0.22, 0.18)
    return jnp.clip(values, -most, most).astype(held_as)


def setup_inputs(seed: int = 0) -> dict:
    seeds = jax.random.split(jax.random.key(seed), 11)
    volume = draw_volume(jax.random.fold_in(seeds[10], 71), 0)
    amax_history = draw_amax_history(jax.random.fold_in(seeds[10], 71), 0)
    conv_first = gaussian(seeds[2], (27, C1, C1), (27 * C1) ** -0.5, 0.21875)
    conv_second = gaussian(seeds[3], (27, C1, C1), (27 * C1) ** -0.5, 0.21875)
    conv_third = gaussian(seeds[4], (27, C2, C1), (27 * C1) ** -0.5, 0.21875, ((1, 4),))
    conv_fourth = gaussian(seeds[5], (27, C2, C2), (27 * C2) ** -0.5, 0.15625, ((1, 4),))
    gain_fine = jnp.clip(1.0 + 0.1 * jax.random.normal(seeds[6], (2, C1), jnp.float32), 0.5, 1.5)
    shift_fine = jnp.clip(jax.random.uniform(seeds[7], (2, C1), jnp.float32, -0.5, 0.5), -0.5, 0.5)
    gain_coarse = jnp.clip(1.0 + 0.1 * jax.random.normal(seeds[8], (2, C2), jnp.float32), 0.5, 1.5)
    shift_coarse = jnp.clip(jax.random.uniform(seeds[9], (2, C2), jnp.float32, -0.5, 0.5) * level_of(seeds[9], (2, C2), ((1, 4),), -0.4, 0.0), -0.5, 0.5)
    return {"volume": volume, "amax_history": amax_history, "conv_first": conv_first, "conv_second": conv_second, "conv_third": conv_third, "conv_fourth": conv_fourth, "gain_fine": gain_fine, "shift_fine": shift_fine, "gain_coarse": gain_coarse, "shift_coarse": shift_coarse}


norm_eps = 1e-05
leak_slope = 0.01

def convolve(values, weight):
    out_chan = weight.shape[1]
    in_chan = weight.shape[2]
    kernel = jnp.transpose(weight.reshape(3, 3, 3, out_chan, in_chan), (3, 4, 0, 1, 2))
    result = lax.conv_general_dilated(values.astype(jnp.float32)[None], kernel.astype(jnp.float32), (1, 1, 1), 'SAME', dimension_numbers=('NCDHW', 'OIDHW', 'NCDHW'), precision=lax.Precision.HIGHEST)
    return result[0]

def activate(values, gains, offset):
    cell_count = values[0].size
    flat_rows = values.reshape(values.shape[0], -1)
    chan_mean = lax.optimization_barrier(jnp.sum(flat_rows, axis=1)) / cell_count
    spread = lax.optimization_barrier(jnp.sum(flat_rows * flat_rows, axis=1)) / cell_count - chan_mean * chan_mean
    scaling = lax.rsqrt(spread + norm_eps) * gains
    normed = (values - chan_mean[:, None, None, None]) * scaling[:, None, None, None] + offset[:, None, None, None]
    return jnp.where(normed >= 0, normed, leak_slope * normed).astype(jnp.bfloat16)

def limited(values, bound):
    return jnp.clip(values.astype(jnp.float32), -bound, bound).astype(jnp.bfloat16)

def pool_max(values):
    chans, depth_cells, height_cells, width_cells = values.shape
    blocks = values.reshape(chans, depth_cells // 2, 2, height_cells // 2, 2, width_cells // 2, 2)
    return lax.optimization_barrier(jnp.max(blocks, axis=(2, 4, 6)))

def reference(volume, amax_history, conv_first, conv_second, conv_third, conv_fourth, gain_fine, shift_fine, gain_coarse, shift_coarse):
    bounds = lax.optimization_barrier(jnp.max(amax_history, axis=1))

    def single(volume_one):
        first = activate(convolve(limited(volume_one, bounds[0]), conv_first), gain_fine[0], shift_fine[0])
        skip_out = activate(convolve(limited(first, bounds[1]), conv_second), gain_fine[1], shift_fine[1])
        pooled = pool_max(skip_out)
        coarse = activate(convolve(limited(pooled, bounds[2]), conv_third), gain_coarse[0], shift_coarse[0])
        coarse_out = activate(convolve(limited(coarse, bounds[3]), conv_fourth), gain_coarse[1], shift_coarse[1])
        peak_list = jnp.stack([jnp.max(jnp.abs(member.astype(jnp.float32))) for member in (volume_one, first, pooled, coarse)])
        return (skip_out, coarse_out.reshape(coarse_out.shape[0], coarse_out.shape[1], -1), peak_list)
    skip_all, coarse_all, peak_all = lax.map(single, volume)
    return (skip_all, coarse_all, lax.optimization_barrier(jnp.max(peak_all, axis=0)))
```

```python
import functools

import jax
import jax.numpy as jnp
from jax import lax
from jax.experimental import pallas as pl
from jax.experimental.pallas import tpu as pltpu
from jax.sharding import PartitionSpec as P

MESH = pl.DeviceIdType.MESH
F32 = jnp.float32
BF16 = jnp.bfloat16
EPS = 1e-05
SLOPE = 0.01
DIRS = ((-1, 0), (1, 0), (-1, -1), (-1, 1), (1, -1), (1, 1), (0, -1), (0, 1))


def body(
    ny, nz, gx, gy,
    vol, hist, w1, w2, w3, w4, gf, sf, gc, sc,
    skip, coarse, amax,
    vin, w1v, w2v, w3v, w4v, wf1, wf2, wg3, wg4,
    x1, r1, x2r, x2, r2, h3, p3, c3, h4, r4i, c4, a2a, a2s, gcol,
    st, am, outv, rows8,
    lsem, osem, hs, hr, ss, sr, ws, wr, gs, gr, bs, br, xs, xr,
):
    n = ny * nz
    sy = lax.axis_index("sy")
    sz = lax.axis_index("sz")
    smp = lax.axis_index("sample")
    me = sz * ny + sy
    mx_, my_ = lax.rem(smp, gx), lax.div(smp, gx)

    loads = [pltpu.make_async_copy(vol.at[:, z], vin.at[z], lsem.at[z]) for z in range(4)]
    for i, (s, d) in enumerate(((w1, w1v), (w2, w2v), (w3, w3v), (w4, w4v))):
        loads.append(pltpu.make_async_copy(s, d, lsem.at[4 + i]))
    for c in loads:
        c.start()

    def partner(d):
        p = lax.rem(me + d, n)
        return p, {"sy": lax.rem(p, ny), "sz": lax.div(p, ny)}

    order = sorted(range(1, n), key=lambda d: -min(d, n - d))
    barrier = pltpu.get_barrier_semaphore()
    for d in order:
        pl.semaphore_signal(barrier, inc=1, device_id=partner(d)[1], device_id_type=MESH)

    def xpeer(d):
        q = lax.rem(mx_ + d, gx)
        return q, {"sample": my_ * gx + q}

    def ypeer(d):
        q = lax.rem(my_ + d, gy)
        return q, {"sample": q * gx + mx_}

    for d in range(1, gx):
        pl.semaphore_signal(barrier, inc=1, device_id=xpeer(d)[1], device_id_type=MESH)
    for d in range(1, gy):
        pl.semaphore_signal(barrier, inc=1, device_id=ypeer(d)[1], device_id_type=MESH)

    def exists(dz, dy):
        cond = None
        for idx, cnt, d in ((sz, nz, dz), (sy, ny, dy)):
            if d == 0:
                continue
            c = (idx > 0) if d < 0 else (idx < cnt - 1)
            cond = c if cond is None else jnp.logical_and(cond, c)
        return cond

    lane = lax.broadcasted_iota(jnp.int32, (1, 128), 1)

    def bound_of(l):
        b = jnp.max(hist[l : l + 1, :], axis=1, keepdims=True)
        return b.astype(BF16).astype(F32)

    def src_z(dz, zl):
        return pl.ds(1, zl) if dz == 0 else (pl.ds(1, 1) if dz < 0 else pl.ds(zl, 1))

    def dst_z(dz, zl):
        return pl.ds(1, zl) if dz == 0 else (pl.ds(zl + 1, 1) if dz < 0 else pl.ds(0, 1))

    def halo(ph, buf, zl, yl, i):
        dz, dy = DIRS[i]
        return pltpu.make_async_remote_copy(
            src_ref=buf.at[src_z(dz, zl), src_z(dy, yl)],
            dst_ref=buf.at[dst_z(dz, zl), dst_z(dy, yl)],
            send_sem=hs.at[ph, i],
            recv_sem=hr.at[ph, i],
            device_id={"sy": sy + dy, "sz": sz + dz},
            device_id_type=MESH,
        )

    def halo_send(ph, buf, zl, yl, which):
        for i in which:
            @pl.when(exists(*DIRS[i]))
            def _():
                halo(ph, buf, zl, yl, i).start()

    def halo_wait(ph, buf, zl, yl, which):
        for i in which:
            @pl.when(exists(-DIRS[i][0], -DIRS[i][1]))
            def _():
                halo(ph, buf, zl, yl, i).wait_recv()

    def halo_done(ph, buf, zl, yl):
        for i in range(8):
            @pl.when(exists(*DIRS[i]))
            def _():
                halo(ph, buf, zl, yl, i).wait_send()

    def slots(d, length):
        return range(1, length + 1) if d == 0 else ((0,) if d > 0 else (length + 1,))

    def stat_copy(ph, d, src):
        p, dev = partner(d)
        return pltpu.make_async_remote_copy(
            src_ref=st.at[ph, me],
            dst_ref=st.at[ph, src],
            send_sem=ss.at[ph, d],
            recv_sem=sr.at[ph, src],
            device_id=dev,
            device_id_type=MESH,
        )

    def stat_send(ph, rows):
        st[ph, me] = rows
        for d in order:
            stat_copy(ph, d, me).start()

    def stat_wait(ph):
        for d in order:
            stat_copy(ph, d, partner(d)[0]).wait_recv()
        return st[ph]

    def to_rows(cols):
        return jnp.transpose(cols)

    def to_cols(row):
        return jnp.transpose(jnp.broadcast_to(row, (128, 128)))

    def affine(tot, totsq, cells, g, s):
        m = tot / cells
        var = totsq / cells - m * m
        a = lax.rsqrt(var + EPS) * g
        return a, m, s

    def act(v, aff):
        a, m, s = aff
        t = (v - m) * a + s
        return jnp.maximum(t, SLOPE * t)

    rows8[...] = jnp.zeros_like(rows8)
    rows8[0:2, 0:32] = gf[...]
    rows8[2:4, 0:32] = sf[...]
    rows8[4:6, 0:16] = gc[...]
    rows8[6:8, 0:16] = sc[...]
    gcols = jnp.transpose(rows8[...])

    def gain_col(j, count):
        return jnp.broadcast_to(gcols[0:count, j : j + 1], (count, 128))

    ri = lax.broadcasted_iota(jnp.int32, (256, 256), 0)
    ci = lax.broadcasted_iota(jnp.int32, (256, 256), 1)

    def onehot(cond):
        return jnp.where(cond, 1.0, 0.0).astype(BF16)

    into = onehot(jnp.logical_and((ri & 31) == (ci >> 3), (ri >> 5) == (ci & 7)))

    b0 = bound_of(0)
    for i in range(4):
        loads[i].wait()
    peak0 = jnp.zeros((256, 128), F32)
    for zp in range(2):
        parts = []
        for z in (2 * zp, 2 * zp + 1):
            v = vin[z].astype(F32).reshape(256, 128)
            peak0 = jnp.maximum(peak0, jnp.abs(v))
            parts.append(v.astype(BF16))
        moved = jnp.dot(into, jnp.concatenate(parts, axis=1), preferred_element_type=F32)
        moved = jnp.clip(moved, -b0, b0).astype(BF16)
        for k in range(2):
            for y in range(8):
                x1[1 + 2 * zp + k, 1 + y] = moved[32 * y : 32 * y + 32, 128 * k : 128 * k + 128]
    peak0 = jnp.max(jnp.max(peak0, axis=0, keepdims=True), axis=1, keepdims=True)

    pl.semaphore_wait(barrier, (n - 1) + (gx - 1) + (gy - 1))
    halo_send(0, x1, 4, 8, range(8))

    for i in range(4, 8):
        loads[i].wait()

    def lanes_of(w):
        return jnp.concatenate([w[k] for k in range(9)], axis=1)

    wf1[...] = lanes_of(w1v)
    wf2[...] = lanes_of(w2v)
    wg3[sy] = lanes_of(w3v)
    wg4[sy] = lanes_of(w4v)
    gcol[sy, 0] = gain_col(4, 16)
    gcol[sy, 1] = gain_col(6, 16)

    def zero_missing(buf, zl, yl):
        for i in range(8):
            dz, dy = DIRS[i]
            @pl.when(jnp.logical_not(exists(-dz, -dy)))
            def _():
                for z in slots(dz, zl):
                    for y in slots(dy, yl):
                        buf[z, y] = jnp.zeros(buf.shape[2:], buf.dtype)

    zero_missing(x1, 4, 8)

    first, last = lane == 0, lane == 127

    def combine(p0, p1, p2, lo, hi):
        left = jnp.where(lo, 0.0, pltpu.roll(p0, 1, 1))
        right = jnp.where(hi, 0.0, pltpu.roll(p2, 127, 1))
        return p1 + left + right

    def fine_conv(buf, w, z):
        strips = []
        for zt in range(3):
            blocks = [buf[z + zt, y] for y in range(10)]
            for yt in range(3):
                strips.append(jnp.concatenate(blocks[yt : yt + 8], axis=1))
        got = jnp.dot(w, jnp.concatenate(strips, axis=0), preferred_element_type=F32)
        outs = []
        for y in range(8):
            blk = got[:, 128 * y : 128 * y + 128]
            outs.append(combine(blk[0:32], blk[32:64], blk[64:96], first, last))
        return outs

    zero = jnp.zeros((32, 128), F32)

    def gather_stats(acc, blocks, extremes):
        s, q, hi, lo = acc
        for b in blocks:
            s = s + b
            q = q + b * b
            if extremes:
                hi = jnp.maximum(hi, b)
                lo = jnp.minimum(lo, b)
        return s, q, hi, lo

    def mixed_row(cols):
        t = to_rows(cols)
        total = jnp.sum(t, axis=0, keepdims=True)
        high = jnp.max(t, axis=0, keepdims=True)
        low = jnp.min(t, axis=0, keepdims=True)
        return jnp.where(lane < 64, total, jnp.where(lane < 96, high, low))

    def mixed_total(got):
        total = jnp.sum(got[:, 0:1, :], axis=0)
        high = jnp.max(got[:, 0:1, :], axis=0)
        low = jnp.min(got[:, 0:1, :], axis=0)
        return to_cols(jnp.where(lane < 64, total, jnp.where(lane < 96, high, low)))

    wa = wf1[...]
    acc = (zero, zero, jnp.full((32, 128), -jnp.inf, F32), jnp.full((32, 128), jnp.inf, F32))
    halo_wait(0, x1, 4, 8, (6, 7))
    for z in (1, 2):
        outs = fine_conv(x1, wa, z)
        acc = gather_stats(acc, outs, True)
        for y in range(8):
            r1[z, y] = outs[y]
        x2r[z + 1, 1] = outs[0].astype(BF16)
        x2r[z + 1, 8] = outs[7].astype(BF16)
    halo_wait(0, x1, 4, 8, range(6))
    for z in (0, 3):
        outs = fine_conv(x1, wa, z)
        acc = gather_stats(acc, outs, True)
        for y in range(8):
            r1[z, y] = outs[y]
            x2r[z + 1, y + 1] = outs[y].astype(BF16)
        halo_send(1, x2r, 4, 8, (0, 2, 3) if z == 0 else (1, 4, 5))
    halo_send(1, x2r, 4, 8, (6, 7))
    row = mixed_row(jnp.concatenate(acc, axis=0))
    stat_send(0, jnp.concatenate([row, jnp.broadcast_to(peak0, (1, 128))], axis=0))

    fine_cells = float(4 * nz * 8 * ny * 128)
    coarse_cells = fine_cells / 8

    def fine_affine(cols, j):
        return affine(cols[0:32], cols[32:64], fine_cells, gain_col(j, 32), gain_col(2 + j, 32))

    def peak_of(high, low, aff):
        v = jnp.maximum(jnp.abs(act(high, aff)), jnp.abs(act(low, aff))).astype(BF16).astype(F32)
        return jnp.max(jnp.max(v, axis=0, keepdims=True), axis=1, keepdims=True)

    got = stat_wait(0)
    peak0 = jnp.max(jnp.max(got[:, 1:2, :], axis=0), axis=1, keepdims=True)
    cols = mixed_total(got)
    aff = fine_affine(cols, 0)
    peak1 = peak_of(cols[64:96], cols[96:128], aff)
    b1 = bound_of(1)

    def settle(v, aff, b):
        return jnp.clip(act(v, aff), -b, b).astype(BF16)

    for z in range(4):
        for y in range(8):
            x2[z + 1, y + 1] = settle(r1[z, y], aff, b1)

    def settle_halo(ph, raw, buf, zl, yl, which, aff, b):
        for i in which:
            dz, dy = DIRS[i]
            there = exists(-dz, -dy)

            @pl.when(there)
            def _():
                halo(ph, raw, zl, yl, i).wait_recv()
                for z in slots(dz, zl):
                    for y in slots(dy, yl):
                        buf[z, y] = settle(raw[z, y].astype(F32), aff, b)

            @pl.when(jnp.logical_not(there))
            def _():
                for z in slots(dz, zl):
                    for y in slots(dy, yl):
                        buf[z, y] = jnp.zeros(buf.shape[2:], buf.dtype)

    wb = wf2[...]
    acc = (zero, zero, None, None)
    settle_halo(1, x2r, x2, 4, 8, (6, 7), aff, b1)
    for z in (1, 2):
        outs = fine_conv(x2, wb, z)
        acc = gather_stats(acc, outs, False)
        for y in range(8):
            r2[z, y] = outs[y]
    settle_halo(1, x2r, x2, 4, 8, range(6), aff, b1)

    def group(d, src, which):
        q = lax.rem(sy + d, ny)
        buf = (wg3, wg4, gcol)[which]
        return pltpu.make_async_remote_copy(
            src_ref=buf.at[sy], dst_ref=buf.at[src],
            send_sem=ws.at[which, d], recv_sem=wr.at[which, src],
            device_id={"sy": q}, device_id_type=MESH,
        )

    for which in range(3):
        for d in range(1, ny):
            group(d, sy, which).start()

    for z in (0, 3):
        outs = fine_conv(x2, wb, z)
        acc = gather_stats(acc, outs, False)
        for y in range(8):
            r2[z, y] = outs[y]

    s_r = lax.broadcasted_iota(jnp.int32, (256, 128), 0)
    s_c = lax.broadcasted_iota(jnp.int32, (256, 128), 1)
    pick = onehot(s_r == jnp.where(s_c < 64, 2 * s_c, 2 * s_c))
    highs, lows = [], []
    for zp in range(2):
        hrow, lrow = [], []
        for yp in range(4):
            m = jnp.maximum(
                jnp.maximum(r2[2 * zp, 2 * yp], r2[2 * zp, 2 * yp + 1]),
                jnp.maximum(r2[2 * zp + 1, 2 * yp], r2[2 * zp + 1, 2 * yp + 1]),
            )
            m = jnp.maximum(m, pltpu.roll(m, 127, 1))
            h = m.astype(BF16)
            hrow.append(h)
            lrow.append((m - h.astype(F32)).astype(BF16))
        highs.append(jnp.concatenate(hrow, axis=0))
        lows.append(jnp.concatenate(lrow, axis=0))
    pooled = jnp.dot(jnp.concatenate(highs, axis=1), pick, preferred_element_type=F32)
    pooled = pooled + jnp.dot(jnp.concatenate(lows, axis=1), pick, preferred_element_type=F32)
    hi = jnp.full((32, 128), -jnp.inf, F32)
    lo = jnp.full((32, 128), jnp.inf, F32)
    for yp in range(4):
        blk = pooled[32 * yp : 32 * yp + 32]
        p3[yp] = blk
        h3[1, yp + 1] = blk.astype(BF16)
        hi = jnp.maximum(hi, blk)
        lo = jnp.minimum(lo, blk)
    halo_send(2, h3, 1, 4, range(8))
    row = mixed_row(jnp.concatenate([acc[0], acc[1], hi, lo], axis=0))
    stat_send(1, jnp.concatenate([row, row], axis=0))

    got = stat_wait(1)
    cols = mixed_total(got)
    aff2 = fine_affine(cols, 1)
    peak2 = peak_of(cols[64:96], cols[96:128], aff2)
    b2 = bound_of(2)
    for yp in range(4):
        c3[1, yp + 1] = settle(p3[yp], aff2, b2)
    settle_halo(2, h3, c3, 1, 4, range(8), aff2, b2)

    lower = lane < 64
    cfirst, clast = (lane & 63) == 0, (lane & 63) == 63

    def coarse_conv(buf, w):
        strips = []
        mids = [buf[1, y] for y in range(6)]
        pairs = [[], mids, []]
        for y in range(6):
            own = mids[y].astype(F32)
            prev = buf[0, y].astype(F32)
            nxt = buf[2, y].astype(F32)
            pairs[0].append(pltpu.roll(jnp.where(lower, own, prev), 64, 1).astype(BF16))
            pairs[2].append(pltpu.roll(jnp.where(lower, nxt, own), 64, 1).astype(BF16))
        for zt in range(3):
            for yt in range(3):
                strips.append(jnp.concatenate(pairs[zt][yt : yt + 4], axis=1))
        got = jnp.dot(w, jnp.concatenate(strips, axis=0), preferred_element_type=F32)
        outs = []
        for y in range(4):
            blk = got[:, 128 * y : 128 * y + 128]
            parts = []
            for g in range(4):
                t = blk[48 * g : 48 * g + 48]
                parts.append(combine(t[0:16], t[16:32], t[32:48], cfirst, clast))
            outs.append(jnp.concatenate(parts, axis=0))
        return outs

    for d in range(1, ny):
        group(d, lax.rem(sy + d, ny), 0).wait_recv()
    outs = coarse_conv(c3, wg3[...].reshape(192, 288))
    zero64 = jnp.zeros((64, 128), F32)
    acc = (zero64, zero64, jnp.full((64, 128), -jnp.inf, F32), jnp.full((64, 128), jnp.inf, F32))
    acc = gather_stats(acc, outs, True)
    for y in range(4):
        h4[1, y + 1] = outs[y].astype(BF16)
        r4i[y] = outs[y]
    halo_send(3, h4, 1, 4, range(8))

    def double_rows(acc, extremes):
        t = to_rows(jnp.concatenate(acc[0:2], axis=0))
        r0 = jnp.sum(t, axis=0, keepdims=True)
        if not extremes:
            return jnp.concatenate([r0, r0], axis=0)
        t = to_rows(jnp.concatenate(acc[2:4], axis=0))
        high = jnp.max(t, axis=0, keepdims=True)
        low = jnp.min(t, axis=0, keepdims=True)
        return jnp.concatenate([r0, jnp.where(lower, high, low)], axis=0)

    stat_send(2, double_rows(acc, True))

    outof = onehot(jnp.logical_and((ci & 31) == (ri >> 3), (ci >> 5) == (ri & 7)))
    stores = []
    for zp in range(2):
        parts = []
        for z in (2 * zp, 2 * zp + 1):
            parts.append(jnp.concatenate([act(r2[z, y], aff2).astype(BF16) for y in range(8)], axis=0))
        moved = jnp.dot(outof, jnp.concatenate(parts, axis=1), preferred_element_type=F32)
        for k in range(2):
            z = 2 * zp + k
            outv[z] = moved[:, 128 * k : 128 * k + 128].reshape(32, 8, 128).astype(BF16)
            stores.append(pltpu.make_async_copy(outv.at[z], skip.at[:, z], osem.at[z]))
            stores[-1].start()

    for d in range(1, ny):
        group(d, lax.rem(sy + d, ny), 2).wait_recv()
    gall = gcol[...]
    got = stat_wait(2)
    cols = to_cols(jnp.sum(got[:, 0:1, :], axis=0))
    high = jnp.max(got[:, 1:2, :], axis=0)
    low = jnp.min(got[:, 1:2, :], axis=0)
    ext = to_cols(jnp.where(lower, high, low))
    aff3 = affine(cols[0:64], cols[64:128], coarse_cells, gall[:, 0].reshape(64, 128), gall[:, 1].reshape(64, 128))
    peak3 = peak_of(ext[0:64], ext[64:128], aff3)
    b3 = bound_of(3)

    peaks = jnp.where(lane == 0, peak0, jnp.where(lane == 1, peak1, jnp.where(lane == 2, peak2, peak3)))

    def cross(step, d, src):
        mine, peer = (mx_, xpeer) if step == 0 else (my_, ypeer)
        return pltpu.make_async_remote_copy(
            src_ref=am.at[step, mine], dst_ref=am.at[step, src],
            send_sem=xs.at[step, d], recv_sem=xr.at[step, src],
            device_id=peer(d)[1], device_id_type=MESH,
        )

    am[0, mx_] = peaks
    for d in range(1, gx):
        cross(0, d, mx_).start()

    for y in range(4):
        c4[1, y + 1] = settle(r4i[y], aff3, b3)
    settle_halo(3, h4, c4, 1, 4, range(8), aff3, b3)

    for d in range(1, ny):
        group(d, lax.rem(sy + d, ny), 1).wait_recv()
    outs = coarse_conv(c4, wg4[...].reshape(192, 576))
    acc = gather_stats((zero64, zero64, None, None), outs, False)
    for g in range(4):
        for y in range(4):
            a2s[g, y] = outs[y][16 * g : 16 * g + 16]

    def swap(d, src):
        q = lax.rem(sy + d, ny)
        return pltpu.make_async_remote_copy(
            src_ref=a2s.at[q], dst_ref=a2a.at[src],
            send_sem=bs.at[d], recv_sem=br.at[src],
            device_id={"sy": q}, device_id_type=MESH,
        )

    for d in range(1, ny):
        swap(d, sy).start()
    stat_send(3, double_rows(acc, False))
    a2a[sy] = a2s[sy]

    for d in range(1, gx):
        cross(0, d, xpeer(d)[0]).wait_recv()
    am[1, my_] = jnp.max(am[0, 0:gx], axis=0)
    for d in range(1, gy):
        cross(1, d, my_).start()

    for d in range(1, ny):
        swap(d, lax.rem(sy + d, ny)).wait_recv()
    got = stat_wait(3)
    rows8b = to_cols(jnp.sum(got[:, 0:1, :], axis=0))
    gs[...] = rows8b
    tot = gs[pl.ds(pl.multiple_of(sy * 16, 8), 16), :]
    totsq = gs[pl.ds(pl.multiple_of(64 + sy * 16, 8), 16), :]
    aff4 = affine(tot, totsq, coarse_cells, gain_col(5, 16), gain_col(7, 16))
    planes = [[], []]
    for g in range(4):
        for yp in range(2):
            u = act(a2a[g, 2 * yp], aff4)
            v = act(a2a[g, 2 * yp + 1], aff4)
            planes[0].append(jnp.where(lower, u, pltpu.roll(v, 64, 1)))
            planes[1].append(jnp.where(lower, pltpu.roll(u, 64, 1), v))
    for z in range(2):
        coarse[z] = jnp.concatenate(planes[z], axis=1).astype(BF16)

    for d in range(1, gy):
        cross(1, d, ypeer(d)[0]).wait_recv()
    amax[...] = jnp.max(am[1, 0:gy], axis=0)

    for c in stores:
        c.wait()
    halo_done(0, x1, 4, 8)
    halo_done(1, x2r, 4, 8)
    halo_done(2, h3, 1, 4)
    halo_done(3, h4, 1, 4)
    for ph in range(4):
        for d in order:
            stat_copy(ph, d, me).wait_send()
    for which in range(3):
        for d in range(1, ny):
            group(d, sy, which).wait_send()
    for d in range(1, ny):
        swap(d, sy).wait_send()
    for d in range(1, gx):
        cross(0, d, mx_).wait_send()
    for d in range(1, gy):
        cross(1, d, my_).wait_send()


def solution(mesh):
    ny, nz, ns = mesh.shape["sy"], mesh.shape["sz"], mesh.shape["sample"]
    gx = 4 if ns % 4 == 0 else ns
    gy = ns // gx
    n = ny * nz
    vmem = pl.BlockSpec(memory_space=pltpu.VMEM)
    hbm = pl.BlockSpec(memory_space=pl.ANY)

    def step(volume, hist, w1, w2, w3, w4, gf, sf, gc, sc):
        dma = pltpu.SemaphoreType.DMA
        skip, coarse, amax = pl.pallas_call(
            functools.partial(body_entry, ny, nz, gx, gy),
            out_shape=(
                jax.ShapeDtypeStruct((32, 4, 8, 128), BF16),
                jax.ShapeDtypeStruct((2, 16, 1024), BF16),
                jax.ShapeDtypeStruct((1, 128), F32),
            ),
            in_specs=[hbm, vmem, hbm, hbm, hbm, hbm, vmem, vmem, vmem, vmem],
            out_specs=(hbm, vmem, vmem),
            scratch_shapes=[
                pltpu.VMEM((4, 32, 8, 128), BF16),
                pltpu.VMEM((9, 96, 32), BF16),
                pltpu.VMEM((9, 96, 32), BF16),
                pltpu.VMEM((9, 48, 32), BF16),
                pltpu.VMEM((9, 48, 64), BF16),
                pltpu.VMEM((96, 288), BF16),
                pltpu.VMEM((96, 288), BF16),
                pltpu.VMEM((ny, 48, 288), BF16),
                pltpu.VMEM((ny, 48, 576), BF16),
                pltpu.VMEM((6, 10, 32, 128), BF16),
                pltpu.VMEM((4, 8, 32, 128), F32),
                pltpu.VMEM((6, 10, 32, 128), BF16),
                pltpu.VMEM((6, 10, 32, 128), BF16),
                pltpu.VMEM((4, 8, 32, 128), F32),
                pltpu.VMEM((3, 6, 32, 128), BF16),
                pltpu.VMEM((4, 32, 128), F32),
                pltpu.VMEM((3, 6, 32, 128), BF16),
                pltpu.VMEM((3, 6, 64, 128), BF16),
                pltpu.VMEM((4, 64, 128), F32),
                pltpu.VMEM((3, 6, 64, 128), BF16),
                pltpu.VMEM((ny, 4, 16, 128), F32),
                pltpu.VMEM((ny, 4, 16, 128), F32),
                pltpu.VMEM((ny, 2, 16, 128), F32),
                pltpu.VMEM((4, n, 2, 128), F32),
                pltpu.VMEM((2, 4, 1, 128), F32),
                pltpu.VMEM((4, 32, 8, 128), BF16),
                pltpu.VMEM((8, 128), F32),
                pltpu.VMEM((128, 128), F32),
                dma((8,)),
                dma((4,)),
                dma((4, 8)),
                dma((4, 8)),
                dma((4, n)),
                dma((4, n)),
                dma((3, ny)),
                dma((3, ny)),
                dma((ny,)),
                dma((ny,)),
                dma((2, 4)),
                dma((2, 4)),
            ],
            compiler_params=pltpu.CompilerParams(collective_id=0, has_side_effects=True),
            name="encoder",
        )(
            volume.reshape(32, 4, 8, 128), hist, w1.reshape(9, 96, 32), w2.reshape(9, 96, 32),
            w3.reshape(9, 48, 32), w4.reshape(9, 48, 64), gf, sf, gc, sc,
        )
        return (
            skip.reshape(1, 32, 4, 8, 128),
            jnp.transpose(coarse, (1, 0, 2)).reshape(1, 16, 2, 1024),
            amax[0, :4],
        )

    return jax.shard_map(
        step,
        mesh=mesh,
        in_specs=(
            P("sample", None, "sz", "sy", None), P(), P(), P(),
            P(None, "sy", None), P(None, "sy", None), P(), P(), P(None, "sy"), P(None, "sy"),
        ),
        out_specs=(P("sample", None, "sz", "sy", None), P("sample", "sy", "sz", None), P()),
        check_vma=False,
    )


def body_entry(ny, nz, gx, gy, *refs):
    (
        vol, hist, w1, w2, w3, w4, gf, sf, gc, sc, skip, coarse, amax,
        vin, w1v, w2v, w3v, w4v, wf1, wf2, wg3, wg4,
        x1, r1, x2r, x2, r2, h3, p3, c3, h4, r4i, c4, a2a, a2s, gcol,
        st, am, outv, rows8, tcols,
        lsem, osem, hs, hr, ss, sr, ws, wr, bs, br, xs, xr,
    ) = refs
    body(
        ny, nz, gx, gy,
        vol, hist, w1, w2, w3, w4, gf, sf, gc, sc, skip, coarse, amax,
        vin, w1v, w2v, w3v, w4v, wf1, wf2, wg3, wg4,
        x1, r1, x2r, x2, r2, h3, p3, c3, h4, r4i, c4, a2a, a2s, gcol,
        st, am, outv, rows8,
        lsem, osem, hs, hr, ss, sr, ws, wr, tcols, None, bs, br, xs, xr,
    )
```

```python
import functools

import jax
import jax.numpy as jnp
from jax import lax
from jax.experimental import pallas as pl
from jax.experimental.pallas import tpu as pltpu
from jax.sharding import PartitionSpec as P

MESH = pl.DeviceIdType.MESH
F32 = jnp.float32
BF16 = jnp.bfloat16
EPS = 1e-05
SLOPE = 0.01
DIRS = ((-1, 0), (1, 0), (-1, -1), (-1, 1), (1, -1), (1, 1), (0, -1), (0, 1))


def body(
    ny, nz, gx, gy,
    vol, hist_h, w1, w2, w3, w4, gf_h, sf_h, gc_h, sc_h,
    skip, coarse, amax,
    hist, gf, sf, gc, sc, vin, w1v, w2v, w3v, w4v, wf1, wf2, wg3, wg4,
    x1, r1, x2r, x2, r2, h3, z3s, z3r, p3, c3, c3z, h4, z4s, z4r, r4i, c4, c4z, a2a, a2s, gcol,
    st, am, outv, rows8,
    lsem, osem, hs, hr, ss, sr, ws, wr, gs, gr, bs, br, xs, xr,
):
    n = ny * nz
    sy = lax.axis_index("sy")
    sz = lax.axis_index("sz")
    smp = lax.axis_index("sample")
    me = sz * ny + sy
    mx_, my_ = lax.rem(smp, gx), lax.div(smp, gx)

    loads = [pltpu.make_async_copy(vol.at[:, z], vin.at[z], lsem.at[z]) for z in range(4)]
    small = ((hist_h, hist), (w1, w1v), (w2, w2v), (w3, w3v), (w4, w4v), (gf_h, gf), (sf_h, sf), (gc_h, gc), (sc_h, sc))
    for i, (s, d) in enumerate(small):
        loads.append(pltpu.make_async_copy(s, d, lsem.at[4 + i]))
    for i in (4, 0, 3, 1, 2, 5, 6, 7, 8, 9, 10, 11, 12):
        loads[i].start()

    def partner(d):
        p = lax.rem(me + d, n)
        return p, {"sy": lax.rem(p, ny), "sz": lax.div(p, ny)}

    order = sorted(range(1, n), key=lambda d: -min(d, n - d))
    barrier = pltpu.get_barrier_semaphore()
    for d in order:
        pl.semaphore_signal(barrier, inc=1, device_id=partner(d)[1], device_id_type=MESH)

    def xpeer(d):
        q = lax.rem(mx_ + d, gx)
        return q, {"sample": my_ * gx + q}

    def ypeer(d):
        q = lax.rem(my_ + d, gy)
        return q, {"sample": q * gx + mx_}

    for d in range(1, gx):
        pl.semaphore_signal(barrier, inc=1, device_id=xpeer(d)[1], device_id_type=MESH)
    for d in range(1, gy):
        pl.semaphore_signal(barrier, inc=1, device_id=ypeer(d)[1], device_id_type=MESH)

    def exists(dz, dy):
        cond = None
        for idx, cnt, d in ((sz, nz, dz), (sy, ny, dy)):
            if d == 0:
                continue
            c = (idx > 0) if d < 0 else (idx < cnt - 1)
            cond = c if cond is None else jnp.logical_and(cond, c)
        return cond

    lane = lax.broadcasted_iota(jnp.int32, (1, 128), 1)
    lower = lane < 64

    def bound_of(l):
        b = jnp.max(hist[l : l + 1, :], axis=1, keepdims=True)
        return b.astype(BF16).astype(F32)

    def src_z(dz, zl):
        return pl.ds(1, zl) if dz == 0 else (pl.ds(1, 1) if dz < 0 else pl.ds(zl, 1))

    def dst_z(dz, zl):
        return pl.ds(1, zl) if dz == 0 else (pl.ds(zl + 1, 1) if dz < 0 else pl.ds(0, 1))

    def halo(ph, buf, zl, yl, i):
        dz, dy = DIRS[i]
        return pltpu.make_async_remote_copy(
            src_ref=buf.at[src_z(dz, zl), src_z(dy, yl)],
            dst_ref=buf.at[dst_z(dz, zl), dst_z(dy, yl)],
            send_sem=hs.at[ph, i],
            recv_sem=hr.at[ph, i],
            device_id={"sy": sy + dy, "sz": sz + dz},
            device_id_type=MESH,
        )

    def halo_send(ph, buf, zl, yl, which):
        for i in which:
            @pl.when(exists(*DIRS[i]))
            def _():
                halo(ph, buf, zl, yl, i).start()

    def halo_wait(ph, buf, zl, yl, which):
        for i in which:
            @pl.when(exists(-DIRS[i][0], -DIRS[i][1]))
            def _():
                halo(ph, buf, zl, yl, i).wait_recv()

    def halo_done(ph, buf, zl, yl):
        for i in range(8):
            @pl.when(exists(*DIRS[i]))
            def _():
                halo(ph, buf, zl, yl, i).wait_send()

    def coarse_halo(ph, own, zs, zr, i):
        dz, dy = DIRS[i]
        if dz == 0:
            src, dst = own.at[src_z(dy, 4)], own.at[dst_z(dy, 4)]
        else:
            up = 1 if dz > 0 else 0
            src, dst = zs.at[up, src_z(dy, 4)], zr.at[1 - up, dst_z(dy, 4)]
        return pltpu.make_async_remote_copy(
            src_ref=src, dst_ref=dst, send_sem=hs.at[ph, i], recv_sem=hr.at[ph, i],
            device_id={"sy": sy + dy, "sz": sz + dz}, device_id_type=MESH,
        )

    def coarse_send(ph, own, zs, zr):
        for i in range(8):
            @pl.when(exists(*DIRS[i]))
            def _():
                coarse_halo(ph, own, zs, zr, i).start()

    def coarse_done(ph, own, zs, zr):
        for i in range(8):
            @pl.when(exists(*DIRS[i]))
            def _():
                coarse_halo(ph, own, zs, zr, i).wait_send()

    def put_raw(blk, y, own, zs):
        half = blk.shape[0] // 2
        top, low = blk[:half], blk[half:]
        own[y] = blk.astype(BF16)
        zs[0, y] = jnp.where(lower, top, pltpu.roll(low, 64, 1)).astype(BF16)
        zs[1, y] = jnp.where(lower, pltpu.roll(top, 64, 1), low).astype(BF16)

    def coarse_settle(ph, own, zs, zr, buf, zbuf, aff, b):
        half = buf.shape[1] // 2
        paff = tuple(jnp.where(lower, t[:half], t[half:]) for t in aff)
        for i in range(8):
            dz, dy = DIRS[i]
            there = exists(-dz, -dy)
            ys = slots(dy, 4)

            @pl.when(there)
            def _():
                coarse_halo(ph, own, zs, zr, i).wait_recv()
                for y in ys:
                    if dz == 0:
                        buf[y] = settle(own[y].astype(F32), aff, b)
                    else:
                        k = 0 if dz > 0 else 1
                        zbuf[k, y] = settle(zr[k, y].astype(F32), paff, b)

            @pl.when(jnp.logical_not(there))
            def _():
                for y in ys:
                    if dz == 0:
                        buf[y] = jnp.zeros(buf.shape[1:], BF16)
                    else:
                        k = 0 if dz > 0 else 1
                        zbuf[k, y] = jnp.zeros(zbuf.shape[2:], BF16)

    def slots(d, length):
        return range(1, length + 1) if d == 0 else ((0,) if d > 0 else (length + 1,))

    def stat_copy(ph, d, src):
        p, dev = partner(d)
        return pltpu.make_async_remote_copy(
            src_ref=st.at[ph, me],
            dst_ref=st.at[ph, src],
            send_sem=ss.at[ph, d],
            recv_sem=sr.at[ph, src],
            device_id=dev,
            device_id_type=MESH,
        )

    def stat_send(ph, rows):
        st[ph, me] = rows
        for d in order:
            stat_copy(ph, d, me).start()

    def stat_wait(ph):
        for d in order:
            stat_copy(ph, d, partner(d)[0]).wait_recv()
        return st[ph]

    def to_rows(cols):
        return jnp.transpose(cols)

    def to_cols(row):
        return jnp.transpose(jnp.broadcast_to(row, (128, 128)))

    def affine(tot, totsq, cells, g, s):
        m = tot / cells
        var = totsq / cells - m * m
        a = lax.rsqrt(var + EPS) * g
        return a, m, s

    def act(v, aff):
        a, m, s = aff
        t = (v - m) * a + s
        return jnp.maximum(t, SLOPE * t)

    ri = lax.broadcasted_iota(jnp.int32, (256, 256), 0)
    ci = lax.broadcasted_iota(jnp.int32, (256, 256), 1)

    def onehot(cond):
        return jnp.where(cond, 1.0, 0.0).astype(BF16)

    into = onehot(jnp.logical_and((ri & 31) == (ci >> 3), (ri >> 5) == (ci & 7)))

    loads[4].wait()
    b0 = bound_of(0)
    peak0 = jnp.zeros((256, 128), F32)
    for zp in ((0, 3), (1, 2)):
        parts = []
        for z in zp:
            loads[z].wait()
            v = vin[z].astype(F32).reshape(256, 128)
            peak0 = jnp.maximum(peak0, jnp.abs(v))
            parts.append(v.astype(BF16))
        moved = jnp.dot(into, jnp.concatenate(parts, axis=1), preferred_element_type=F32)
        moved = jnp.clip(moved, -b0, b0).astype(BF16)
        for k in range(2):
            for y in range(8):
                x1[1 + zp[k], 1 + y] = moved[32 * y : 32 * y + 32, 128 * k : 128 * k + 128]
    peak0 = jnp.max(jnp.max(peak0, axis=0, keepdims=True), axis=1, keepdims=True)

    pl.semaphore_wait(barrier, (n - 1) + (gx - 1) + (gy - 1))
    halo_send(0, x1, 4, 8, range(8))

    for i in range(5, 13):
        loads[i].wait()
    rows8[...] = jnp.zeros_like(rows8)
    rows8[0:2, 0:32] = gf[...]
    rows8[2:4, 0:32] = sf[...]
    rows8[4:6, 0:16] = gc[...]
    rows8[6:8, 0:16] = sc[...]
    gcols = jnp.transpose(rows8[...])

    def gain_col(j, count):
        return jnp.broadcast_to(gcols[0:count, j : j + 1], (count, 128))


    def lanes_of(w):
        return jnp.concatenate([w[k] for k in range(9)], axis=1)

    wf1[...] = lanes_of(w1v)
    wf2[...] = lanes_of(w2v)
    wg3[sy] = lanes_of(w3v)
    wg4[sy] = lanes_of(w4v)
    gcol[sy, 0] = gain_col(4, 16)
    gcol[sy, 1] = gain_col(6, 16)

    def zero_missing(buf, zl, yl):
        for i in range(8):
            dz, dy = DIRS[i]
            @pl.when(jnp.logical_not(exists(-dz, -dy)))
            def _():
                for z in slots(dz, zl):
                    for y in slots(dy, yl):
                        buf[z, y] = jnp.zeros(buf.shape[2:], buf.dtype)

    zero_missing(x1, 4, 8)

    first, last = lane == 0, lane == 127

    def combine(p0, p1, p2, lo, hi):
        left = jnp.where(lo, 0.0, pltpu.roll(p0, 1, 1))
        right = jnp.where(hi, 0.0, pltpu.roll(p2, 127, 1))
        return p1 + left + right

    def fine_conv(buf, w, z):
        strips = []
        for zt in range(3):
            blocks = [buf[z + zt, y] for y in range(10)]
            for yt in range(3):
                strips.append(jnp.concatenate(blocks[yt : yt + 8], axis=1))
        got = jnp.dot(w, jnp.concatenate(strips, axis=0), preferred_element_type=F32)
        outs = []
        for y in range(8):
            blk = got[:, 128 * y : 128 * y + 128]
            outs.append(combine(blk[0:32], blk[32:64], blk[64:96], first, last))
        return outs

    zero = jnp.zeros((32, 128), F32)

    def gather_stats(acc, blocks, extremes):
        s, q, hi, lo = acc
        for b in blocks:
            s = s + b
            q = q + b * b
            if extremes:
                hi = jnp.maximum(hi, b)
                lo = jnp.minimum(lo, b)
        return s, q, hi, lo

    def mixed_row(cols):
        t = to_rows(cols)
        total = jnp.sum(t, axis=0, keepdims=True)
        high = jnp.max(t, axis=0, keepdims=True)
        low = jnp.min(t, axis=0, keepdims=True)
        return jnp.where(lane < 64, total, jnp.where(lane < 96, high, low))

    def mixed_total(got):
        total = jnp.sum(got[:, 0:1, :], axis=0)
        high = jnp.max(got[:, 0:1, :], axis=0)
        low = jnp.min(got[:, 0:1, :], axis=0)
        return to_cols(jnp.where(lane < 64, total, jnp.where(lane < 96, high, low)))

    wa = wf1[...]
    acc = (zero, zero, jnp.full((32, 128), -jnp.inf, F32), jnp.full((32, 128), jnp.inf, F32))
    halo_wait(0, x1, 4, 8, (6, 7))
    for z in (1, 2):
        outs = fine_conv(x1, wa, z)
        acc = gather_stats(acc, outs, True)
        for y in range(8):
            r1[z, y] = outs[y]
        x2r[z + 1, 1] = outs[0].astype(BF16)
        x2r[z + 1, 8] = outs[7].astype(BF16)
    halo_wait(0, x1, 4, 8, range(6))
    for z in (0, 3):
        outs = fine_conv(x1, wa, z)
        acc = gather_stats(acc, outs, True)
        for y in range(8):
            r1[z, y] = outs[y]
            x2r[z + 1, y + 1] = outs[y].astype(BF16)
    row = mixed_row(jnp.concatenate(acc, axis=0))
    stat_send(0, jnp.concatenate([row, jnp.broadcast_to(peak0, (1, 128))], axis=0))
    halo_send(1, x2r, 4, 8, range(8))

    mate = sy + 1 - 2 * lax.rem(sy, 2)
    cross_sy = lax.rem(sy + 2, 4)
    cross_mate = lax.rem(mate + 2, 4)

    def group(which, kind, src):
        buf = (wg3, wg4, gcol)[which]
        return pltpu.make_async_remote_copy(
            src_ref=buf.at[src], dst_ref=buf.at[src],
            send_sem=ws.at[which, kind], recv_sem=wr.at[which, src],
            device_id={"sy": cross_sy if kind == 1 else mate}, device_id_type=MESH,
        )

    for which in (2, 0, 1):
        group(which, 1, sy).start()
        group(which, 0, sy).start()

    def group_forward(which):
        group(which, 1, cross_sy).wait_recv()
        group(which, 2, cross_sy).start()

    def group_wait(which):
        group(which, 0, mate).wait_recv()
        group(which, 2, cross_mate).wait_recv()

    def group_done(which):
        group(which, 0, sy).wait_send()
        group(which, 1, sy).wait_send()
        group(which, 2, cross_sy).wait_send()

    fine_cells = float(4 * nz * 8 * ny * 128)
    coarse_cells = fine_cells / 8

    def fine_affine(cols, j):
        return affine(cols[0:32], cols[32:64], fine_cells, gain_col(j, 32), gain_col(2 + j, 32))

    def peak_of(high, low, aff):
        v = jnp.maximum(jnp.abs(act(high, aff)), jnp.abs(act(low, aff))).astype(BF16).astype(F32)
        return jnp.max(jnp.max(v, axis=0, keepdims=True), axis=1, keepdims=True)

    got = stat_wait(0)
    peak0 = jnp.max(jnp.max(got[:, 1:2, :], axis=0), axis=1, keepdims=True)
    cols = mixed_total(got)
    aff = fine_affine(cols, 0)
    peak1 = peak_of(cols[64:96], cols[96:128], aff)
    b1 = bound_of(1)

    def settle(v, aff, b):
        return jnp.clip(act(v, aff), -b, b).astype(BF16)

    for z in range(4):
        for y in range(8):
            x2[z + 1, y + 1] = settle(r1[z, y], aff, b1)

    def settle_halo(ph, raw, buf, zl, yl, which, aff, b):
        for i in which:
            dz, dy = DIRS[i]
            there = exists(-dz, -dy)

            @pl.when(there)
            def _():
                halo(ph, raw, zl, yl, i).wait_recv()
                for z in slots(dz, zl):
                    for y in slots(dy, yl):
                        buf[z, y] = settle(raw[z, y].astype(F32), aff, b)

            @pl.when(jnp.logical_not(there))
            def _():
                for z in slots(dz, zl):
                    for y in slots(dy, yl):
                        buf[z, y] = jnp.zeros(buf.shape[2:], buf.dtype)

    wb = wf2[...]
    acc = (zero, zero, None, None)
    settle_halo(1, x2r, x2, 4, 8, (6, 7), aff, b1)
    for z in (1, 2):
        outs = fine_conv(x2, wb, z)
        acc = gather_stats(acc, outs, False)
        for y in range(8):
            r2[z, y] = outs[y]
    settle_halo(1, x2r, x2, 4, 8, range(6), aff, b1)

    for which in (2, 0, 1):
        group_forward(which)

    for z in (0, 3):
        outs = fine_conv(x2, wb, z)
        acc = gather_stats(acc, outs, False)
        for y in range(8):
            r2[z, y] = outs[y]

    s_r = lax.broadcasted_iota(jnp.int32, (256, 128), 0)
    s_c = lax.broadcasted_iota(jnp.int32, (256, 128), 1)
    pick = onehot(s_r == jnp.where(s_c < 64, 2 * s_c, 2 * s_c))
    highs, lows = [], []
    for zp in range(2):
        hrow, lrow = [], []
        for yp in range(4):
            m = jnp.maximum(
                jnp.maximum(r2[2 * zp, 2 * yp], r2[2 * zp, 2 * yp + 1]),
                jnp.maximum(r2[2 * zp + 1, 2 * yp], r2[2 * zp + 1, 2 * yp + 1]),
            )
            m = jnp.maximum(m, pltpu.roll(m, 127, 1))
            h = m.astype(BF16)
            hrow.append(h)
            lrow.append((m - h.astype(F32)).astype(BF16))
        highs.append(jnp.concatenate(hrow, axis=0))
        lows.append(jnp.concatenate(lrow, axis=0))
    pooled = jnp.dot(jnp.concatenate(highs, axis=1), pick, preferred_element_type=F32)
    pooled = pooled + jnp.dot(jnp.concatenate(lows, axis=1), pick, preferred_element_type=F32)
    hi = jnp.full((32, 128), -jnp.inf, F32)
    lo = jnp.full((32, 128), jnp.inf, F32)
    for yp in range(4):
        blk = pooled[32 * yp : 32 * yp + 32]
        p3[yp] = blk
        put_raw(blk, yp + 1, h3, z3s)
        hi = jnp.maximum(hi, blk)
        lo = jnp.minimum(lo, blk)
    row = mixed_row(jnp.concatenate([acc[0], acc[1], hi, lo], axis=0))
    stat_send(1, jnp.concatenate([row, row], axis=0))
    coarse_send(2, h3, z3s, z3r)

    got = stat_wait(1)
    cols = mixed_total(got)
    aff2 = fine_affine(cols, 1)
    peak2 = peak_of(cols[64:96], cols[96:128], aff2)
    b2 = bound_of(2)
    for yp in range(4):
        c3[yp + 1] = settle(p3[yp], aff2, b2)
    coarse_settle(2, h3, z3s, z3r, c3, c3z, aff2, b2)

    cfirst, clast = (lane & 63) == 0, (lane & 63) == 63

    def coarse_conv(buf, zbuf, w):
        strips = []
        mids = [buf[y] for y in range(6)]
        pairs = [[], mids, []]
        half = buf.shape[1] // 2
        for y in range(6):
            own = pltpu.roll(mids[y].astype(F32), 64, 1)
            prev = zbuf[0, y].astype(F32)
            nxt = zbuf[1, y].astype(F32)
            a = jnp.where(lower, prev, own[:half])
            b = jnp.where(lower, pltpu.roll(prev, 64, 1), own[half:])
            pairs[0].append(jnp.concatenate([a, b], axis=0).astype(BF16))
            a = jnp.where(lower, own[:half], pltpu.roll(nxt, 64, 1))
            b = jnp.where(lower, own[half:], nxt)
            pairs[2].append(jnp.concatenate([a, b], axis=0).astype(BF16))
        for zt in range(3):
            for yt in range(3):
                strips.append(jnp.concatenate(pairs[zt][yt : yt + 4], axis=1))
        got = jnp.dot(w, jnp.concatenate(strips, axis=0), preferred_element_type=F32)
        outs = []
        for y in range(4):
            blk = got[:, 128 * y : 128 * y + 128]
            parts = []
            for g in range(4):
                t = blk[48 * g : 48 * g + 48]
                parts.append(combine(t[0:16], t[16:32], t[32:48], cfirst, clast))
            outs.append(jnp.concatenate(parts, axis=0))
        return outs

    group_wait(0)
    outs = coarse_conv(c3, c3z, wg3[...].reshape(192, 288))
    zero64 = jnp.zeros((64, 128), F32)
    acc = (zero64, zero64, jnp.full((64, 128), -jnp.inf, F32), jnp.full((64, 128), jnp.inf, F32))
    acc = gather_stats(acc, outs, True)
    for y in range(4):
        put_raw(outs[y], y + 1, h4, z4s)
        r4i[y] = outs[y]

    def double_rows(acc, extremes):
        t = to_rows(jnp.concatenate(acc[0:2], axis=0))
        r0 = jnp.sum(t, axis=0, keepdims=True)
        if not extremes:
            return jnp.concatenate([r0, r0], axis=0)
        t = to_rows(jnp.concatenate(acc[2:4], axis=0))
        high = jnp.max(t, axis=0, keepdims=True)
        low = jnp.min(t, axis=0, keepdims=True)
        return jnp.concatenate([r0, jnp.where(lower, high, low)], axis=0)

    stat_send(2, double_rows(acc, True))
    coarse_send(3, h4, z4s, z4r)

    outof = onehot(jnp.logical_and((ci & 31) == (ri >> 3), (ci >> 5) == (ri & 7)))
    stores = []
    for zp in range(2):
        parts = []
        for z in (2 * zp, 2 * zp + 1):
            parts.append(jnp.concatenate([act(r2[z, y], aff2).astype(BF16) for y in range(8)], axis=0))
        moved = jnp.dot(outof, jnp.concatenate(parts, axis=1), preferred_element_type=F32)
        for k in range(2):
            z = 2 * zp + k
            outv[z] = moved[:, 128 * k : 128 * k + 128].reshape(32, 8, 128).astype(BF16)
            stores.append(pltpu.make_async_copy(outv.at[z], skip.at[:, z], osem.at[z]))
            stores[-1].start()

    group_wait(2)
    gall = gcol[...]
    got = stat_wait(2)
    cols = to_cols(jnp.sum(got[:, 0:1, :], axis=0))
    high = jnp.max(got[:, 1:2, :], axis=0)
    low = jnp.min(got[:, 1:2, :], axis=0)
    ext = to_cols(jnp.where(lower, high, low))
    aff3 = affine(cols[0:64], cols[64:128], coarse_cells, gall[:, 0].reshape(64, 128), gall[:, 1].reshape(64, 128))
    peak3 = peak_of(ext[0:64], ext[64:128], aff3)
    b3 = bound_of(3)

    peaks = jnp.where(lane == 0, peak0, jnp.where(lane == 1, peak1, jnp.where(lane == 2, peak2, peak3)))

    def cross(step, d, src):
        mine, peer = (mx_, xpeer) if step == 0 else (my_, ypeer)
        return pltpu.make_async_remote_copy(
            src_ref=am.at[step, mine], dst_ref=am.at[step, src],
            send_sem=xs.at[step, d], recv_sem=xr.at[step, src],
            device_id=peer(d)[1], device_id_type=MESH,
        )

    am[0, mx_] = peaks
    for d in range(1, gx):
        cross(0, d, mx_).start()

    for y in range(4):
        c4[y + 1] = settle(r4i[y], aff3, b3)
    coarse_settle(3, h4, z4s, z4r, c4, c4z, aff3, b3)

    group_wait(1)
    outs = coarse_conv(c4, c4z, wg4[...].reshape(192, 576))
    acc = gather_stats((zero64, zero64, None, None), outs, False)
    for g in range(4):
        for y in range(4):
            a2s[g, y] = outs[y][16 * g : 16 * g + 16]

    def swap(d, src):
        q = lax.rem(sy + d, ny)
        return pltpu.make_async_remote_copy(
            src_ref=a2s.at[q], dst_ref=a2a.at[src],
            send_sem=bs.at[d], recv_sem=br.at[src],
            device_id={"sy": q}, device_id_type=MESH,
        )

    stat_send(3, double_rows(acc, False))
    for d in range(1, ny):
        swap(d, sy).start()
    a2a[sy] = a2s[sy]

    for d in range(1, gx):
        cross(0, d, xpeer(d)[0]).wait_recv()
    am[1, my_] = jnp.max(am[0, 0:gx], axis=0)
    for d in range(1, gy):
        cross(1, d, my_).start()

    for d in range(1, ny):
        swap(d, lax.rem(sy + d, ny)).wait_recv()
    got = stat_wait(3)
    rows8b = to_cols(jnp.sum(got[:, 0:1, :], axis=0))
    gs[...] = rows8b
    tot = gs[pl.ds(pl.multiple_of(sy * 16, 8), 16), :]
    totsq = gs[pl.ds(pl.multiple_of(64 + sy * 16, 8), 16), :]
    aff4 = affine(tot, totsq, coarse_cells, gain_col(5, 16), gain_col(7, 16))
    planes = [[], []]
    for g in range(4):
        for yp in range(2):
            u = act(a2a[g, 2 * yp], aff4)
            v = act(a2a[g, 2 * yp + 1], aff4)
            planes[0].append(jnp.where(lower, u, pltpu.roll(v, 64, 1)))
            planes[1].append(jnp.where(lower, pltpu.roll(u, 64, 1), v))
    for z in range(2):
        coarse[z] = jnp.concatenate(planes[z], axis=1).astype(BF16)

    for d in range(1, gy):
        cross(1, d, ypeer(d)[0]).wait_recv()
    amax[...] = jnp.max(am[1, 0:gy], axis=0)

    for c in stores:
        c.wait()
    halo_done(0, x1, 4, 8)
    halo_done(1, x2r, 4, 8)
    coarse_done(2, h3, z3s, z3r)
    coarse_done(3, h4, z4s, z4r)
    for ph in range(4):
        for d in order:
            stat_copy(ph, d, me).wait_send()
    for which in range(3):
        group_done(which)
    for d in range(1, ny):
        swap(d, sy).wait_send()
    for d in range(1, gx):
        cross(0, d, mx_).wait_send()
    for d in range(1, gy):
        cross(1, d, my_).wait_send()


def solution(mesh):
    ny, nz, ns = mesh.shape["sy"], mesh.shape["sz"], mesh.shape["sample"]
    gx = 4 if ns % 4 == 0 else ns
    gy = ns // gx
    n = ny * nz
    vmem = pl.BlockSpec(memory_space=pltpu.VMEM)
    hbm = pl.BlockSpec(memory_space=pl.ANY)

    def step(volume, hist, w1, w2, w3, w4, gf, sf, gc, sc):
        dma = pltpu.SemaphoreType.DMA
        skip, coarse, amax = pl.pallas_call(
            functools.partial(body_entry, ny, nz, gx, gy),
            out_shape=(
                jax.ShapeDtypeStruct((32, 4, 8, 128), BF16),
                jax.ShapeDtypeStruct((2, 16, 1024), BF16),
                jax.ShapeDtypeStruct((1, 128), F32),
            ),
            in_specs=[hbm] * 10,
            out_specs=(hbm, vmem, vmem),
            scratch_shapes=[
                pltpu.VMEM((4, 16), F32),
                pltpu.VMEM((2, 32), F32),
                pltpu.VMEM((2, 32), F32),
                pltpu.VMEM((2, 16), F32),
                pltpu.VMEM((2, 16), F32),
                pltpu.VMEM((4, 32, 8, 128), BF16),
                pltpu.VMEM((9, 96, 32), BF16),
                pltpu.VMEM((9, 96, 32), BF16),
                pltpu.VMEM((9, 48, 32), BF16),
                pltpu.VMEM((9, 48, 64), BF16),
                pltpu.VMEM((96, 288), BF16),
                pltpu.VMEM((96, 288), BF16),
                pltpu.VMEM((ny, 48, 288), BF16),
                pltpu.VMEM((ny, 48, 576), BF16),
                pltpu.VMEM((6, 10, 32, 128), BF16),
                pltpu.VMEM((4, 8, 32, 128), F32),
                pltpu.VMEM((6, 10, 32, 128), BF16),
                pltpu.VMEM((6, 10, 32, 128), BF16),
                pltpu.VMEM((4, 8, 32, 128), F32),
                pltpu.VMEM((6, 32, 128), BF16),
                pltpu.VMEM((2, 6, 16, 128), BF16),
                pltpu.VMEM((2, 6, 16, 128), BF16),
                pltpu.VMEM((4, 32, 128), F32),
                pltpu.VMEM((6, 32, 128), BF16),
                pltpu.VMEM((2, 6, 16, 128), BF16),
                pltpu.VMEM((6, 64, 128), BF16),
                pltpu.VMEM((2, 6, 32, 128), BF16),
                pltpu.VMEM((2, 6, 32, 128), BF16),
                pltpu.VMEM((4, 64, 128), F32),
                pltpu.VMEM((6, 64, 128), BF16),
                pltpu.VMEM((2, 6, 32, 128), BF16),
                pltpu.VMEM((ny, 4, 16, 128), F32),
                pltpu.VMEM((ny, 4, 16, 128), F32),
                pltpu.VMEM((ny, 2, 16, 128), F32),
                pltpu.VMEM((4, n, 2, 128), F32),
                pltpu.VMEM((2, 4, 1, 128), F32),
                pltpu.VMEM((4, 32, 8, 128), BF16),
                pltpu.VMEM((8, 128), F32),
                pltpu.VMEM((128, 128), F32),
                dma((13,)),
                dma((4,)),
                dma((4, 8)),
                dma((4, 8)),
                dma((4, n)),
                dma((4, n)),
                dma((3, 3)),
                dma((3, ny)),
                dma((ny,)),
                dma((ny,)),
                dma((2, 4)),
                dma((2, 4)),
            ],
            compiler_params=pltpu.CompilerParams(collective_id=0, has_side_effects=True),
            name="encoder",
        )(
            volume.reshape(32, 4, 8, 128), hist, w1.reshape(9, 96, 32), w2.reshape(9, 96, 32),
            w3.reshape(9, 48, 32), w4.reshape(9, 48, 64), gf, sf, gc, sc,
        )
        return (
            skip.reshape(1, 32, 4, 8, 128),
            jnp.transpose(coarse, (1, 0, 2)).reshape(1, 16, 2, 1024),
            amax[0, :4],
        )

    return jax.shard_map(
        step,
        mesh=mesh,
        in_specs=(
            P("sample", None, "sz", "sy", None), P(), P(), P(),
            P(None, "sy", None), P(None, "sy", None), P(), P(), P(None, "sy"), P(None, "sy"),
        ),
        out_specs=(P("sample", None, "sz", "sy", None), P("sample", "sy", "sz", None), P()),
        check_vma=False,
    )


def body_entry(ny, nz, gx, gy, *refs):
    (
        vol, hist, w1, w2, w3, w4, gf, sf, gc, sc, skip, coarse, amax,
        hist_v, gf_v, sf_v, gc_v, sc_v, vin, w1v, w2v, w3v, w4v, wf1, wf2, wg3, wg4,
        x1, r1, x2r, x2, r2, h3, z3s, z3r, p3, c3, c3z, h4, z4s, z4r, r4i, c4, c4z, a2a, a2s, gcol,
        st, am, outv, rows8, tcols,
        lsem, osem, hs, hr, ss, sr, ws, wr, bs, br, xs, xr,
    ) = refs
    body(
        ny, nz, gx, gy,
        vol, hist, w1, w2, w3, w4, gf, sf, gc, sc, skip, coarse, amax,
        hist_v, gf_v, sf_v, gc_v, sc_v, vin, w1v, w2v, w3v, w4v, wf1, wf2, wg3, wg4,
        x1, r1, x2r, x2, r2, h3, z3s, z3r, p3, c3, c3z, h4, z4s, z4r, r4i, c4, c4z, a2a, a2s, gcol,
        st, am, outv, rows8,
        lsem, osem, hs, hr, ss, sr, ws, wr, tcols, None, bs, br, xs, xr,
    )
```

```python
import functools

import jax
import jax.numpy as jnp
from jax import lax
from jax.experimental import pallas as pl
from jax.experimental.pallas import tpu as pltpu
from jax.sharding import PartitionSpec as P

MESH = pl.DeviceIdType.MESH
F32 = jnp.float32
BF16 = jnp.bfloat16
EPS = 1e-05
SLOPE = 0.01
DIRS = ((-1, 0), (1, 0), (-1, -1), (-1, 1), (1, -1), (1, 1), (0, -1), (0, 1))


def body(
    ny, nz, ns,
    vol, hist_h, w1, w2, w3, w4, gf_h, sf_h, gc_h, sc_h,
    skip, coarse, amax,
    hist, gf, sf, gc, sc, vin, w1v, w2v, w3v, w4v, wf1, wf2, wg3, wg4,
    x1, r1, x2r, x2, r2, h3, z3s, z3r, p3, c3, c3z, h4, z4s, z4r, r4i, c4, c4z, a2a, a2s, gcol,
    st, am, rows8,
    rounds, lsem, hs, hr, ss, sr, ws, wr, gs, gr, bs, br, xs, xr,
):
    n = ny * nz
    sy = lax.axis_index("sy")
    sz = lax.axis_index("sz")
    smp = lax.axis_index("sample")
    me = sz * ny + sy

    near = [{"sz": lax.rem(sz + d, nz)} for d in sorted({1, nz - 1})]
    near += [{"sy": lax.rem(sy + d, ny)} for d in range(1, ny)]
    if ns > 1:
        sx, sv = lax.rem(smp, 4), lax.div(smp, 4)
        near += [{"sample": sv * 4 + lax.rem(sx + d, 4)} for d in (1, 3)]
        near += [{"sample": lax.rem(sv + d, 4) * 4 + sx} for d in (1, 3)]
    barrier = pltpu.get_barrier_semaphore()
    for dev in near:
        pl.semaphore_signal(barrier, inc=1, device_id=dev, device_id_type=MESH)

    def greet(r):
        for dev in near:
            pl.semaphore_signal(rounds.at[r], inc=1, device_id=dev, device_id_type=MESH)

    def greeted(r):
        pl.semaphore_wait(rounds.at[r], len(near))

    loads = [pltpu.make_async_copy(vol.at[:, z], vin.at[z], lsem.at[z]) for z in range(4)]
    small = ((hist_h, hist), (w1, w1v), (w2, w2v), (w3, w3v), (w4, w4v), (gf_h, gf), (sf_h, sf), (gc_h, gc), (sc_h, sc))
    for i, (s, d) in enumerate(small):
        loads.append(pltpu.make_async_copy(s, d, lsem.at[4 + i]))
    for i in (4, 0, 3, 1, 2, 5, 6, 7, 8, 9, 10, 11, 12):
        loads[i].start()

    def partner(d):
        p = lax.rem(me + d, n)
        return p, {"sy": lax.rem(p, ny), "sz": lax.div(p, ny)}

    order = sorted(range(1, n), key=lambda d: -min(d, n - d))
    def other_sample(d):
        q = lax.rem(smp + d, ns)
        return q, {"sample": q}

    def exists(dz, dy):
        cond = None
        for idx, cnt, d in ((sz, nz, dz), (sy, ny, dy)):
            if d == 0:
                continue
            c = (idx > 0) if d < 0 else (idx < cnt - 1)
            cond = c if cond is None else jnp.logical_and(cond, c)
        return cond

    lane = lax.broadcasted_iota(jnp.int32, (1, 128), 1)
    lower = lane < 64

    def bound_of(l):
        b = jnp.max(hist[l : l + 1, :], axis=1, keepdims=True)
        return b.astype(BF16).astype(F32)

    def src_z(dz, zl):
        return pl.ds(1, zl) if dz == 0 else (pl.ds(1, 1) if dz < 0 else pl.ds(zl, 1))

    def dst_z(dz, zl):
        return pl.ds(1, zl) if dz == 0 else (pl.ds(zl + 1, 1) if dz < 0 else pl.ds(0, 1))

    def halo(ph, buf, zl, yl, i):
        dz, dy = DIRS[i]
        return pltpu.make_async_remote_copy(
            src_ref=buf.at[src_z(dz, zl), src_z(dy, yl)],
            dst_ref=buf.at[dst_z(dz, zl), dst_z(dy, yl)],
            send_sem=hs.at[ph, i],
            recv_sem=hr.at[ph, i],
            device_id={"sy": sy + dy, "sz": sz + dz},
            device_id_type=MESH,
        )

    def halo_send(ph, buf, zl, yl, which):
        for i in which:
            @pl.when(exists(*DIRS[i]))
            def _():
                halo(ph, buf, zl, yl, i).start()

    def halo_wait(ph, buf, zl, yl, which):
        for i in which:
            @pl.when(exists(-DIRS[i][0], -DIRS[i][1]))
            def _():
                halo(ph, buf, zl, yl, i).wait_recv()

    def halo_done(ph, buf, zl, yl):
        for i in range(8):
            @pl.when(exists(*DIRS[i]))
            def _():
                halo(ph, buf, zl, yl, i).wait_send()

    def coarse_halo(ph, own, zs, zr, i):
        dz, dy = DIRS[i]
        if dz == 0:
            src, dst = own.at[src_z(dy, 4)], own.at[dst_z(dy, 4)]
        else:
            up = 1 if dz > 0 else 0
            src, dst = zs.at[up, src_z(dy, 4)], zr.at[1 - up, dst_z(dy, 4)]
        return pltpu.make_async_remote_copy(
            src_ref=src, dst_ref=dst, send_sem=hs.at[ph, i], recv_sem=hr.at[ph, i],
            device_id={"sy": sy + dy, "sz": sz + dz}, device_id_type=MESH,
        )

    def coarse_send(ph, own, zs, zr):
        for i in range(8):
            @pl.when(exists(*DIRS[i]))
            def _():
                coarse_halo(ph, own, zs, zr, i).start()

    def coarse_done(ph, own, zs, zr):
        for i in range(8):
            @pl.when(exists(*DIRS[i]))
            def _():
                coarse_halo(ph, own, zs, zr, i).wait_send()

    def put_raw(blk, y, own, zs):
        half = blk.shape[0] // 2
        top, low = blk[:half], blk[half:]
        own[y] = blk.astype(BF16)
        zs[0, y] = jnp.where(lower, top, pltpu.roll(low, 64, 1)).astype(BF16)
        zs[1, y] = jnp.where(lower, pltpu.roll(top, 64, 1), low).astype(BF16)

    def coarse_settle(ph, own, zs, zr, buf, zbuf, aff, b):
        half = buf.shape[1] // 2
        paff = tuple(jnp.where(lower, t[:half], t[half:]) for t in aff)
        for i in range(8):
            dz, dy = DIRS[i]
            there = exists(-dz, -dy)
            ys = slots(dy, 4)

            @pl.when(there)
            def _():
                coarse_halo(ph, own, zs, zr, i).wait_recv()
                for y in ys:
                    if dz == 0:
                        buf[y] = settle(own[y].astype(F32), aff, b)
                    else:
                        k = 0 if dz > 0 else 1
                        zbuf[k, y] = settle(zr[k, y].astype(F32), paff, b)

            @pl.when(jnp.logical_not(there))
            def _():
                for y in ys:
                    if dz == 0:
                        buf[y] = jnp.zeros(buf.shape[1:], BF16)
                    else:
                        k = 0 if dz > 0 else 1
                        zbuf[k, y] = jnp.zeros(zbuf.shape[2:], BF16)

    def slots(d, length):
        return range(1, length + 1) if d == 0 else ((0,) if d > 0 else (length + 1,))

    def stat_copy(ph, d, src):
        p, dev = partner(d)
        return pltpu.make_async_remote_copy(
            src_ref=st.at[ph, me],
            dst_ref=st.at[ph, src],
            send_sem=ss.at[ph, d],
            recv_sem=sr.at[ph, src],
            device_id=dev,
            device_id_type=MESH,
        )

    def stat_send(ph, rows):
        st[ph, me] = rows
        for d in order:
            stat_copy(ph, d, me).start()

    def stat_wait(ph):
        for d in order:
            stat_copy(ph, d, partner(d)[0]).wait_recv()
        return st[ph]

    def to_rows(cols):
        return jnp.transpose(cols)

    def to_cols(row):
        return jnp.transpose(jnp.broadcast_to(row, (128, 128)))

    def affine(tot, totsq, cells, g, s):
        m = tot / cells
        var = totsq / cells - m * m
        a = lax.rsqrt(var + EPS) * g
        return a, m, s

    def act(v, aff):
        a, m, s = aff
        t = (v - m) * a + s
        return jnp.maximum(t, SLOPE * t)

    ri = lax.broadcasted_iota(jnp.int32, (256, 256), 0)
    ci = lax.broadcasted_iota(jnp.int32, (256, 256), 1)

    def onehot(cond):
        return jnp.where(cond, 1.0, 0.0).astype(BF16)

    into = onehot(jnp.logical_and((ri & 31) == (ci >> 3), (ri >> 5) == (ci & 7)))

    loads[4].wait()
    b0 = bound_of(0)
    peak0 = jnp.zeros((256, 128), F32)
    for zp in ((0, 3), (1, 2)):
        parts = []
        for z in zp:
            loads[z].wait()
            v = vin[z].astype(F32).reshape(256, 128)
            peak0 = jnp.maximum(peak0, jnp.abs(v))
            parts.append(v.astype(BF16))
        moved = jnp.dot(into, jnp.concatenate(parts, axis=1), preferred_element_type=F32)
        moved = jnp.clip(moved, -b0, b0).astype(BF16)
        for k in range(2):
            for y in range(8):
                x1[1 + zp[k], 1 + y] = moved[32 * y : 32 * y + 32, 128 * k : 128 * k + 128]
    peak0 = jnp.max(jnp.max(peak0, axis=0, keepdims=True), axis=1, keepdims=True)

    pl.semaphore_wait(barrier, len(near))
    greet(0)
    halo_send(0, x1, 4, 8, (0, 1, 6, 7))

    for i in range(5, 13):
        loads[i].wait()
    rows8[...] = jnp.zeros_like(rows8)
    rows8[0:2, 0:32] = gf[...]
    rows8[2:4, 0:32] = sf[...]
    rows8[4:6, 0:16] = gc[...]
    rows8[6:8, 0:16] = sc[...]
    gcols = jnp.transpose(rows8[...])

    def gain_col(j, count):
        return jnp.broadcast_to(gcols[0:count, j : j + 1], (count, 128))


    def lanes_of(w):
        return jnp.concatenate([w[k] for k in range(9)], axis=1)

    wf1[...] = lanes_of(w1v)
    wf2[...] = lanes_of(w2v)
    wg3[sy] = lanes_of(w3v)
    wg4[sy] = lanes_of(w4v)
    gcol[sy, 0] = gain_col(4, 16)
    gcol[sy, 1] = gain_col(6, 16)

    def zero_missing(buf, zl, yl):
        for i in range(8):
            dz, dy = DIRS[i]
            @pl.when(jnp.logical_not(exists(-dz, -dy)))
            def _():
                for z in slots(dz, zl):
                    for y in slots(dy, yl):
                        buf[z, y] = jnp.zeros(buf.shape[2:], buf.dtype)

    zero_missing(x1, 4, 8)
    greeted(0)
    greet(1)
    halo_send(0, x1, 4, 8, (2, 3, 4, 5))

    first, last = lane == 0, lane == 127

    def combine(p0, p1, p2, lo, hi):
        left = jnp.where(lo, 0.0, pltpu.roll(p0, 1, 1))
        right = jnp.where(hi, 0.0, pltpu.roll(p2, 127, 1))
        return p1 + left + right

    def fine_conv(buf, w, z):
        strips = []
        for zt in range(3):
            blocks = [buf[z + zt, y] for y in range(10)]
            for yt in range(3):
                strips.append(jnp.concatenate(blocks[yt : yt + 8], axis=1))
        got = jnp.dot(w, jnp.concatenate(strips, axis=0), preferred_element_type=F32)
        outs = []
        for y in range(8):
            blk = got[:, 128 * y : 128 * y + 128]
            outs.append(combine(blk[0:32], blk[32:64], blk[64:96], first, last))
        return outs

    zero = jnp.zeros((32, 128), F32)

    def gather_stats(acc, blocks, extremes):
        s, q, hi, lo = acc
        for b in blocks:
            s = s + b
            q = q + b * b
            if extremes:
                hi = jnp.maximum(hi, b)
                lo = jnp.minimum(lo, b)
        return s, q, hi, lo

    def mixed_row(cols):
        t = to_rows(cols)
        total = jnp.sum(t, axis=0, keepdims=True)
        high = jnp.max(t, axis=0, keepdims=True)
        low = jnp.min(t, axis=0, keepdims=True)
        return jnp.where(lane < 64, total, jnp.where(lane < 96, high, low))

    def mixed_total(got):
        total = jnp.sum(got[:, 0:1, :], axis=0)
        high = jnp.max(got[:, 0:1, :], axis=0)
        low = jnp.min(got[:, 0:1, :], axis=0)
        return to_cols(jnp.where(lane < 64, total, jnp.where(lane < 96, high, low)))

    wa = wf1[...]
    acc = (zero, zero, jnp.full((32, 128), -jnp.inf, F32), jnp.full((32, 128), jnp.inf, F32))
    halo_wait(0, x1, 4, 8, (6, 7))
    for z in (1, 2):
        outs = fine_conv(x1, wa, z)
        acc = gather_stats(acc, outs, True)
        for y in range(8):
            r1[z, y] = outs[y]
        x2r[z + 1, 1] = outs[0].astype(BF16)
        x2r[z + 1, 8] = outs[7].astype(BF16)
    halo_wait(0, x1, 4, 8, range(6))
    for z in (0, 3):
        outs = fine_conv(x1, wa, z)
        acc = gather_stats(acc, outs, True)
        for y in range(8):
            r1[z, y] = outs[y]
            x2r[z + 1, y + 1] = outs[y].astype(BF16)
    row = mixed_row(jnp.concatenate(acc, axis=0))
    greeted(1)
    greet(2)
    stat_send(0, jnp.concatenate([row, jnp.broadcast_to(peak0, (1, 128))], axis=0))
    halo_send(1, x2r, 4, 8, range(8))

    mate = sy + 1 - 2 * lax.rem(sy, 2)
    cross_sy = lax.rem(sy + 2, 4)
    cross_mate = lax.rem(mate + 2, 4)

    def group(which, kind, src):
        buf = (wg3, wg4, gcol)[which]
        return pltpu.make_async_remote_copy(
            src_ref=buf.at[src], dst_ref=buf.at[src],
            send_sem=ws.at[which, kind], recv_sem=wr.at[which, src],
            device_id={"sy": cross_sy if kind == 1 else mate}, device_id_type=MESH,
        )

    for which in (2, 0, 1):
        group(which, 1, sy).start()
        group(which, 0, sy).start()

    def group_forward(which):
        group(which, 1, cross_sy).wait_recv()
        group(which, 2, cross_sy).start()

    def group_wait(which):
        group(which, 0, mate).wait_recv()
        group(which, 2, cross_mate).wait_recv()

    def group_done(which):
        group(which, 0, sy).wait_send()
        group(which, 1, sy).wait_send()
        group(which, 2, cross_sy).wait_send()

    fine_cells = float(4 * nz * 8 * ny * 128)
    coarse_cells = fine_cells / 8

    def fine_affine(cols, j):
        return affine(cols[0:32], cols[32:64], fine_cells, gain_col(j, 32), gain_col(2 + j, 32))

    def peak_of(high, low, aff):
        v = jnp.maximum(jnp.abs(act(high, aff)), jnp.abs(act(low, aff))).astype(BF16).astype(F32)
        return jnp.max(jnp.max(v, axis=0, keepdims=True), axis=1, keepdims=True)

    got = stat_wait(0)
    peak0 = jnp.max(jnp.max(got[:, 1:2, :], axis=0), axis=1, keepdims=True)
    cols = mixed_total(got)
    aff = fine_affine(cols, 0)
    peak1 = peak_of(cols[64:96], cols[96:128], aff)
    b1 = bound_of(1)

    def settle(v, aff, b):
        return jnp.clip(act(v, aff), -b, b).astype(BF16)

    for z in range(4):
        for y in range(8):
            x2[z + 1, y + 1] = settle(r1[z, y], aff, b1)

    def settle_halo(ph, raw, buf, zl, yl, which, aff, b):
        for i in which:
            dz, dy = DIRS[i]
            there = exists(-dz, -dy)

            @pl.when(there)
            def _():
                halo(ph, raw, zl, yl, i).wait_recv()
                for z in slots(dz, zl):
                    for y in slots(dy, yl):
                        buf[z, y] = settle(raw[z, y].astype(F32), aff, b)

            @pl.when(jnp.logical_not(there))
            def _():
                for z in slots(dz, zl):
                    for y in slots(dy, yl):
                        buf[z, y] = jnp.zeros(buf.shape[2:], buf.dtype)

    wb = wf2[...]
    acc = (zero, zero, None, None)
    settle_halo(1, x2r, x2, 4, 8, (6, 7), aff, b1)
    for z in (1, 2):
        outs = fine_conv(x2, wb, z)
        acc = gather_stats(acc, outs, False)
        for y in range(8):
            r2[z, y] = outs[y]
    settle_halo(1, x2r, x2, 4, 8, range(6), aff, b1)

    for z in (0, 3):
        outs = fine_conv(x2, wb, z)
        acc = gather_stats(acc, outs, False)
        for y in range(8):
            r2[z, y] = outs[y]

    s_r = lax.broadcasted_iota(jnp.int32, (256, 128), 0)
    s_c = lax.broadcasted_iota(jnp.int32, (256, 128), 1)
    pick = onehot(s_r == jnp.where(s_c < 64, 2 * s_c, 2 * s_c))
    highs, lows = [], []
    for zp in range(2):
        hrow, lrow = [], []
        for yp in range(4):
            m = jnp.maximum(
                jnp.maximum(r2[2 * zp, 2 * yp], r2[2 * zp, 2 * yp + 1]),
                jnp.maximum(r2[2 * zp + 1, 2 * yp], r2[2 * zp + 1, 2 * yp + 1]),
            )
            m = jnp.maximum(m, pltpu.roll(m, 127, 1))
            h = m.astype(BF16)
            hrow.append(h)
            lrow.append((m - h.astype(F32)).astype(BF16))
        highs.append(jnp.concatenate(hrow, axis=0))
        lows.append(jnp.concatenate(lrow, axis=0))
    pooled = jnp.dot(jnp.concatenate(highs, axis=1), pick, preferred_element_type=F32)
    pooled = pooled + jnp.dot(jnp.concatenate(lows, axis=1), pick, preferred_element_type=F32)
    hi = jnp.full((32, 128), -jnp.inf, F32)
    lo = jnp.full((32, 128), jnp.inf, F32)
    for yp in range(4):
        blk = pooled[32 * yp : 32 * yp + 32]
        p3[yp] = blk
        put_raw(blk, yp + 1, h3, z3s)
        hi = jnp.maximum(hi, blk)
        lo = jnp.minimum(lo, blk)
    row = mixed_row(jnp.concatenate([acc[0], acc[1], hi, lo], axis=0))
    stat_send(1, jnp.concatenate([row, row], axis=0))
    coarse_send(2, h3, z3s, z3r)
    for which in (2, 0, 1):
        group_forward(which)

    got = stat_wait(1)
    cols = mixed_total(got)
    aff2 = fine_affine(cols, 1)
    peak2 = peak_of(cols[64:96], cols[96:128], aff2)
    b2 = bound_of(2)
    for yp in range(4):
        c3[yp + 1] = settle(p3[yp], aff2, b2)
    coarse_settle(2, h3, z3s, z3r, c3, c3z, aff2, b2)

    cfirst, clast = (lane & 63) == 0, (lane & 63) == 63

    def coarse_conv(buf, zbuf, w):
        strips = []
        mids = [buf[y] for y in range(6)]
        pairs = [[], mids, []]
        half = buf.shape[1] // 2
        for y in range(6):
            own = pltpu.roll(mids[y].astype(F32), 64, 1)
            prev = zbuf[0, y].astype(F32)
            nxt = zbuf[1, y].astype(F32)
            a = jnp.where(lower, prev, own[:half])
            b = jnp.where(lower, pltpu.roll(prev, 64, 1), own[half:])
            pairs[0].append(jnp.concatenate([a, b], axis=0).astype(BF16))
            a = jnp.where(lower, own[:half], pltpu.roll(nxt, 64, 1))
            b = jnp.where(lower, own[half:], nxt)
            pairs[2].append(jnp.concatenate([a, b], axis=0).astype(BF16))
        for zt in range(3):
            for yt in range(3):
                strips.append(jnp.concatenate(pairs[zt][yt : yt + 4], axis=1))
        got = jnp.dot(w, jnp.concatenate(strips, axis=0), preferred_element_type=F32)
        outs = []
        for y in range(4):
            blk = got[:, 128 * y : 128 * y + 128]
            parts = []
            for g in range(4):
                t = blk[48 * g : 48 * g + 48]
                parts.append(combine(t[0:16], t[16:32], t[32:48], cfirst, clast))
            outs.append(jnp.concatenate(parts, axis=0))
        return outs

    group_wait(0)
    outs = coarse_conv(c3, c3z, wg3[...].reshape(192, 288))
    zero64 = jnp.zeros((64, 128), F32)
    acc = (zero64, zero64, jnp.full((64, 128), -jnp.inf, F32), jnp.full((64, 128), jnp.inf, F32))
    acc = gather_stats(acc, outs, True)
    for y in range(4):
        put_raw(outs[y], y + 1, h4, z4s)
        r4i[y] = outs[y]

    def double_rows(acc, extremes):
        t = to_rows(jnp.concatenate(acc[0:2], axis=0))
        r0 = jnp.sum(t, axis=0, keepdims=True)
        if not extremes:
            return jnp.concatenate([r0, r0], axis=0)
        t = to_rows(jnp.concatenate(acc[2:4], axis=0))
        high = jnp.max(t, axis=0, keepdims=True)
        low = jnp.min(t, axis=0, keepdims=True)
        return jnp.concatenate([r0, jnp.where(lower, high, low)], axis=0)

    stat_send(2, double_rows(acc, True))
    coarse_send(3, h4, z4s, z4r)

    outof = onehot(jnp.logical_and((ci & 31) == (ri >> 3), (ci >> 5) == (ri & 7)))
    for zp in range(2):
        parts = []
        for z in (2 * zp, 2 * zp + 1):
            parts.append(jnp.concatenate([act(r2[z, y], aff2).astype(BF16) for y in range(8)], axis=0))
        moved = jnp.dot(outof, jnp.concatenate(parts, axis=1), preferred_element_type=F32)
        for k in range(2):
            z = 2 * zp + k
            skip[z] = moved[:, 128 * k : 128 * k + 128].reshape(32, 8, 128).astype(BF16)

    group_wait(2)
    gall = gcol[...]
    got = stat_wait(2)
    cols = to_cols(jnp.sum(got[:, 0:1, :], axis=0))
    high = jnp.max(got[:, 1:2, :], axis=0)
    low = jnp.min(got[:, 1:2, :], axis=0)
    ext = to_cols(jnp.where(lower, high, low))
    aff3 = affine(cols[0:64], cols[64:128], coarse_cells, gall[:, 0].reshape(64, 128), gall[:, 1].reshape(64, 128))
    peak3 = peak_of(ext[0:64], ext[64:128], aff3)
    b3 = bound_of(3)

    peaks = jnp.where(lane == 0, peak0, jnp.where(lane == 1, peak1, jnp.where(lane == 2, peak2, peak3)))

    def cross(d, src):
        return pltpu.make_async_remote_copy(
            src_ref=am.at[smp], dst_ref=am.at[src],
            send_sem=xs.at[d], recv_sem=xr.at[src],
            device_id=other_sample(d)[1], device_id_type=MESH,
        )

    greeted(2)
    am[smp] = peaks
    for d in range(1, ns):
        cross(d, smp).start()

    for y in range(4):
        c4[y + 1] = settle(r4i[y], aff3, b3)
    coarse_settle(3, h4, z4s, z4r, c4, c4z, aff3, b3)

    group_wait(1)
    outs = coarse_conv(c4, c4z, wg4[...].reshape(192, 576))
    acc = gather_stats((zero64, zero64, None, None), outs, False)
    for g in range(4):
        for y in range(4):
            a2s[g, y] = outs[y][16 * g : 16 * g + 16]

    def swap(d, src):
        q = lax.rem(sy + d, ny)
        return pltpu.make_async_remote_copy(
            src_ref=a2s.at[q], dst_ref=a2a.at[src],
            send_sem=bs.at[d], recv_sem=br.at[src],
            device_id={"sy": q}, device_id_type=MESH,
        )

    stat_send(3, double_rows(acc, False))
    for d in range(1, ny):
        swap(d, sy).start()
    a2a[sy] = a2s[sy]

    for d in range(1, ny):
        swap(d, lax.rem(sy + d, ny)).wait_recv()
    got = stat_wait(3)
    rows8b = to_cols(jnp.sum(got[:, 0:1, :], axis=0))
    gs[...] = rows8b
    tot = gs[pl.ds(pl.multiple_of(sy * 16, 8), 16), :]
    totsq = gs[pl.ds(pl.multiple_of(64 + sy * 16, 8), 16), :]
    aff4 = affine(tot, totsq, coarse_cells, gain_col(5, 16), gain_col(7, 16))
    planes = [[], []]
    for g in range(4):
        for yp in range(2):
            u = act(a2a[g, 2 * yp], aff4)
            v = act(a2a[g, 2 * yp + 1], aff4)
            planes[0].append(jnp.where(lower, u, pltpu.roll(v, 64, 1)))
            planes[1].append(jnp.where(lower, pltpu.roll(u, 64, 1), v))
    for z in range(2):
        coarse[z] = jnp.concatenate(planes[z], axis=1).astype(BF16)

    for d in range(1, ns):
        cross(d, other_sample(d)[0]).wait_recv()
    amax[...] = jnp.max(am[...], axis=0)

    halo_done(0, x1, 4, 8)
    halo_done(1, x2r, 4, 8)
    coarse_done(2, h3, z3s, z3r)
    coarse_done(3, h4, z4s, z4r)
    for ph in range(4):
        for d in order:
            stat_copy(ph, d, me).wait_send()
    for which in range(3):
        group_done(which)
    for d in range(1, ny):
        swap(d, sy).wait_send()
    for d in range(1, ns):
        cross(d, smp).wait_send()


def solution(mesh):
    ny, nz, ns = mesh.shape["sy"], mesh.shape["sz"], mesh.shape["sample"]
    n = ny * nz
    vmem = pl.BlockSpec(memory_space=pltpu.VMEM)
    hbm = pl.BlockSpec(memory_space=pl.ANY)

    def step(volume, hist, w1, w2, w3, w4, gf, sf, gc, sc):
        dma = pltpu.SemaphoreType.DMA
        skip, coarse, amax = pl.pallas_call(
            functools.partial(body_entry, ny, nz, ns),
            out_shape=(
                pltpu.VMEM((4, 32, 8, 128), BF16),
                pltpu.VMEM((2, 16, 1024), BF16),
                pltpu.VMEM((1, 128), F32),
            ),
            in_specs=[hbm] * 10,
            out_specs=(vmem, vmem, vmem),
            scratch_shapes=[
                pltpu.VMEM((4, 16), F32),
                pltpu.VMEM((2, 32), F32),
                pltpu.VMEM((2, 32), F32),
                pltpu.VMEM((2, 16), F32),
                pltpu.VMEM((2, 16), F32),
                pltpu.VMEM((4, 32, 8, 128), BF16),
                pltpu.VMEM((9, 96, 32), BF16),
                pltpu.VMEM((9, 96, 32), BF16),
                pltpu.VMEM((9, 48, 32), BF16),
                pltpu.VMEM((9, 48, 64), BF16),
                pltpu.VMEM((96, 288), BF16),
                pltpu.VMEM((96, 288), BF16),
                pltpu.VMEM((ny, 48, 288), BF16),
                pltpu.VMEM((ny, 48, 576), BF16),
                pltpu.VMEM((6, 10, 32, 128), BF16),
                pltpu.VMEM((4, 8, 32, 128), F32),
                pltpu.VMEM((6, 10, 32, 128), BF16),
                pltpu.VMEM((6, 10, 32, 128), BF16),
                pltpu.VMEM((4, 8, 32, 128), F32),
                pltpu.VMEM((6, 32, 128), BF16),
                pltpu.VMEM((2, 6, 16, 128), BF16),
                pltpu.VMEM((2, 6, 16, 128), BF16),
                pltpu.VMEM((4, 32, 128), F32),
                pltpu.VMEM((6, 32, 128), BF16),
                pltpu.VMEM((2, 6, 16, 128), BF16),
                pltpu.VMEM((6, 64, 128), BF16),
                pltpu.VMEM((2, 6, 32, 128), BF16),
                pltpu.VMEM((2, 6, 32, 128), BF16),
                pltpu.VMEM((4, 64, 128), F32),
                pltpu.VMEM((6, 64, 128), BF16),
                pltpu.VMEM((2, 6, 32, 128), BF16),
                pltpu.VMEM((ny, 4, 16, 128), F32),
                pltpu.VMEM((ny, 4, 16, 128), F32),
                pltpu.VMEM((ny, 2, 16, 128), F32),
                pltpu.VMEM((4, n, 2, 128), F32),
                pltpu.VMEM((ns, 1, 128), F32),
                pltpu.VMEM((8, 128), F32),
                pltpu.VMEM((128, 128), F32),
                pltpu.SemaphoreType.REGULAR((3,)),
                dma((13,)),
                dma((4, 8)),
                dma((4, 8)),
                dma((4, n)),
                dma((4, n)),
                dma((3, 3)),
                dma((3, ny)),
                dma((ny,)),
                dma((ny,)),
                dma((ns,)),
                dma((ns,)),
            ],
            compiler_params=pltpu.CompilerParams(collective_id=0, has_side_effects=True),
            name="encoder",
        )(
            volume.reshape(32, 4, 8, 128), hist, w1.reshape(9, 96, 32), w2.reshape(9, 96, 32),
            w3.reshape(9, 48, 32), w4.reshape(9, 48, 64), gf, sf, gc, sc,
        )
        skip, coarse, amax = pl.pallas_call(
            emit,
            out_shape=(
                jax.ShapeDtypeStruct((32, 4, 8, 128), BF16),
                jax.ShapeDtypeStruct((16, 2, 1024), BF16),
                jax.ShapeDtypeStruct((1, 4), F32),
            ),
            in_specs=[vmem] * 3,
            out_specs=(hbm, vmem, vmem),
            scratch_shapes=[dma((4,))],
            name="emit",
        )(*(pltpu.with_memory_space_constraint(t, pltpu.VMEM) for t in (skip, coarse, amax)))
        return skip.reshape(1, 32, 4, 8, 128), coarse.reshape(1, 16, 2, 1024), amax.reshape(4)

    return jax.shard_map(
        step,
        mesh=mesh,
        in_specs=(
            P("sample", None, "sz", "sy", None), P(), P(), P(),
            P(None, "sy", None), P(None, "sy", None), P(), P(), P(None, "sy"), P(None, "sy"),
        ),
        out_specs=(P("sample", None, "sz", "sy", None), P("sample", "sy", "sz", None), P()),
        check_vma=False,
    )


def body_entry(ny, nz, ns, *refs):
    (
        vol, hist, w1, w2, w3, w4, gf, sf, gc, sc, skip, coarse, amax,
        hist_v, gf_v, sf_v, gc_v, sc_v, vin, w1v, w2v, w3v, w4v, wf1, wf2, wg3, wg4,
        x1, r1, x2r, x2, r2, h3, z3s, z3r, p3, c3, c3z, h4, z4s, z4r, r4i, c4, c4z, a2a, a2s, gcol,
        st, am, rows8, tcols,
        rounds, lsem, hs, hr, ss, sr, ws, wr, bs, br, xs, xr,
    ) = refs
    body(
        ny, nz, ns,
        vol, hist, w1, w2, w3, w4, gf, sf, gc, sc, skip, coarse, amax,
        hist_v, gf_v, sf_v, gc_v, sc_v, vin, w1v, w2v, w3v, w4v, wf1, wf2, wg3, wg4,
        x1, r1, x2r, x2, r2, h3, z3s, z3r, p3, c3, c3z, h4, z4s, z4r, r4i, c4, c4z, a2a, a2s, gcol,
        st, am, rows8,
        rounds, lsem, hs, hr, ss, sr, ws, wr, tcols, None, bs, br, xs, xr,
    )


def emit(skip_v, coarse_v, amax_v, skip, coarse, amax, sem):
    copies = [pltpu.make_async_copy(skip_v.at[z], skip.at[:, z], sem.at[z]) for z in range(4)]
    for c in copies:
        c.start()
    coarse[...] = jnp.stack([coarse_v[0].astype(F32), coarse_v[1].astype(F32)], axis=1).astype(BF16)
    amax[...] = amax_v[0:1, 0:4]
    for c in copies:
        c.wait()
```

```python
import functools

import jax
import jax.numpy as jnp
from jax import lax
from jax.experimental import pallas as pl
from jax.experimental.pallas import tpu as pltpu
from jax.sharding import PartitionSpec as P

MESH = pl.DeviceIdType.MESH
F32 = jnp.float32
BF16 = jnp.bfloat16
EPS = 1e-05
SLOPE = 0.01
DIRS = ((-1, 0), (1, 0), (-1, -1), (-1, 1), (1, -1), (1, 1), (0, -1), (0, 1))


def body(
    ny, nz, ns,
    vol, hist_h, w1, w2, w3, w4, gf_h, sf_h, gc_h, sc_h,
    skip, coarse, amax,
    hist, gf, sf, gc, sc, vin, w1v, w2v, w3v, w4v, wf1, wf2, wg3, wg4,
    x1, r1, x2r, x2, r2, h3, z3s, z3r, p3, c3, c3z, h4, z4s, z4r, r4i, c4, c4z, a2a, a2s, grow,
    st, am, rows8,
    rounds, lsem, hs, hr, ss, sr, ws, wr, gs, gr, bs, br, xs, xr,
):
    n = ny * nz
    sy = lax.axis_index("sy")
    sz = lax.axis_index("sz")
    smp = lax.axis_index("sample")
    me = sz * ny + sy

    near = [{"sz": lax.rem(sz + d, nz)} for d in sorted({1, nz - 1})]
    near += [{"sy": lax.rem(sy + d, ny)} for d in range(1, ny)]
    if ns > 1:
        sx, sv = lax.rem(smp, 4), lax.div(smp, 4)
        near += [{"sample": sv * 4 + lax.rem(sx + d, 4)} for d in (1, 3)]
        near += [{"sample": lax.rem(sv + d, 4) * 4 + sx} for d in (1, 3)]
    barrier = pltpu.get_barrier_semaphore()
    for dev in near:
        pl.semaphore_signal(barrier, inc=1, device_id=dev, device_id_type=MESH)

    def greet(r):
        for dev in near:
            pl.semaphore_signal(rounds.at[r], inc=1, device_id=dev, device_id_type=MESH)

    def greeted(r):
        pl.semaphore_wait(rounds.at[r], len(near))

    loads = [pltpu.make_async_copy(vol.at[:, z], vin.at[z], lsem.at[z]) for z in range(4)]
    small = ((hist_h, hist), (w1, w1v), (w2, w2v), (w3, w3v), (w4, w4v), (gf_h, gf), (sf_h, sf), (gc_h, gc), (sc_h, sc))
    for i, (s, d) in enumerate(small):
        loads.append(pltpu.make_async_copy(s, d, lsem.at[4 + i]))
    for i in (4, 0, 3, 1, 2, 5, 6, 7, 8, 9, 10, 11, 12):
        loads[i].start()

    def partner(d):
        p = lax.rem(me + d, n)
        return p, {"sy": lax.rem(p, ny), "sz": lax.div(p, ny)}

    order = sorted(range(1, n), key=lambda d: -min(d, n - d))
    def other_sample(d):
        q = lax.rem(smp + d, ns)
        return q, {"sample": q}

    def exists(dz, dy):
        cond = None
        for idx, cnt, d in ((sz, nz, dz), (sy, ny, dy)):
            if d == 0:
                continue
            c = (idx > 0) if d < 0 else (idx < cnt - 1)
            cond = c if cond is None else jnp.logical_and(cond, c)
        return cond

    lane = lax.broadcasted_iota(jnp.int32, (1, 128), 1)
    lower = lane < 64

    def bound_of(l):
        b = jnp.max(hist[l : l + 1, :], axis=1, keepdims=True)
        return b.astype(BF16).astype(F32)

    def src_z(dz, zl):
        return pl.ds(1, zl) if dz == 0 else (pl.ds(1, 1) if dz < 0 else pl.ds(zl, 1))

    def dst_z(dz, zl):
        return pl.ds(1, zl) if dz == 0 else (pl.ds(zl + 1, 1) if dz < 0 else pl.ds(0, 1))

    def halo(ph, buf, zl, yl, i):
        dz, dy = DIRS[i]
        return pltpu.make_async_remote_copy(
            src_ref=buf.at[src_z(dz, zl), src_z(dy, yl)],
            dst_ref=buf.at[dst_z(dz, zl), dst_z(dy, yl)],
            send_sem=hs.at[ph, i],
            recv_sem=hr.at[ph, i],
            device_id={"sy": sy + dy, "sz": sz + dz},
            device_id_type=MESH,
        )

    def halo_send(ph, buf, zl, yl, which):
        for i in which:
            @pl.when(exists(*DIRS[i]))
            def _():
                halo(ph, buf, zl, yl, i).start()

    def halo_wait(ph, buf, zl, yl, which):
        for i in which:
            @pl.when(exists(-DIRS[i][0], -DIRS[i][1]))
            def _():
                halo(ph, buf, zl, yl, i).wait_recv()

    def halo_done(ph, buf, zl, yl):
        for i in range(8):
            @pl.when(exists(*DIRS[i]))
            def _():
                halo(ph, buf, zl, yl, i).wait_send()

    def coarse_halo(ph, own, zs, zr, i):
        dz, dy = DIRS[i]
        if dz == 0:
            src, dst = own.at[src_z(dy, 4)], own.at[dst_z(dy, 4)]
        else:
            up = 1 if dz > 0 else 0
            src, dst = zs.at[up, src_z(dy, 4)], zr.at[1 - up, dst_z(dy, 4)]
        return pltpu.make_async_remote_copy(
            src_ref=src, dst_ref=dst, send_sem=hs.at[ph, i], recv_sem=hr.at[ph, i],
            device_id={"sy": sy + dy, "sz": sz + dz}, device_id_type=MESH,
        )

    def coarse_send(ph, own, zs, zr):
        for i in range(8):
            @pl.when(exists(*DIRS[i]))
            def _():
                coarse_halo(ph, own, zs, zr, i).start()

    def coarse_done(ph, own, zs, zr):
        for i in range(8):
            @pl.when(exists(*DIRS[i]))
            def _():
                coarse_halo(ph, own, zs, zr, i).wait_send()

    def put_raw(blk, y, own, zs):
        half = blk.shape[0] // 2
        top, low = blk[:half], blk[half:]
        own[y] = blk.astype(BF16)
        zs[0, y] = jnp.where(lower, top, pltpu.roll(low, 64, 1)).astype(BF16)
        zs[1, y] = jnp.where(lower, pltpu.roll(top, 64, 1), low).astype(BF16)

    def coarse_settle(ph, own, zs, zr, buf, zbuf, aff, b):
        half = buf.shape[1] // 2
        paff = tuple(jnp.where(lower, t[:half], t[half:]) for t in aff)
        for i in range(8):
            dz, dy = DIRS[i]
            there = exists(-dz, -dy)
            ys = slots(dy, 4)

            @pl.when(there)
            def _():
                coarse_halo(ph, own, zs, zr, i).wait_recv()
                for y in ys:
                    if dz == 0:
                        buf[y] = settle(own[y].astype(F32), aff, b)
                    else:
                        k = 0 if dz > 0 else 1
                        zbuf[k, y] = settle(zr[k, y].astype(F32), paff, b)

            @pl.when(jnp.logical_not(there))
            def _():
                for y in ys:
                    if dz == 0:
                        buf[y] = jnp.zeros(buf.shape[1:], BF16)
                    else:
                        k = 0 if dz > 0 else 1
                        zbuf[k, y] = jnp.zeros(zbuf.shape[2:], BF16)

    def slots(d, length):
        return range(1, length + 1) if d == 0 else ((0,) if d > 0 else (length + 1,))

    def stat_copy(ph, d, src):
        p, dev = partner(d)
        return pltpu.make_async_remote_copy(
            src_ref=st.at[ph, me],
            dst_ref=st.at[ph, src],
            send_sem=ss.at[ph, d],
            recv_sem=sr.at[ph, src],
            device_id=dev,
            device_id_type=MESH,
        )

    def stat_send(ph, rows):
        st[ph, me] = jnp.concatenate(rows + [rows[0]] * (4 - len(rows)), axis=0)
        for d in order:
            stat_copy(ph, d, me).start()

    def stat_wait(ph):
        for d in order:
            stat_copy(ph, d, partner(d)[0]).wait_recv()
        return st[ph]

    def to_rows(cols):
        return jnp.transpose(cols)

    def to_cols(row):
        return jnp.transpose(jnp.broadcast_to(row, (128, 128)))

    def affine(tot, totsq, cells, g, s):
        m = tot / cells
        var = totsq / cells - m * m
        a = lax.rsqrt(var + EPS) * g
        return a, m, s

    def act(v, aff):
        a, m, s = aff
        t = (v - m) * a + s
        return jnp.maximum(t, SLOPE * t)

    ri = lax.broadcasted_iota(jnp.int32, (256, 256), 0)
    ci = lax.broadcasted_iota(jnp.int32, (256, 256), 1)

    def onehot(cond):
        return jnp.where(cond, 1.0, 0.0).astype(BF16)

    into = onehot(jnp.logical_and((ri & 31) == (ci >> 3), (ri >> 5) == (ci & 7)))

    loads[4].wait()
    b0 = bound_of(0)
    peaks0 = []

    def take(zp):
        parts = []
        for z in zp:
            loads[z].wait()
            v = vin[z].astype(F32).reshape(256, 128)
            peaks0.append(jnp.abs(v))
            parts.append(v.astype(BF16))
        moved = jnp.dot(into, jnp.concatenate(parts, axis=1), preferred_element_type=F32)
        moved = jnp.clip(moved, -b0, b0).astype(BF16)
        for k in range(2):
            for y in range(8):
                x1[1 + zp[k], 1 + y] = moved[32 * y : 32 * y + 32, 128 * k : 128 * k + 128]

    take((0, 3))
    pl.semaphore_wait(barrier, len(near))
    greet(0)
    halo_send(0, x1, 4, 8, (0, 1))
    take((1, 2))
    halo_send(0, x1, 4, 8, (6, 7))
    peak0 = jnp.maximum(jnp.maximum(peaks0[0], peaks0[1]), jnp.maximum(peaks0[2], peaks0[3]))
    peak0 = jnp.max(jnp.max(peak0, axis=0, keepdims=True), axis=1, keepdims=True)

    for i in range(5, 13):
        loads[i].wait()
    rows8[...] = jnp.zeros_like(rows8)
    rows8[0:2, 0:32] = gf[...]
    rows8[2:4, 0:32] = sf[...]
    rows8[4:6, 0:16] = gc[...]
    rows8[6:8, 0:16] = sc[...]
    gcols = jnp.transpose(rows8[...])

    def gain_col(j, count):
        return jnp.broadcast_to(gcols[0:count, j : j + 1], (count, 128))


    def lanes_of(w):
        return jnp.concatenate([w[k] for k in range(9)], axis=1)

    wf1[...] = lanes_of(w1v)
    wf2[...] = lanes_of(w2v)
    wg3[sy] = lanes_of(w3v)
    wg4[sy] = lanes_of(w4v)
    grow[sy, 0] = rows8[4]
    grow[sy, 1] = rows8[6]

    def zero_missing(buf, zl, yl):
        for i in range(8):
            dz, dy = DIRS[i]
            @pl.when(jnp.logical_not(exists(-dz, -dy)))
            def _():
                for z in slots(dz, zl):
                    for y in slots(dy, yl):
                        buf[z, y] = jnp.zeros(buf.shape[2:], buf.dtype)

    zero_missing(x1, 4, 8)
    mate = sy + 1 - 2 * lax.rem(sy, 2)
    cross_sy = lax.rem(sy + 2, 4)
    cross_mate = lax.rem(mate + 2, 4)

    def group(which, kind, src):
        buf = (wg3, wg4, grow)[which]
        return pltpu.make_async_remote_copy(
            src_ref=buf.at[src], dst_ref=buf.at[src],
            send_sem=ws.at[which, kind], recv_sem=wr.at[which, src],
            device_id={"sy": cross_sy if kind == 1 else mate}, device_id_type=MESH,
        )

    def group_send(which):
        group(which, 1, sy).start()
        group(which, 0, sy).start()

    def group_forward(which):
        group(which, 1, cross_sy).wait_recv()
        group(which, 2, cross_sy).start()

    def group_wait(which):
        group(which, 0, mate).wait_recv()
        group(which, 2, cross_mate).wait_recv()

    def group_done(which):
        group(which, 0, sy).wait_send()
        group(which, 1, sy).wait_send()
        group(which, 2, cross_sy).wait_send()

    fine_cells = float(4 * nz * 8 * ny * 128)
    coarse_cells = fine_cells / 8

    def fine_affine(cols, j):
        return affine(cols[0:32], cols[32:64], fine_cells, gain_col(j, 32), gain_col(2 + j, 32))

    def peak_of(high, low, aff):
        v = jnp.maximum(jnp.abs(act(high, aff)), jnp.abs(act(low, aff))).astype(BF16).astype(F32)
        return jnp.max(jnp.max(v, axis=0, keepdims=True), axis=1, keepdims=True)

    greeted(0)
    greet(1)
    halo_send(0, x1, 4, 8, (2, 3, 4, 5))
    group_send(2)
    group_send(0)

    first, last = lane == 0, lane == 127

    def combine(p0, p1, p2, lo, hi):
        left = jnp.where(lo, 0.0, pltpu.roll(p0, 1, 1))
        right = jnp.where(hi, 0.0, pltpu.roll(p2, 127, 1))
        return p1 + left + right

    def fine_conv(buf, w, z):
        strips = []
        for zt in range(3):
            blocks = [buf[z + zt, y] for y in range(10)]
            for yt in range(3):
                strips.append(jnp.concatenate(blocks[yt : yt + 8], axis=1))
        got = jnp.dot(w, jnp.concatenate(strips, axis=0), preferred_element_type=F32)
        outs = []
        for y in range(8):
            blk = got[:, 128 * y : 128 * y + 128]
            outs.append(combine(blk[0:32], blk[32:64], blk[64:96], first, last))
        return outs

    zero = jnp.zeros((32, 128), F32)

    def gather_stats(acc, blocks, extremes):
        s, q, hi, lo = acc
        for b in blocks:
            s = s + b
            q = q + b * b
            if extremes:
                hi = jnp.maximum(hi, b)
                lo = jnp.minimum(lo, b)
        return s, q, hi, lo

    def sum_row(cols):
        cols = jnp.concatenate(cols, axis=0)
        if cols.shape[0] < 128:
            cols = jnp.concatenate([cols, cols], axis=0)
        return jnp.sum(to_rows(cols), axis=0, keepdims=True)

    def mixed_row(cols):
        t = to_rows(cols)
        total = jnp.sum(t, axis=0, keepdims=True)
        high = jnp.max(t, axis=0, keepdims=True)
        low = jnp.min(t, axis=0, keepdims=True)
        return jnp.where(lane < 64, total, jnp.where(lane < 96, high, low))

    def mixed_total(got):
        total = jnp.sum(got[:, 0:1, :], axis=0)
        high = jnp.max(got[:, 0:1, :], axis=0)
        low = jnp.min(got[:, 0:1, :], axis=0)
        return to_cols(jnp.where(lane < 64, total, jnp.where(lane < 96, high, low)))

    wa = wf1[...]
    acc = (zero, zero, jnp.full((32, 128), -jnp.inf, F32), jnp.full((32, 128), jnp.inf, F32))
    halo_wait(0, x1, 4, 8, (6, 7))
    for z in (1, 2):
        outs = fine_conv(x1, wa, z)
        acc = gather_stats(acc, outs, True)
        for y in range(8):
            r1[z, y] = outs[y]
        x2r[z + 1, 1] = outs[0].astype(BF16)
        x2r[z + 1, 8] = outs[7].astype(BF16)
    halo_wait(0, x1, 4, 8, range(6))
    for z in (0, 3):
        outs = fine_conv(x1, wa, z)
        acc = gather_stats(acc, outs, True)
        for y in range(8):
            r1[z, y] = outs[y]
            x2r[z + 1, y + 1] = outs[y].astype(BF16)
    row = mixed_row(jnp.concatenate(acc, axis=0))
    greeted(1)
    greet(2)
    stat_send(0, [row, jnp.broadcast_to(peak0, (1, 128))])
    halo_send(1, x2r, 4, 8, range(8))
    group_forward(2)
    group_forward(0)

    got = stat_wait(0)
    peak0 = jnp.max(jnp.max(got[:, 1:2, :], axis=0), axis=1, keepdims=True)
    cols = mixed_total(got)
    aff = fine_affine(cols, 0)
    peak1 = peak_of(cols[64:96], cols[96:128], aff)
    b1 = bound_of(1)

    def settle(v, aff, b):
        return jnp.clip(act(v, aff), -b, b).astype(BF16)

    for z in range(4):
        for y in range(8):
            x2[z + 1, y + 1] = settle(r1[z, y], aff, b1)

    def settle_halo(ph, raw, buf, zl, yl, which, aff, b):
        for i in which:
            dz, dy = DIRS[i]
            there = exists(-dz, -dy)

            @pl.when(there)
            def _():
                halo(ph, raw, zl, yl, i).wait_recv()
                for z in slots(dz, zl):
                    for y in slots(dy, yl):
                        buf[z, y] = settle(raw[z, y].astype(F32), aff, b)

            @pl.when(jnp.logical_not(there))
            def _():
                for z in slots(dz, zl):
                    for y in slots(dy, yl):
                        buf[z, y] = jnp.zeros(buf.shape[2:], buf.dtype)

    wb = wf2[...]
    acc = (zero, zero, None, None)
    settle_halo(1, x2r, x2, 4, 8, (6, 7), aff, b1)
    for z in (1, 2):
        outs = fine_conv(x2, wb, z)
        acc = gather_stats(acc, outs, False)
        for y in range(8):
            r2[z, y] = outs[y]
    settle_halo(1, x2r, x2, 4, 8, range(6), aff, b1)

    for z in (0, 3):
        outs = fine_conv(x2, wb, z)
        acc = gather_stats(acc, outs, False)
        for y in range(8):
            r2[z, y] = outs[y]

    stat_send(1, [sum_row(acc[0:2])])
    s_r = lax.broadcasted_iota(jnp.int32, (256, 128), 0)
    s_c = lax.broadcasted_iota(jnp.int32, (256, 128), 1)
    pick = onehot(s_r == jnp.where(s_c < 64, 2 * s_c, 2 * s_c))
    highs, lows = [], []
    for zp in range(2):
        hrow, lrow = [], []
        for yp in range(4):
            m = jnp.maximum(
                jnp.maximum(r2[2 * zp, 2 * yp], r2[2 * zp, 2 * yp + 1]),
                jnp.maximum(r2[2 * zp + 1, 2 * yp], r2[2 * zp + 1, 2 * yp + 1]),
            )
            m = jnp.maximum(m, pltpu.roll(m, 127, 1))
            h = m.astype(BF16)
            hrow.append(h)
            lrow.append((m - h.astype(F32)).astype(BF16))
        highs.append(jnp.concatenate(hrow, axis=0))
        lows.append(jnp.concatenate(lrow, axis=0))
    pooled = jnp.dot(jnp.concatenate(highs, axis=1), pick, preferred_element_type=F32)
    pooled = pooled + jnp.dot(jnp.concatenate(lows, axis=1), pick, preferred_element_type=F32)
    hi = jnp.full((32, 128), -jnp.inf, F32)
    lo = jnp.full((32, 128), jnp.inf, F32)
    for yp in range(4):
        blk = pooled[32 * yp : 32 * yp + 32]
        p3[yp] = blk
        put_raw(blk, yp + 1, h3, z3s)
        hi = jnp.maximum(hi, blk)
        lo = jnp.minimum(lo, blk)
    coarse_send(2, h3, z3s, z3r)
    group_send(1)

    got = stat_wait(1)
    cols = to_cols(jnp.sum(got[:, 0:1, :], axis=0))
    aff2 = fine_affine(cols, 1)
    b2 = bound_of(2)
    for yp in range(4):
        c3[yp + 1] = settle(p3[yp], aff2, b2)
    coarse_settle(2, h3, z3s, z3r, c3, c3z, aff2, b2)

    cfirst, clast = (lane & 63) == 0, (lane & 63) == 63

    def coarse_conv(buf, zbuf, w):
        strips = []
        mids = [buf[y] for y in range(6)]
        pairs = [[], mids, []]
        half = buf.shape[1] // 2
        for y in range(6):
            own = pltpu.roll(mids[y].astype(F32), 64, 1)
            prev = zbuf[0, y].astype(F32)
            nxt = zbuf[1, y].astype(F32)
            a = jnp.where(lower, prev, own[:half])
            b = jnp.where(lower, pltpu.roll(prev, 64, 1), own[half:])
            pairs[0].append(jnp.concatenate([a, b], axis=0).astype(BF16))
            a = jnp.where(lower, own[:half], pltpu.roll(nxt, 64, 1))
            b = jnp.where(lower, own[half:], nxt)
            pairs[2].append(jnp.concatenate([a, b], axis=0).astype(BF16))
        for zt in range(3):
            for yt in range(3):
                strips.append(jnp.concatenate(pairs[zt][yt : yt + 4], axis=1))
        got = jnp.dot(w, jnp.concatenate(strips, axis=0), preferred_element_type=F32)
        outs = []
        for y in range(4):
            blk = got[:, 128 * y : 128 * y + 128]
            parts = []
            for g in range(4):
                t = blk[48 * g : 48 * g + 48]
                parts.append(combine(t[0:16], t[16:32], t[32:48], cfirst, clast))
            outs.append(jnp.concatenate(parts, axis=0))
        return outs

    group_wait(0)
    outs = coarse_conv(c3, c3z, wg3[...].reshape(192, 288))
    zero64 = jnp.zeros((64, 128), F32)
    acc = (zero64, zero64, jnp.full((64, 128), -jnp.inf, F32), jnp.full((64, 128), jnp.inf, F32))
    acc = gather_stats(acc, outs, True)

    def extreme_row(cols, split):
        t = to_rows(jnp.concatenate(cols, axis=0))
        return jnp.where(split, jnp.max(t, axis=0, keepdims=True), jnp.min(t, axis=0, keepdims=True))

    stat_send(2, [sum_row(acc[0:2]), extreme_row(acc[2:4], lower), extreme_row((hi, hi, lo, lo), lower)])
    for y in range(4):
        put_raw(outs[y], y + 1, h4, z4s)
        r4i[y] = outs[y]
    coarse_send(3, h4, z4s, z4r)
    group_forward(1)

    outof = onehot(jnp.logical_and((ci & 31) == (ri >> 3), (ci >> 5) == (ri & 7)))
    for zp in range(2):
        parts = []
        for z in (2 * zp, 2 * zp + 1):
            parts.append(jnp.concatenate([act(r2[z, y], aff2).astype(BF16) for y in range(8)], axis=0))
        moved = jnp.dot(outof, jnp.concatenate(parts, axis=1), preferred_element_type=F32)
        for k in range(2):
            z = 2 * zp + k
            skip[z] = moved[:, 128 * k : 128 * k + 128].reshape(32, 8, 128).astype(BF16)

    group_wait(2)
    gall = jnp.transpose(grow[...].reshape(2 * ny, 128))

    def gathered(k):
        parts = [gall[0:16, 2 * g + k : 2 * g + k + 1] for g in range(ny)]
        return jnp.broadcast_to(jnp.concatenate(parts, axis=0), (64, 128))

    got = stat_wait(2)
    cols = to_cols(jnp.sum(got[:, 0:1, :], axis=0))
    high = jnp.max(got[:, 1:3, :], axis=0)
    low = jnp.min(got[:, 1:3, :], axis=0)
    ext = jnp.where(lower, high, low)
    pext, ext = to_cols(ext[1:2]), to_cols(ext[0:1])
    peak2 = peak_of(pext[0:32], pext[64:96], aff2)
    aff3 = affine(cols[0:64], cols[64:128], coarse_cells, gathered(0), gathered(1))
    peak3 = peak_of(ext[0:64], ext[64:128], aff3)
    b3 = bound_of(3)

    peaks = jnp.where(lane == 0, peak0, jnp.where(lane == 1, peak1, jnp.where(lane == 2, peak2, peak3)))

    def cross(d, src):
        return pltpu.make_async_remote_copy(
            src_ref=am.at[smp], dst_ref=am.at[src],
            send_sem=xs.at[d], recv_sem=xr.at[src],
            device_id=other_sample(d)[1], device_id_type=MESH,
        )

    for y in range(4):
        c4[y + 1] = settle(r4i[y], aff3, b3)
    coarse_settle(3, h4, z4s, z4r, c4, c4z, aff3, b3)
    greeted(2)
    am[smp] = peaks
    for d in range(1, ns):
        cross(d, smp).start()


    group_wait(1)
    outs = coarse_conv(c4, c4z, wg4[...].reshape(192, 576))
    acc = gather_stats((zero64, zero64, None, None), outs, False)
    def swap(d, src):
        q = lax.rem(sy + d, ny)
        return pltpu.make_async_remote_copy(
            src_ref=a2s.at[q], dst_ref=a2a.at[src],
            send_sem=bs.at[d], recv_sem=br.at[src],
            device_id={"sy": q}, device_id_type=MESH,
        )

    stat_send(3, [sum_row(acc[0:2])])
    for g in range(4):
        for y in range(4):
            a2s[g, y] = outs[y][16 * g : 16 * g + 16]

    for d in range(1, ny):
        swap(d, sy).start()
    a2a[sy] = a2s[sy]

    halo_done(0, x1, 4, 8)
    halo_done(1, x2r, 4, 8)
    coarse_done(2, h3, z3s, z3r)
    coarse_done(3, h4, z4s, z4r)
    for ph in range(3):
        for d in order:
            stat_copy(ph, d, me).wait_send()
    for which in range(3):
        group_done(which)
    for d in range(1, ny):
        swap(d, lax.rem(sy + d, ny)).wait_recv()
    got = stat_wait(3)
    rows8b = to_cols(jnp.sum(got[:, 0:1, :], axis=0))
    gs[...] = rows8b
    tot = gs[pl.ds(pl.multiple_of(sy * 16, 8), 16), :]
    totsq = gs[pl.ds(pl.multiple_of(64 + sy * 16, 8), 16), :]
    aff4 = affine(tot, totsq, coarse_cells, gain_col(5, 16), gain_col(7, 16))
    planes = [[], []]
    for g in range(4):
        for yp in range(2):
            u = act(a2a[g, 2 * yp], aff4)
            v = act(a2a[g, 2 * yp + 1], aff4)
            planes[0].append(jnp.where(lower, u, pltpu.roll(v, 64, 1)))
            planes[1].append(jnp.where(lower, pltpu.roll(u, 64, 1), v))
    both = [jnp.concatenate(planes[z], axis=1) for z in range(2)]
    coarse[...] = jnp.stack(both, axis=1).astype(BF16)

    for d in range(1, ns):
        cross(d, other_sample(d)[0]).wait_recv()
    amax[...] = jnp.max(am[...], axis=0)[:, 0:4]

    for d in order:
        stat_copy(3, d, me).wait_send()
    for d in range(1, ny):
        swap(d, sy).wait_send()
    for d in range(1, ns):
        cross(d, smp).wait_send()


def solution(mesh):
    ny, nz, ns = mesh.shape["sy"], mesh.shape["sz"], mesh.shape["sample"]
    n = ny * nz
    vmem = pl.BlockSpec(memory_space=pltpu.VMEM)
    hbm = pl.BlockSpec(memory_space=pl.ANY)

    def step(volume, hist, w1, w2, w3, w4, gf, sf, gc, sc):
        dma = pltpu.SemaphoreType.DMA
        skip, coarse, amax = pl.pallas_call(
            functools.partial(body_entry, ny, nz, ns),
            out_shape=(
                pltpu.VMEM((4, 32, 8, 128), BF16),
                pltpu.VMEM((16, 2, 1024), BF16),
                pltpu.VMEM((1, 4), F32),
            ),
            in_specs=[hbm] * 10,
            out_specs=(vmem, vmem, vmem),
            scratch_shapes=[
                pltpu.VMEM((4, 16), F32),
                pltpu.VMEM((2, 32), F32),
                pltpu.VMEM((2, 32), F32),
                pltpu.VMEM((2, 16), F32),
                pltpu.VMEM((2, 16), F32),
                pltpu.VMEM((4, 32, 8, 128), BF16),
                pltpu.VMEM((9, 96, 32), BF16),
                pltpu.VMEM((9, 96, 32), BF16),
                pltpu.VMEM((9, 48, 32), BF16),
                pltpu.VMEM((9, 48, 64), BF16),
                pltpu.VMEM((96, 288), BF16),
                pltpu.VMEM((96, 288), BF16),
                pltpu.VMEM((ny, 48, 288), BF16),
                pltpu.VMEM((ny, 48, 576), BF16),
                pltpu.VMEM((6, 10, 32, 128), BF16),
                pltpu.VMEM((4, 8, 32, 128), F32),
                pltpu.VMEM((6, 10, 32, 128), BF16),
                pltpu.VMEM((6, 10, 32, 128), BF16),
                pltpu.VMEM((4, 8, 32, 128), F32),
                pltpu.VMEM((6, 32, 128), BF16),
                pltpu.VMEM((2, 6, 16, 128), BF16),
                pltpu.VMEM((2, 6, 16, 128), BF16),
                pltpu.VMEM((4, 32, 128), F32),
                pltpu.VMEM((6, 32, 128), BF16),
                pltpu.VMEM((2, 6, 16, 128), BF16),
                pltpu.VMEM((6, 64, 128), BF16),
                pltpu.VMEM((2, 6, 32, 128), BF16),
                pltpu.VMEM((2, 6, 32, 128), BF16),
                pltpu.VMEM((4, 64, 128), F32),
                pltpu.VMEM((6, 64, 128), BF16),
                pltpu.VMEM((2, 6, 32, 128), BF16),
                pltpu.VMEM((ny, 4, 16, 128), F32),
                pltpu.VMEM((ny, 4, 16, 128), F32),
                pltpu.VMEM((ny, 2, 128), F32),
                pltpu.VMEM((4, n, 4, 128), F32),
                pltpu.VMEM((ns, 1, 128), F32),
                pltpu.VMEM((8, 128), F32),
                pltpu.VMEM((128, 128), F32),
                pltpu.SemaphoreType.REGULAR((3,)),
                dma((13,)),
                dma((4, 8)),
                dma((4, 8)),
                dma((4, n)),
                dma((4, n)),
                dma((3, 3)),
                dma((3, ny)),
                dma((ny,)),
                dma((ny,)),
                dma((ns,)),
                dma((ns,)),
            ],
            compiler_params=pltpu.CompilerParams(collective_id=0, has_side_effects=True),
            name="encoder",
        )(
            volume.reshape(32, 4, 8, 128), hist, w1.reshape(9, 96, 32), w2.reshape(9, 96, 32),
            w3.reshape(9, 48, 32), w4.reshape(9, 48, 64), gf, sf, gc, sc,
        )
        skip, coarse, amax = pl.pallas_call(
            emit,
            out_shape=(
                jax.ShapeDtypeStruct((32, 4, 8, 128), BF16),
                jax.ShapeDtypeStruct((16, 2, 1024), BF16),
                jax.ShapeDtypeStruct((1, 4), F32),
            ),
            in_specs=[vmem] * 3,
            out_specs=(hbm, hbm, hbm),
            scratch_shapes=[dma((6,))],
            name="emit",
        )(*(pltpu.with_memory_space_constraint(t, pltpu.VMEM) for t in (skip, coarse, amax)))
        return skip.reshape(1, 32, 4, 8, 128), coarse.reshape(1, 16, 2, 1024), amax.reshape(4)

    return jax.shard_map(
        step,
        mesh=mesh,
        in_specs=(
            P("sample", None, "sz", "sy", None), P(), P(), P(),
            P(None, "sy", None), P(None, "sy", None), P(), P(), P(None, "sy"), P(None, "sy"),
        ),
        out_specs=(P("sample", None, "sz", "sy", None), P("sample", "sy", "sz", None), P()),
        check_vma=False,
    )


def body_entry(ny, nz, ns, *refs):
    (
        vol, hist, w1, w2, w3, w4, gf, sf, gc, sc, skip, coarse, amax,
        hist_v, gf_v, sf_v, gc_v, sc_v, vin, w1v, w2v, w3v, w4v, wf1, wf2, wg3, wg4,
        x1, r1, x2r, x2, r2, h3, z3s, z3r, p3, c3, c3z, h4, z4s, z4r, r4i, c4, c4z, a2a, a2s, grow,
        st, am, rows8, tcols,
        rounds, lsem, hs, hr, ss, sr, ws, wr, bs, br, xs, xr,
    ) = refs
    body(
        ny, nz, ns,
        vol, hist, w1, w2, w3, w4, gf, sf, gc, sc, skip, coarse, amax,
        hist_v, gf_v, sf_v, gc_v, sc_v, vin, w1v, w2v, w3v, w4v, wf1, wf2, wg3, wg4,
        x1, r1, x2r, x2, r2, h3, z3s, z3r, p3, c3, c3z, h4, z4s, z4r, r4i, c4, c4z, a2a, a2s, grow,
        st, am, rows8,
        rounds, lsem, hs, hr, ss, sr, ws, wr, tcols, None, bs, br, xs, xr,
    )


def emit(skip_v, coarse_v, amax_v, skip, coarse, amax, sem):
    copies = [pltpu.make_async_copy(skip_v.at[z], skip.at[:, z], sem.at[z]) for z in range(4)]
    copies.append(pltpu.make_async_copy(coarse_v, coarse, sem.at[4]))
    copies.append(pltpu.make_async_copy(amax_v, amax, sem.at[5]))
    for c in copies:
        c.start()
    for c in copies:
        c.wait()
```

```python
import functools

import jax
import jax.numpy as jnp
from jax import lax
from jax.experimental import pallas as pl
from jax.experimental.pallas import tpu as pltpu
from jax.sharding import PartitionSpec as P

MESH = pl.DeviceIdType.MESH
F32 = jnp.float32
BF16 = jnp.bfloat16
EPS = 1e-05
SLOPE = 0.01
PIECES = (
    ((-1, 0, 1, 6), (1, 0, 1, 6), (-1, 0, 7, 2), (1, 0, 7, 2), (-1, -1, 1, 1), (-1, 1, 8, 1), (1, -1, 1, 1), (1, 1, 8, 1),
     (0, -1, 1, 1), (0, 1, 8, 1)),
    ((-1, 0, 2, 4), (1, 0, 2, 4), (-1, 0, 6, 3), (1, 0, 6, 3), (-1, -1, 1, 1), (-1, 1, 8, 1), (1, -1, 1, 1), (1, 1, 8, 1),
     (0, -1, 1, 1), (0, 1, 8, 1), (-1, 0, 1, 1), (1, 0, 1, 1)),
)
DIRS = ((-1, 0), (1, 0), (-1, -1), (-1, 1), (1, -1), (1, 1), (0, -1), (0, 1))


def body(
    ny, nz, ns,
    vol, hist_h, w1, w2, w3, w4, gf_h, sf_h, gc_h, sc_h,
    skip, coarse, amax,
    hist, gf, sf, gc, sc, vin, w1v, w2v, w3v, w4v, wf1, wf2, wg3, wg4,
    x1, r1, x2r, x2, r2, h3, z3s, z3r, p3, c3, c3z, h4, z4s, z4r, r4i, c4, c4z, a2a, a2s, grow,
    st, am, rows8,
    rounds, lsem, hs, hr, ss, sr, ws, wr, gs, bs, xs,
):
    n = ny * nz
    sy = lax.axis_index("sy")
    sz = lax.axis_index("sz")
    smp = lax.axis_index("sample")
    me = sz * ny + sy

    near = [{"sz": lax.rem(sz + d, nz)} for d in sorted({1, nz - 1})]
    near += [{"sy": lax.rem(sy + d, ny)} for d in range(1, ny)]
    if ns > 1:
        sx, sv = lax.rem(smp, 4), lax.div(smp, 4)
        near += [{"sample": sv * 4 + lax.rem(sx + d, 4)} for d in (1, 3)]
        near += [{"sample": lax.rem(sv + d, 4) * 4 + sx} for d in (1, 3)]
    barrier = pltpu.get_barrier_semaphore()
    for dev in near:
        pl.semaphore_signal(barrier, inc=1, device_id=dev, device_id_type=MESH)

    def greet(r):
        for dev in near:
            pl.semaphore_signal(rounds.at[r], inc=1, device_id=dev, device_id_type=MESH)

    def greeted(r):
        pl.semaphore_wait(rounds.at[r], len(near))

    loads = [pltpu.make_async_copy(vol.at[:, z], vin.at[z], lsem.at[z]) for z in range(4)]
    small = ((hist_h, hist), (w1, w1v), (w2, w2v), (w3, w3v), (w4, w4v), (gf_h, gf), (sf_h, sf), (gc_h, gc), (sc_h, sc))
    for i, (s, d) in enumerate(small):
        loads.append(pltpu.make_async_copy(s, d, lsem.at[4 + i]))
    for i in (4, 0, 3, 1, 2, 5, 6, 7, 8, 9, 10, 11, 12):
        loads[i].start()

    def partner(d):
        p = lax.rem(me + d, n)
        return p, {"sy": lax.rem(p, ny), "sz": lax.div(p, ny)}

    order = sorted(range(1, n), key=lambda d: -min(d, n - d))
    def other_sample(d):
        q = lax.rem(smp + d, ns)
        return q, {"sample": q}

    def exists(dz, dy):
        cond = None
        for idx, cnt, d in ((sz, nz, dz), (sy, ny, dy)):
            if d == 0:
                continue
            c = (idx > 0) if d < 0 else (idx < cnt - 1)
            cond = c if cond is None else jnp.logical_and(cond, c)
        return cond

    lane = lax.broadcasted_iota(jnp.int32, (1, 128), 1)
    lower = lane < 64

    def bound_of(l):
        b = jnp.max(hist[l : l + 1, :], axis=1, keepdims=True)
        return b.astype(BF16).astype(F32)

    def src_z(dz, zl):
        return pl.ds(1, zl) if dz == 0 else (pl.ds(1, 1) if dz < 0 else pl.ds(zl, 1))

    def dst_z(dz, zl):
        return pl.ds(1, zl) if dz == 0 else (pl.ds(zl + 1, 1) if dz < 0 else pl.ds(0, 1))

    def halo(ph, buf, i):
        dz, dy, row, count = PIECES[ph][i]
        return pltpu.make_async_remote_copy(
            src_ref=buf.at[src_z(dz, 4), pl.ds(row, count)],
            dst_ref=buf.at[dst_z(dz, 4), pl.ds(row - 8 * dy, count)],
            send_sem=hs.at[ph % 2, i],
            recv_sem=hr.at[ph % 2, i],
            device_id={"sy": sy + dy, "sz": sz + dz},
            device_id_type=MESH,
        )

    def halo_send(ph, buf, which):
        for i in which:
            @pl.when(exists(*PIECES[ph][i][:2]))
            def _():
                halo(ph, buf, i).start()

    def halo_wait(ph, buf, which):
        for i in which:
            @pl.when(exists(-PIECES[ph][i][0], -PIECES[ph][i][1]))
            def _():
                halo(ph, buf, i).wait_recv()

    def halo_done(ph, buf):
        for i in range(len(PIECES[ph])):
            @pl.when(exists(*PIECES[ph][i][:2]))
            def _():
                halo(ph, buf, i).wait_send()

    def halo_slots(ph, i):
        dz, dy, row, count = PIECES[ph][i]
        return slots(dz, 4), range(row - 8 * dy, row - 8 * dy + count)

    def coarse_halo(ph, own, zs, zr, i):
        dz, dy = DIRS[i]
        if dz == 0:
            src, dst = own.at[src_z(dy, 4)], own.at[dst_z(dy, 4)]
        else:
            up = 1 if dz > 0 else 0
            src, dst = zs.at[up, src_z(dy, 4)], zr.at[1 - up, dst_z(dy, 4)]
        return pltpu.make_async_remote_copy(
            src_ref=src, dst_ref=dst, send_sem=hs.at[ph % 2, i], recv_sem=hr.at[ph % 2, i],
            device_id={"sy": sy + dy, "sz": sz + dz}, device_id_type=MESH,
        )

    def coarse_send(ph, own, zs, zr):
        for i in range(8):
            @pl.when(exists(*DIRS[i]))
            def _():
                coarse_halo(ph, own, zs, zr, i).start()

    def coarse_done(ph, own, zs, zr):
        for i in range(8):
            @pl.when(exists(*DIRS[i]))
            def _():
                coarse_halo(ph, own, zs, zr, i).wait_send()

    def put_raw(blk, y, own, zs):
        half = blk.shape[0] // 2
        top, low = blk[:half], blk[half:]
        own[y] = blk.astype(BF16)
        zs[0, y] = jnp.where(lower, top, pltpu.roll(low, 64, 1)).astype(BF16)
        zs[1, y] = jnp.where(lower, pltpu.roll(top, 64, 1), low).astype(BF16)

    def coarse_settle(ph, own, zs, zr, buf, zbuf, aff, b):
        half = buf.shape[1] // 2
        paff = tuple(jnp.where(lower, t[:half], t[half:]) for t in aff)
        for i in range(8):
            dz, dy = DIRS[i]
            there = exists(-dz, -dy)
            ys = slots(dy, 4)

            @pl.when(there)
            def _():
                coarse_halo(ph, own, zs, zr, i).wait_recv()
                for y in ys:
                    if dz == 0:
                        buf[y] = settle(own[y].astype(F32), aff, b)
                    else:
                        k = 0 if dz > 0 else 1
                        zbuf[k, y] = settle(zr[k, y].astype(F32), paff, b)

            @pl.when(jnp.logical_not(there))
            def _():
                for y in ys:
                    if dz == 0:
                        buf[y] = jnp.zeros(buf.shape[1:], BF16)
                    else:
                        k = 0 if dz > 0 else 1
                        zbuf[k, y] = jnp.zeros(zbuf.shape[2:], BF16)

    def slots(d, length):
        return range(1, length + 1) if d == 0 else ((0,) if d > 0 else (length + 1,))

    def stat_copy(ph, src, dst, dev):
        return pltpu.make_async_remote_copy(
            src_ref=st.at[ph, src], dst_ref=st.at[ph, dst],
            send_sem=ss.at[ph], recv_sem=sr.at[ph],
            device_id=dev, device_id_type=MESH,
        )

    def stat_all(ph):
        rest = pl.ds(0, n - 1)
        return stat_copy(ph, rest, rest, partner(1)[1])

    def stat_send(ph, rows):
        st[ph, me] = jnp.concatenate(rows + [rows[0]] * (4 - len(rows)), axis=0)
        for d in order:
            stat_copy(ph, me, me, partner(d)[1]).start()

    def stat_wait(ph):
        stat_all(ph).wait_recv()
        return st[ph]

    def to_rows(cols):
        return jnp.transpose(cols)

    def to_cols(row):
        return jnp.transpose(jnp.broadcast_to(row, (128, 128)))

    def affine(tot, totsq, cells, g, s):
        m = tot / cells
        var = totsq / cells - m * m
        a = lax.rsqrt(var + EPS) * g
        return a, m, s

    def act(v, aff):
        a, m, s = aff
        t = (v - m) * a + s
        return jnp.maximum(t, SLOPE * t)

    ri = lax.broadcasted_iota(jnp.int32, (256, 256), 0)
    ci = lax.broadcasted_iota(jnp.int32, (256, 256), 1)

    def onehot(cond):
        return jnp.where(cond, 1.0, 0.0).astype(BF16)

    into = onehot(jnp.logical_and((ri & 31) == (ci >> 3), (ri >> 5) == (ci & 7)))

    loads[4].wait()
    b0 = bound_of(0)
    peaks0 = []

    def take(zp):
        parts = []
        for z in zp:
            loads[z].wait()
            v = vin[z].astype(F32).reshape(256, 128)
            peaks0.append(jnp.abs(v))
            parts.append(v.astype(BF16))
        moved = jnp.dot(into, jnp.concatenate(parts, axis=1), preferred_element_type=F32)
        moved = jnp.clip(moved, -b0, b0).astype(BF16)
        for k in range(2):
            for y in range(8):
                x1[1 + zp[k], 1 + y] = moved[32 * y : 32 * y + 32, 128 * k : 128 * k + 128]

    take((0, 3))
    pl.semaphore_wait(barrier, len(near))
    greet(0)
    halo_send(0, x1, (0, 1))
    take((1, 2))
    halo_send(0, x1, (8, 9, 2, 3))
    peak0 = jnp.maximum(jnp.maximum(peaks0[0], peaks0[1]), jnp.maximum(peaks0[2], peaks0[3]))
    peak0 = jnp.max(jnp.max(peak0, axis=0, keepdims=True), axis=1, keepdims=True)

    for i in range(5, 13):
        loads[i].wait()
    rows8[...] = jnp.zeros_like(rows8)
    rows8[0:2, 0:32] = gf[...]
    rows8[2:4, 0:32] = sf[...]
    rows8[4:6, 0:16] = gc[...]
    rows8[6:8, 0:16] = sc[...]
    gcols = jnp.transpose(rows8[...])

    def gain_col(j, count):
        return jnp.broadcast_to(gcols[0:count, j : j + 1], (count, 128))


    def lanes_of(w):
        return jnp.concatenate([w[k] for k in range(9)], axis=1)

    wf1[...] = lanes_of(w1v)
    wf2[...] = lanes_of(w2v)
    wg3[sy] = lanes_of(w3v)
    wg4[sy] = lanes_of(w4v)
    grow[sy, 0] = rows8[4]
    grow[sy, 1] = rows8[6]

    for i in range(len(PIECES[0])):
        @pl.when(jnp.logical_not(exists(-PIECES[0][i][0], -PIECES[0][i][1])))
        def _():
            for z in halo_slots(0, i)[0]:
                for y in halo_slots(0, i)[1]:
                    x1[z, y] = jnp.zeros((32, 128), BF16)

    mate = sy + 1 - 2 * lax.rem(sy, 2)
    cross_sy = lax.rem(sy + 2, 4)
    cross_mate = lax.rem(mate + 2, 4)

    def group(which, kind, src):
        buf = (wg3, wg4, grow)[which]
        return pltpu.make_async_remote_copy(
            src_ref=buf.at[src], dst_ref=buf.at[src],
            send_sem=ws.at[which, kind], recv_sem=wr.at[which, src],
            device_id={"sy": cross_sy if kind == 1 else mate}, device_id_type=MESH,
        )

    def group_send(which):
        group(which, 1, sy).start()
        group(which, 0, sy).start()

    def group_forward(which):
        group(which, 1, cross_sy).wait_recv()
        group(which, 2, cross_sy).start()

    def group_wait(which):
        group(which, 0, mate).wait_recv()
        group(which, 2, cross_mate).wait_recv()

    def group_done(which):
        group(which, 0, sy).wait_send()
        group(which, 1, sy).wait_send()
        group(which, 2, cross_sy).wait_send()

    fine_cells = float(4 * nz * 8 * ny * 128)
    coarse_cells = fine_cells / 8

    def fine_affine(cols, j):
        return affine(cols[0:32], cols[32:64], fine_cells, gain_col(j, 32), gain_col(2 + j, 32))

    def peak_of(high, low, aff):
        v = jnp.maximum(jnp.abs(act(high, aff)), jnp.abs(act(low, aff))).astype(BF16).astype(F32)
        return jnp.max(jnp.max(v, axis=0, keepdims=True), axis=1, keepdims=True)

    greeted(0)
    greet(1)
    halo_send(0, x1, (4, 5, 6, 7))

    first, last = lane == 0, lane == 127

    def combine(p0, p1, p2, lo, hi):
        left = jnp.where(lo, 0.0, pltpu.roll(p0, 1, 1))
        right = jnp.where(hi, 0.0, pltpu.roll(p2, 127, 1))
        return p1 + left + right

    def fine_conv(buf, w, z, rows=range(8)):
        strips = []
        for zt in range(3):
            for yt in range(3):
                strips.append(jnp.concatenate([buf[z + zt, y + yt] for y in rows], axis=1))
        got = jnp.dot(w, jnp.concatenate(strips, axis=0), preferred_element_type=F32)
        outs = []
        for k in range(len(rows)):
            blk = got[:, 128 * k : 128 * k + 128]
            outs.append(combine(blk[0:32], blk[32:64], blk[64:96], first, last))
        return outs

    zero = jnp.zeros((32, 128), F32)

    def gather_stats(acc, blocks, extremes):
        s, q, hi, lo = acc
        for b in blocks:
            s = s + b
            q = q + b * b
            if extremes:
                hi = jnp.maximum(hi, b)
                lo = jnp.minimum(lo, b)
        return s, q, hi, lo

    def sum_row(cols):
        cols = jnp.concatenate(cols, axis=0)
        if cols.shape[0] < 128:
            cols = jnp.concatenate([cols, cols], axis=0)
        return jnp.sum(to_rows(cols), axis=0, keepdims=True)

    def mixed_row(cols):
        t = to_rows(cols)
        total = jnp.sum(t, axis=0, keepdims=True)
        high = jnp.max(t, axis=0, keepdims=True)
        low = jnp.min(t, axis=0, keepdims=True)
        return jnp.where(lane < 64, total, jnp.where(lane < 96, high, low))

    def mixed_total(got):
        total = jnp.sum(got[:, 0:1, :], axis=0)
        high = jnp.max(got[:, 0:1, :], axis=0)
        low = jnp.min(got[:, 0:1, :], axis=0)
        return to_cols(jnp.where(lane < 64, total, jnp.where(lane < 96, high, low)))

    wa = wf1[...]
    acc = (zero, zero, jnp.full((32, 128), -jnp.inf, F32), jnp.full((32, 128), jnp.inf, F32))
    def first_rows(z, rows, acc):
        outs = fine_conv(x1, wa, z, rows)
        for k, y in enumerate(rows):
            r1[z, y] = outs[k]
            if z in (0, 3) or y in (0, 7):
                x2r[z + 1, y + 1] = outs[k].astype(BF16)
        return gather_stats(acc, outs, True)

    halo_wait(0, x1, (0, 1))
    for z in (0, 3):
        acc = first_rows(z, (1, 2, 3, 4), acc)
    halo_send(1, x2r, (0, 1))
    halo_wait(0, x1, (8, 9))
    for z in (1, 2):
        acc = first_rows(z, range(8), acc)
    halo_wait(0, x1, range(2, 8))
    for z in (0, 3):
        acc = first_rows(z, (0, 5, 6, 7), acc)
    row = mixed_row(jnp.concatenate(acc, axis=0))
    greeted(1)
    greet(2)
    stat_send(0, [row, jnp.broadcast_to(peak0, (1, 128))])
    halo_send(1, x2r, (2, 3, 10, 11, 4, 5, 6, 7, 8, 9))
    group_send(2)
    group_send(0)

    got = stat_wait(0)
    peak0 = jnp.max(jnp.max(got[:, 1:2, :], axis=0), axis=1, keepdims=True)
    cols = mixed_total(got)
    aff = fine_affine(cols, 0)
    peak1 = peak_of(cols[64:96], cols[96:128], aff)
    b1 = bound_of(1)

    def settle(v, aff, b):
        return jnp.clip(act(v, aff), -b, b).astype(BF16)

    for z in range(4):
        for y in range(8):
            x2[z + 1, y + 1] = settle(r1[z, y], aff, b1)

    def settle_halo(ph, raw, buf, which, aff, b):
        for i in which:
            dz, dy = PIECES[ph][i][:2]
            there = exists(-dz, -dy)
            zs, ys = halo_slots(ph, i)

            @pl.when(there)
            def _():
                halo(ph, raw, i).wait_recv()
                for z in zs:
                    for y in ys:
                        buf[z, y] = settle(raw[z, y].astype(F32), aff, b)

            @pl.when(jnp.logical_not(there))
            def _():
                for z in zs:
                    for y in ys:
                        buf[z, y] = jnp.zeros(buf.shape[2:], buf.dtype)

    wb = wf2[...]
    acc = (zero, zero, None, None)
    settle_halo(1, x2r, x2, (8, 9), aff, b1)
    for z in (1, 2):
        outs = fine_conv(x2, wb, z)
        acc = gather_stats(acc, outs, False)
        for y in range(8):
            r2[z, y] = outs[y]
    settle_halo(1, x2r, x2, (0, 1, 4, 5, 6, 7, 2, 3, 10, 11), aff, b1)

    for z in (0, 3):
        outs = fine_conv(x2, wb, z)
        acc = gather_stats(acc, outs, False)
        for y in range(8):
            r2[z, y] = outs[y]

    stat_send(1, [sum_row(acc[0:2])])
    s_r = lax.broadcasted_iota(jnp.int32, (256, 128), 0)
    s_c = lax.broadcasted_iota(jnp.int32, (256, 128), 1)
    pick = onehot(s_r == jnp.where(s_c < 64, 2 * s_c, 2 * s_c))
    highs, lows = [], []
    for zp in range(2):
        hrow, lrow = [], []
        for yp in range(4):
            m = jnp.maximum(
                jnp.maximum(r2[2 * zp, 2 * yp], r2[2 * zp, 2 * yp + 1]),
                jnp.maximum(r2[2 * zp + 1, 2 * yp], r2[2 * zp + 1, 2 * yp + 1]),
            )
            m = jnp.maximum(m, pltpu.roll(m, 127, 1))
            h = m.astype(BF16)
            hrow.append(h)
            lrow.append((m - h.astype(F32)).astype(BF16))
        highs.append(jnp.concatenate(hrow, axis=0))
        lows.append(jnp.concatenate(lrow, axis=0))
    pooled = jnp.dot(jnp.concatenate(highs, axis=1), pick, preferred_element_type=F32)
    pooled = pooled + jnp.dot(jnp.concatenate(lows, axis=1), pick, preferred_element_type=F32)
    hi = jnp.full((32, 128), -jnp.inf, F32)
    lo = jnp.full((32, 128), jnp.inf, F32)
    for yp in range(4):
        blk = pooled[32 * yp : 32 * yp + 32]
        p3[yp] = blk
        put_raw(blk, yp + 1, h3, z3s)
        hi = jnp.maximum(hi, blk)
        lo = jnp.minimum(lo, blk)
    halo_done(0, x1)
    coarse_send(2, h3, z3s, z3r)
    group_forward(2)
    group_forward(0)
    group_send(1)

    got = stat_wait(1)
    cols = to_cols(jnp.sum(got[:, 0:1, :], axis=0))
    aff2 = fine_affine(cols, 1)
    b2 = bound_of(2)
    for yp in range(4):
        c3[yp + 1] = settle(p3[yp], aff2, b2)
    coarse_settle(2, h3, z3s, z3r, c3, c3z, aff2, b2)

    cfirst, clast = (lane & 63) == 0, (lane & 63) == 63

    def coarse_conv(buf, zbuf, w):
        strips = []
        mids = [buf[y] for y in range(6)]
        pairs = [[], mids, []]
        half = buf.shape[1] // 2
        for y in range(6):
            own = pltpu.roll(mids[y].astype(F32), 64, 1)
            prev = zbuf[0, y].astype(F32)
            nxt = zbuf[1, y].astype(F32)
            a = jnp.where(lower, prev, own[:half])
            b = jnp.where(lower, pltpu.roll(prev, 64, 1), own[half:])
            pairs[0].append(jnp.concatenate([a, b], axis=0).astype(BF16))
            a = jnp.where(lower, own[:half], pltpu.roll(nxt, 64, 1))
            b = jnp.where(lower, own[half:], nxt)
            pairs[2].append(jnp.concatenate([a, b], axis=0).astype(BF16))
        for zt in range(3):
            for yt in range(3):
                strips.append(jnp.concatenate(pairs[zt][yt : yt + 4], axis=1))
        got = jnp.dot(w, jnp.concatenate(strips, axis=0), preferred_element_type=F32)
        outs = []
        for y in range(4):
            blk = got[:, 128 * y : 128 * y + 128]
            parts = []
            for g in range(4):
                t = blk[48 * g : 48 * g + 48]
                parts.append(combine(t[0:16], t[16:32], t[32:48], cfirst, clast))
            outs.append(jnp.concatenate(parts, axis=0))
        return outs

    group_wait(0)
    outs = coarse_conv(c3, c3z, wg3[...].reshape(192, 288))
    zero64 = jnp.zeros((64, 128), F32)
    acc = (zero64, zero64, jnp.full((64, 128), -jnp.inf, F32), jnp.full((64, 128), jnp.inf, F32))
    acc = gather_stats(acc, outs, True)

    def extreme_row(cols, split):
        t = to_rows(jnp.concatenate(cols, axis=0))
        return jnp.where(split, jnp.max(t, axis=0, keepdims=True), jnp.min(t, axis=0, keepdims=True))

    stat_send(2, [sum_row(acc[0:2]), extreme_row(acc[2:4], lower), extreme_row((hi, hi, lo, lo), lower)])
    for y in range(4):
        put_raw(outs[y], y + 1, h4, z4s)
        r4i[y] = outs[y]
    halo_done(1, x2r)
    coarse_send(3, h4, z4s, z4r)
    group_forward(1)

    outof = onehot(jnp.logical_and((ci & 31) == (ri >> 3), (ci >> 5) == (ri & 7)))
    for zp in range(2):
        parts = []
        for z in (2 * zp, 2 * zp + 1):
            parts.append(jnp.concatenate([act(r2[z, y], aff2).astype(BF16) for y in range(8)], axis=0))
        moved = jnp.dot(outof, jnp.concatenate(parts, axis=1), preferred_element_type=F32)
        for k in range(2):
            z = 2 * zp + k
            skip[z] = moved[:, 128 * k : 128 * k + 128].reshape(32, 8, 128).astype(BF16)

    group_wait(2)
    gall = jnp.transpose(grow[...].reshape(2 * ny, 128))

    def gathered(k):
        parts = [gall[0:16, 2 * g + k : 2 * g + k + 1] for g in range(ny)]
        return jnp.broadcast_to(jnp.concatenate(parts, axis=0), (64, 128))

    got = stat_wait(2)
    cols = to_cols(jnp.sum(got[:, 0:1, :], axis=0))
    high = jnp.max(got[:, 1:3, :], axis=0)
    low = jnp.min(got[:, 1:3, :], axis=0)
    ext = jnp.where(lower, high, low)
    pext, ext = to_cols(ext[1:2]), to_cols(ext[0:1])
    peak2 = peak_of(pext[0:32], pext[64:96], aff2)
    aff3 = affine(cols[0:64], cols[64:128], coarse_cells, gathered(0), gathered(1))
    peak3 = peak_of(ext[0:64], ext[64:128], aff3)
    b3 = bound_of(3)

    peaks = jnp.where(lane == 0, peak0, jnp.where(lane == 1, peak1, jnp.where(lane == 2, peak2, peak3)))

    def cross(src, dst, dev):
        return pltpu.make_async_remote_copy(
            src_ref=am.at[src], dst_ref=am.at[dst], send_sem=xs.at[0], recv_sem=xs.at[1],
            device_id=dev, device_id_type=MESH,
        )

    def cross_all():
        return cross(pl.ds(0, ns - 1), pl.ds(0, ns - 1), other_sample(1)[1])

    for y in range(4):
        c4[y + 1] = settle(r4i[y], aff3, b3)
    coarse_settle(3, h4, z4s, z4r, c4, c4z, aff3, b3)
    greeted(2)
    am[smp] = peaks
    for d in range(1, ns):
        cross(smp, smp, other_sample(d)[1]).start()


    group_wait(1)
    outs = coarse_conv(c4, c4z, wg4[...].reshape(192, 576))
    acc = gather_stats((zero64, zero64, None, None), outs, False)
    def swap(src, dst, q):
        return pltpu.make_async_remote_copy(
            src_ref=a2s.at[src], dst_ref=a2a.at[dst], send_sem=bs.at[0], recv_sem=bs.at[1],
            device_id={"sy": q}, device_id_type=MESH,
        )

    stat_send(3, [sum_row(acc[0:2])])
    for g in range(4):
        for y in range(4):
            a2s[g, y] = outs[y][16 * g : 16 * g + 16]

    for d in range(1, ny):
        q = lax.rem(sy + d, ny)
        swap(q, sy, q).start()
    swap_all = swap(pl.ds(0, ny - 1), pl.ds(0, ny - 1), mate)
    a2a[sy] = a2s[sy]

    coarse_done(2, h3, z3s, z3r)
    coarse_done(3, h4, z4s, z4r)
    for ph in range(3):
        stat_all(ph).wait_send()
    for which in range(3):
        group_done(which)
    swap_all.wait_recv()
    got = stat_wait(3)
    rows8b = to_cols(jnp.sum(got[:, 0:1, :], axis=0))
    gs[...] = rows8b
    tot = gs[pl.ds(pl.multiple_of(sy * 16, 8), 16), :]
    totsq = gs[pl.ds(pl.multiple_of(64 + sy * 16, 8), 16), :]
    aff4 = affine(tot, totsq, coarse_cells, gain_col(5, 16), gain_col(7, 16))
    planes = [[], []]
    for g in range(4):
        for yp in range(2):
            u = act(a2a[g, 2 * yp], aff4)
            v = act(a2a[g, 2 * yp + 1], aff4)
            planes[0].append(jnp.where(lower, u, pltpu.roll(v, 64, 1)))
            planes[1].append(jnp.where(lower, pltpu.roll(u, 64, 1), v))
    both = [jnp.concatenate(planes[z], axis=1) for z in range(2)]
    coarse[...] = jnp.stack(both, axis=1).astype(BF16)

    if ns > 1:
        cross_all().wait_recv()
    amax[...] = jnp.max(am[...], axis=0)[:, 0:4]

    stat_all(3).wait_send()
    swap_all.wait_send()
    if ns > 1:
        cross_all().wait_send()


def solution(mesh):
    ny, nz, ns = mesh.shape["sy"], mesh.shape["sz"], mesh.shape["sample"]
    n = ny * nz
    vmem = pl.BlockSpec(memory_space=pltpu.VMEM)
    hbm = pl.BlockSpec(memory_space=pl.ANY)

    def step(volume, hist, w1, w2, w3, w4, gf, sf, gc, sc):
        dma = pltpu.SemaphoreType.DMA
        skip, coarse, amax = pl.pallas_call(
            functools.partial(body_entry, ny, nz, ns),
            out_shape=(
                pltpu.VMEM((4, 32, 8, 128), BF16),
                pltpu.VMEM((16, 2, 1024), BF16),
                pltpu.VMEM((1, 4), F32),
            ),
            in_specs=[hbm] * 10,
            out_specs=(vmem, vmem, vmem),
            scratch_shapes=[
                pltpu.VMEM((4, 16), F32),
                pltpu.VMEM((2, 32), F32),
                pltpu.VMEM((2, 32), F32),
                pltpu.VMEM((2, 16), F32),
                pltpu.VMEM((2, 16), F32),
                pltpu.VMEM((4, 32, 8, 128), BF16),
                pltpu.VMEM((9, 96, 32), BF16),
                pltpu.VMEM((9, 96, 32), BF16),
                pltpu.VMEM((9, 48, 32), BF16),
                pltpu.VMEM((9, 48, 64), BF16),
                pltpu.VMEM((96, 288), BF16),
                pltpu.VMEM((96, 288), BF16),
                pltpu.VMEM((ny, 48, 288), BF16),
                pltpu.VMEM((ny, 48, 576), BF16),
                pltpu.VMEM((6, 10, 32, 128), BF16),
                pltpu.VMEM((4, 8, 32, 128), F32),
                pltpu.VMEM((6, 10, 32, 128), BF16),
                pltpu.VMEM((6, 10, 32, 128), BF16),
                pltpu.VMEM((4, 8, 32, 128), F32),
                pltpu.VMEM((6, 32, 128), BF16),
                pltpu.VMEM((2, 6, 16, 128), BF16),
                pltpu.VMEM((2, 6, 16, 128), BF16),
                pltpu.VMEM((4, 32, 128), F32),
                pltpu.VMEM((6, 32, 128), BF16),
                pltpu.VMEM((2, 6, 16, 128), BF16),
                pltpu.VMEM((6, 64, 128), BF16),
                pltpu.VMEM((2, 6, 32, 128), BF16),
                pltpu.VMEM((2, 6, 32, 128), BF16),
                pltpu.VMEM((4, 64, 128), F32),
                pltpu.VMEM((6, 64, 128), BF16),
                pltpu.VMEM((2, 6, 32, 128), BF16),
                pltpu.VMEM((ny, 4, 16, 128), F32),
                pltpu.VMEM((ny, 4, 16, 128), F32),
                pltpu.VMEM((ny, 2, 128), F32),
                pltpu.VMEM((4, n, 4, 128), F32),
                pltpu.VMEM((ns, 1, 128), F32),
                pltpu.VMEM((8, 128), F32),
                pltpu.VMEM((128, 128), F32),
                pltpu.SemaphoreType.REGULAR((3,)),
                dma((13,)),
                dma((2, 12)),
                dma((2, 12)),
                dma((4,)),
                dma((4,)),
                dma((3, 3)),
                dma((3, ny)),
                dma((2,)),
                dma((2,)),
            ],
            compiler_params=pltpu.CompilerParams(collective_id=0, has_side_effects=True),
            name="encoder",
        )(
            volume.reshape(32, 4, 8, 128), hist, w1.reshape(9, 96, 32), w2.reshape(9, 96, 32),
            w3.reshape(9, 48, 32), w4.reshape(9, 48, 64), gf, sf, gc, sc,
        )
        skip, coarse, amax = pl.pallas_call(
            emit,
            out_shape=(
                jax.ShapeDtypeStruct((32, 4, 8, 128), BF16),
                jax.ShapeDtypeStruct((16, 2, 1024), BF16),
                jax.ShapeDtypeStruct((1, 4), F32),
            ),
            in_specs=[vmem] * 3,
            out_specs=(hbm, hbm, hbm),
            scratch_shapes=[dma((6,))],
            name="emit",
        )(*(pltpu.with_memory_space_constraint(t, pltpu.VMEM) for t in (skip, coarse, amax)))
        return skip.reshape(1, 32, 4, 8, 128), coarse.reshape(1, 16, 2, 1024), amax.reshape(4)

    return jax.shard_map(
        step,
        mesh=mesh,
        in_specs=(
            P("sample", None, "sz", "sy", None), P(), P(), P(),
            P(None, "sy", None), P(None, "sy", None), P(), P(), P(None, "sy"), P(None, "sy"),
        ),
        out_specs=(P("sample", None, "sz", "sy", None), P("sample", "sy", "sz", None), P()),
        check_vma=False,
    )


def body_entry(ny, nz, ns, *refs):
    (
        vol, hist, w1, w2, w3, w4, gf, sf, gc, sc, skip, coarse, amax,
        hist_v, gf_v, sf_v, gc_v, sc_v, vin, w1v, w2v, w3v, w4v, wf1, wf2, wg3, wg4,
        x1, r1, x2r, x2, r2, h3, z3s, z3r, p3, c3, c3z, h4, z4s, z4r, r4i, c4, c4z, a2a, a2s, grow,
        st, am, rows8, tcols,
        rounds, lsem, hs, hr, ss, sr, ws, wr, bs, xs,
    ) = refs
    body(
        ny, nz, ns,
        vol, hist, w1, w2, w3, w4, gf, sf, gc, sc, skip, coarse, amax,
        hist_v, gf_v, sf_v, gc_v, sc_v, vin, w1v, w2v, w3v, w4v, wf1, wf2, wg3, wg4,
        x1, r1, x2r, x2, r2, h3, z3s, z3r, p3, c3, c3z, h4, z4s, z4r, r4i, c4, c4z, a2a, a2s, grow,
        st, am, rows8,
        rounds, lsem, hs, hr, ss, sr, ws, wr, tcols, bs, xs,
    )


def emit(skip_v, coarse_v, amax_v, skip, coarse, amax, sem):
    copies = [pltpu.make_async_copy(skip_v.at[z], skip.at[:, z], sem.at[z]) for z in range(4)]
    copies.append(pltpu.make_async_copy(coarse_v, coarse, sem.at[4]))
    copies.append(pltpu.make_async_copy(amax_v, amax, sem.at[5]))
    for c in copies:
        c.start()
    for c in copies:
        c.wait()
```

```python
import functools

import jax
import jax.numpy as jnp
from jax import lax
from jax.experimental import pallas as pl
from jax.experimental.pallas import tpu as pltpu
from jax.sharding import PartitionSpec as P

MESH = pl.DeviceIdType.MESH
F32 = jnp.float32
BF16 = jnp.bfloat16
EPS = 1e-05
SLOPE = 0.01
PIECES = (
    ((-1, 0, 1, 6), (1, 0, 1, 6), (-1, 0, 7, 2), (1, 0, 7, 2), (-1, -1, 1, 1), (-1, 1, 8, 1), (1, -1, 1, 1), (1, 1, 8, 1),
     (0, -1, 1, 1), (0, 1, 8, 1)),
    ((-1, 0, 2, 4), (1, 0, 2, 4), (-1, 0, 6, 3), (1, 0, 6, 3), (-1, -1, 1, 1), (-1, 1, 8, 1), (1, -1, 1, 1), (1, 1, 8, 1),
     (0, -1, 1, 1), (0, 1, 8, 1), (-1, 0, 1, 1), (1, 0, 1, 1)),
)
DIRS = ((-1, 0), (1, 0), (-1, -1), (-1, 1), (1, -1), (1, 1), (0, -1), (0, 1))


def body(
    ny, nz, ns,
    vol, hist_h, w1, w2, w3, w4, gf_h, sf_h, gc_h, sc_h,
    skip, coarse, amax,
    hist, gf, sf, gc, sc, vin, w1v, w2v, w3v, w4v, wf1, wf2, wg3, wg4,
    x1, r1, x2r, x2, r2, h3, z3s, z3r, p3, c3, c3z, h4, z4s, z4r, r4i, c4, c4z, a2a, a2s,
    st, am, rows8,
    rounds, lsem, hs, hr, ss, sr, ws, wr, gs, bs, xs,
):
    n = ny * nz
    sy = lax.axis_index("sy")
    sz = lax.axis_index("sz")
    smp = lax.axis_index("sample")
    me = sz * ny + sy

    near = [{"sz": lax.rem(sz + d, nz)} for d in sorted({1, nz - 1})]
    near += [{"sy": lax.rem(sy + d, ny)} for d in range(1, ny)]
    if ns > 1:
        sx, sv = lax.rem(smp, 4), lax.div(smp, 4)
        near += [{"sample": sv * 4 + lax.rem(sx + d, 4)} for d in (1, 3)]
        near += [{"sample": lax.rem(sv + d, 4) * 4 + sx} for d in (1, 3)]
    barrier = pltpu.get_barrier_semaphore()
    for dev in near:
        pl.semaphore_signal(barrier, inc=1, device_id=dev, device_id_type=MESH)

    def greet(r):
        for dev in near:
            pl.semaphore_signal(rounds.at[r], inc=1, device_id=dev, device_id_type=MESH)

    def greeted(r):
        pl.semaphore_wait(rounds.at[r], len(near))

    place = {0: 0, 3: 1, 1: 2, 2: 3}
    loads = [pltpu.make_async_copy(vol.at[:, z], vin.at[place[z]], lsem.at[place[z] // 2]) for z in range(4)]
    small = ((hist_h, hist), (w1, w1v), (w2, w2v), (w3, w3v), (w4, w4v), (gf_h, gf), (sf_h, sf), (gc_h, gc), (sc_h, sc))
    for i, (s, d) in enumerate(small):
        loads.append(pltpu.make_async_copy(s, d, lsem.at[2 + i]))
    for i in (4, 0, 3, 1, 2, 5, 6, 7, 8, 9, 10, 11, 12):
        loads[i].start()

    def partner(d):
        p = lax.rem(me + d, n)
        return p, {"sy": lax.rem(p, ny), "sz": lax.div(p, ny)}

    order = sorted(range(1, n), key=lambda d: -min(d, n - d))
    def other_sample(d):
        q = lax.rem(smp + d, ns)
        return q, {"sample": q}

    def exists(dz, dy):
        cond = None
        for idx, cnt, d in ((sz, nz, dz), (sy, ny, dy)):
            if d == 0:
                continue
            c = (idx > 0) if d < 0 else (idx < cnt - 1)
            cond = c if cond is None else jnp.logical_and(cond, c)
        return cond

    lane = lax.broadcasted_iota(jnp.int32, (1, 128), 1)
    lower = lane < 64

    def bound_of(l):
        b = jnp.max(hist[l : l + 1, :], axis=1, keepdims=True)
        return b.astype(BF16).astype(F32)

    def src_z(dz, zl):
        return pl.ds(1, zl) if dz == 0 else (pl.ds(1, 1) if dz < 0 else pl.ds(zl, 1))

    def dst_z(dz, zl):
        return pl.ds(1, zl) if dz == 0 else (pl.ds(zl + 1, 1) if dz < 0 else pl.ds(0, 1))

    def halo(ph, buf, i):
        dz, dy, row, count = PIECES[ph][i]
        return pltpu.make_async_remote_copy(
            src_ref=buf.at[src_z(dz, 4), pl.ds(row, count)],
            dst_ref=buf.at[dst_z(dz, 4), pl.ds(row - 8 * dy, count)],
            send_sem=hs.at[i],
            recv_sem=hr.at[ph % 2, i],
            device_id={"sy": sy + dy, "sz": sz + dz},
            device_id_type=MESH,
        )

    def halo_send(ph, buf, which):
        for i in which:
            @pl.when(exists(*PIECES[ph][i][:2]))
            def _():
                halo(ph, buf, i).start()

    def halo_wait(ph, buf, which):
        for i in which:
            @pl.when(exists(-PIECES[ph][i][0], -PIECES[ph][i][1]))
            def _():
                halo(ph, buf, i).wait_recv()

    def halo_done(ph, buf, which):
        for i in which:
            @pl.when(exists(*PIECES[ph][i][:2]))
            def _():
                halo(ph, buf, i).wait_send()

    def halo_slots(ph, i):
        dz, dy, row, count = PIECES[ph][i]
        return slots(dz, 4), range(row - 8 * dy, row - 8 * dy + count)

    def coarse_halo(ph, own, zs, zr, i):
        dz, dy = DIRS[i]
        if dz == 0:
            src, dst = own.at[src_z(dy, 4)], own.at[dst_z(dy, 4)]
        else:
            up = 1 if dz > 0 else 0
            src, dst = zs.at[up, src_z(dy, 4)], zr.at[1 - up, dst_z(dy, 4)]
        return pltpu.make_async_remote_copy(
            src_ref=src, dst_ref=dst, send_sem=hs.at[i], recv_sem=hr.at[ph % 2, i],
            device_id={"sy": sy + dy, "sz": sz + dz}, device_id_type=MESH,
        )

    def coarse_send(ph, own, zs, zr):
        for i in range(8):
            @pl.when(exists(*DIRS[i]))
            def _():
                coarse_halo(ph, own, zs, zr, i).start()

    def coarse_done(ph, own, zs, zr):
        for i in range(8):
            @pl.when(exists(*DIRS[i]))
            def _():
                coarse_halo(ph, own, zs, zr, i).wait_send()

    def put_raw(blk, y, own, zs):
        half = blk.shape[0] // 2
        top, low = blk[:half], blk[half:]
        own[y] = blk.astype(BF16)
        zs[0, y] = jnp.where(lower, top, pltpu.roll(low, 64, 1)).astype(BF16)
        zs[1, y] = jnp.where(lower, pltpu.roll(top, 64, 1), low).astype(BF16)

    def coarse_settle(ph, own, zs, zr, buf, zbuf, aff, b):
        half = buf.shape[1] // 2
        paff = tuple(jnp.where(lower, t[:half], t[half:]) for t in aff)
        for i in range(8):
            dz, dy = DIRS[i]
            there = exists(-dz, -dy)
            ys = slots(dy, 4)

            @pl.when(there)
            def _():
                coarse_halo(ph, own, zs, zr, i).wait_recv()
                for y in ys:
                    if dz == 0:
                        buf[y] = settle(own[y].astype(F32), aff, b)
                    else:
                        k = 0 if dz > 0 else 1
                        zbuf[k, y] = settle(zr[k, y].astype(F32), paff, b)

            @pl.when(jnp.logical_not(there))
            def _():
                for y in ys:
                    if dz == 0:
                        buf[y] = jnp.zeros(buf.shape[1:], BF16)
                    else:
                        k = 0 if dz > 0 else 1
                        zbuf[k, y] = jnp.zeros(zbuf.shape[2:], BF16)

    def slots(d, length):
        return range(1, length + 1) if d == 0 else ((0,) if d > 0 else (length + 1,))

    def stat_copy(ph, src, dst, dev):
        return pltpu.make_async_remote_copy(
            src_ref=st.at[ph, src], dst_ref=st.at[ph, dst],
            send_sem=ss.at[0], recv_sem=sr.at[ph % 2],
            device_id=dev, device_id_type=MESH,
        )

    def stat_all(ph):
        rest = pl.ds(0, n - 1)
        return stat_copy(ph, rest, rest, partner(1)[1])

    def stat_send(ph, rows):
        if ph > 0:
            stat_all(ph - 1).wait_send()
        st[ph, me] = jnp.concatenate(rows + [rows[0]] * (4 - len(rows)), axis=0)
        for d in order:
            stat_copy(ph, me, me, partner(d)[1]).start()

    def stat_wait(ph):
        stat_all(ph).wait_recv()
        return st[ph]

    def to_rows(cols):
        return jnp.transpose(cols)

    def to_cols(row):
        return jnp.transpose(jnp.broadcast_to(row, (128, 128)))

    def affine(tot, totsq, cells, g, s):
        m = tot / cells
        var = totsq / cells - m * m
        a = lax.rsqrt(var + EPS) * g
        return a, m, s

    def act(v, aff):
        a, m, s = aff
        t = (v - m) * a + s
        return jnp.maximum(t, SLOPE * t)

    ri = lax.broadcasted_iota(jnp.int32, (256, 256), 0)
    ci = lax.broadcasted_iota(jnp.int32, (256, 256), 1)

    def onehot(cond):
        return jnp.where(cond, 1.0, 0.0).astype(BF16)

    into = onehot(jnp.logical_and((ri & 31) == (ci >> 3), (ri >> 5) == (ci & 7)))

    loads[4].wait()
    b0 = bound_of(0)
    peaks0 = []

    def take(zp):
        parts = []
        pair = pl.ds(place[zp[0]], 2)
        pltpu.make_async_copy(vin.at[pair], vin.at[pair], lsem.at[place[zp[0]] // 2]).wait()
        for z in zp:
            v = vin[place[z]].astype(F32).reshape(256, 128)
            peaks0.append(jnp.abs(v))
            parts.append(v.astype(BF16))
        moved = jnp.dot(into, jnp.concatenate(parts, axis=1), preferred_element_type=F32)
        moved = jnp.clip(moved, -b0, b0).astype(BF16)
        for k in range(2):
            for y in range(8):
                x1[1 + zp[k], 1 + y] = moved[32 * y : 32 * y + 32, 128 * k : 128 * k + 128]

    take((0, 3))
    pl.semaphore_wait(barrier, len(near))
    greet(0)
    halo_send(0, x1, (0, 1))
    take((1, 2))
    halo_send(0, x1, (8, 9, 2, 3))
    peak0 = jnp.maximum(jnp.maximum(peaks0[0], peaks0[1]), jnp.maximum(peaks0[2], peaks0[3]))
    peak0 = jnp.max(jnp.max(peak0, axis=0, keepdims=True), axis=1, keepdims=True)

    for i in range(5, 13):
        loads[i].wait()
    rows8[...] = jnp.zeros_like(rows8)
    rows8[0:2, 0:32] = gf[...]
    rows8[2:4, 0:32] = sf[...]
    rows8[4:6, 0:16] = gc[...]
    rows8[6:8, 0:16] = sc[...]
    gcols = jnp.transpose(rows8[...])

    def gain_col(j, count):
        return jnp.broadcast_to(gcols[0:count, j : j + 1], (count, 128))


    def lanes_of(w):
        return jnp.concatenate([w[k] for k in range(9)], axis=1)

    wf1[...] = lanes_of(w1v)
    wf2[...] = lanes_of(w2v)
    wg3[sy] = lanes_of(w3v)
    wg4[sy] = lanes_of(w4v)

    for i in range(len(PIECES[0])):
        @pl.when(jnp.logical_not(exists(-PIECES[0][i][0], -PIECES[0][i][1])))
        def _():
            for z in halo_slots(0, i)[0]:
                for y in halo_slots(0, i)[1]:
                    x1[z, y] = jnp.zeros((32, 128), BF16)

    mate = sy + 1 - 2 * lax.rem(sy, 2)
    cross_sy = lax.rem(sy + 2, 4)
    cross_mate = lax.rem(mate + 2, 4)

    def group(which, kind, src):
        buf = (wg3, wg4)[which]
        return pltpu.make_async_remote_copy(
            src_ref=buf.at[src], dst_ref=buf.at[src],
            send_sem=ws.at[which, kind], recv_sem=wr.at[which, kind],
            device_id={"sy": cross_sy if kind == 1 else mate}, device_id_type=MESH,
        )

    def group_send(which):
        group(which, 1, sy).start()
        group(which, 0, sy).start()

    def group_forward(which):
        group(which, 1, cross_sy).wait_recv()
        group(which, 2, cross_sy).start()

    def group_wait(which):
        group(which, 0, mate).wait_recv()
        group(which, 2, cross_mate).wait_recv()

    def group_done(which):
        group(which, 0, sy).wait_send()
        group(which, 1, sy).wait_send()
        group(which, 2, cross_sy).wait_send()

    fine_cells = float(4 * nz * 8 * ny * 128)
    coarse_cells = fine_cells / 8

    def fine_affine(cols, j):
        return affine(cols[0:32], cols[32:64], fine_cells, gain_col(j, 32), gain_col(2 + j, 32))

    def peak_of(high, low, aff):
        v = jnp.maximum(jnp.abs(act(high, aff)), jnp.abs(act(low, aff))).astype(BF16).astype(F32)
        return jnp.max(jnp.max(v, axis=0, keepdims=True), axis=1, keepdims=True)

    greeted(0)
    greet(1)
    halo_send(0, x1, (4, 5, 6, 7))

    first, last = lane == 0, lane == 127

    def combine(p0, p1, p2, lo, hi):
        left = jnp.where(lo, 0.0, pltpu.roll(p0, 1, 1))
        right = jnp.where(hi, 0.0, pltpu.roll(p2, 127, 1))
        return p1 + left + right

    def fine_conv(buf, w, z, rows=range(8)):
        strips = []
        for zt in range(3):
            for yt in range(3):
                strips.append(jnp.concatenate([buf[z + zt, y + yt] for y in rows], axis=1))
        got = jnp.dot(w, jnp.concatenate(strips, axis=0), preferred_element_type=F32)
        outs = []
        for k in range(len(rows)):
            blk = got[:, 128 * k : 128 * k + 128]
            outs.append(combine(blk[0:32], blk[32:64], blk[64:96], first, last))
        return outs

    zero = jnp.zeros((32, 128), F32)

    def gather_stats(acc, blocks, extremes):
        s, q, hi, lo = acc
        for b in blocks:
            s = s + b
            q = q + b * b
            if extremes:
                hi = jnp.maximum(hi, b)
                lo = jnp.minimum(lo, b)
        return s, q, hi, lo

    def sum_row(cols):
        cols = jnp.concatenate(cols, axis=0)
        if cols.shape[0] < 128:
            cols = jnp.concatenate([cols, cols], axis=0)
        return jnp.sum(to_rows(cols), axis=0, keepdims=True)

    def mixed_row(cols):
        t = to_rows(cols)
        total = jnp.sum(t, axis=0, keepdims=True)
        high = jnp.max(t, axis=0, keepdims=True)
        low = jnp.min(t, axis=0, keepdims=True)
        return jnp.where(lane < 64, total, jnp.where(lane < 96, high, low))

    def mixed_total(got):
        total = jnp.sum(got[:, 0:1, :], axis=0)
        high = jnp.max(got[:, 0:1, :], axis=0)
        low = jnp.min(got[:, 0:1, :], axis=0)
        return to_cols(jnp.where(lane < 64, total, jnp.where(lane < 96, high, low)))

    wa = wf1[...]
    acc = (zero, zero, jnp.full((32, 128), -jnp.inf, F32), jnp.full((32, 128), jnp.inf, F32))
    def first_rows(z, rows, acc):
        outs = fine_conv(x1, wa, z, rows)
        for k, y in enumerate(rows):
            r1[z, y] = outs[k]
            if z in (0, 3) or y in (0, 7):
                x2r[z + 1, y + 1] = outs[k].astype(BF16)
        return gather_stats(acc, outs, True)

    halo_wait(0, x1, (0, 1))
    for z in (0, 3):
        acc = first_rows(z, (1, 2, 3, 4), acc)
    halo_done(0, x1, (0, 1))
    halo_send(1, x2r, (0, 1))
    halo_wait(0, x1, (8, 9))
    for z in (1, 2):
        acc = first_rows(z, range(8), acc)
    halo_wait(0, x1, range(2, 8))
    for z in (0, 3):
        acc = first_rows(z, (0, 5, 6, 7), acc)
    row = mixed_row(jnp.concatenate(acc, axis=0))
    greeted(1)
    greet(2)
    stat_send(0, [row, jnp.broadcast_to(peak0, (1, 128)), rows8[4:5], rows8[6:7]])
    halo_done(0, x1, range(2, 10))
    halo_send(1, x2r, (2, 3, 10, 11, 4, 5, 6, 7, 8, 9))
    group_send(0)

    got = stat_wait(0)
    group_send(1)
    peak0 = jnp.max(jnp.max(got[:, 1:2, :], axis=0), axis=1, keepdims=True)
    cols = mixed_total(got)
    aff = fine_affine(cols, 0)
    peak1 = peak_of(cols[64:96], cols[96:128], aff)
    b1 = bound_of(1)

    def settle(v, aff, b):
        return jnp.clip(act(v, aff), -b, b).astype(BF16)


    def settle_halo(ph, raw, buf, which, aff, b):
        for i in which:
            dz, dy = PIECES[ph][i][:2]
            there = exists(-dz, -dy)
            zs, ys = halo_slots(ph, i)

            @pl.when(there)
            def _():
                halo(ph, raw, i).wait_recv()
                for z in zs:
                    for y in ys:
                        buf[z, y] = settle(raw[z, y].astype(F32), aff, b)

            @pl.when(jnp.logical_not(there))
            def _():
                for z in zs:
                    for y in ys:
                        buf[z, y] = jnp.zeros(buf.shape[2:], buf.dtype)

    wb = wf2[...]
    acc = (zero, zero, None, None)
    settle_halo(1, x2r, x2, (8, 9), aff, b1)
    for z in range(4):
        for y in range(8):
            x2[z + 1, y + 1] = settle(r1[z, y], aff, b1)
    for z in (1, 2):
        outs = fine_conv(x2, wb, z)
        acc = gather_stats(acc, outs, False)
        for y in range(8):
            r2[z, y] = outs[y]
    settle_halo(1, x2r, x2, (0, 1, 4, 5, 6, 7, 2, 3, 10, 11), aff, b1)

    for z in (0, 3):
        outs = fine_conv(x2, wb, z)
        acc = gather_stats(acc, outs, False)
        for y in range(8):
            r2[z, y] = outs[y]

    stat_send(1, [sum_row(acc[0:2])])
    s_r = lax.broadcasted_iota(jnp.int32, (256, 128), 0)
    s_c = lax.broadcasted_iota(jnp.int32, (256, 128), 1)
    pick = onehot(s_r == jnp.where(s_c < 64, 2 * s_c, 2 * s_c))
    highs, lows = [], []
    for zp in range(2):
        hrow, lrow = [], []
        for yp in range(4):
            m = jnp.maximum(
                jnp.maximum(r2[2 * zp, 2 * yp], r2[2 * zp, 2 * yp + 1]),
                jnp.maximum(r2[2 * zp + 1, 2 * yp], r2[2 * zp + 1, 2 * yp + 1]),
            )
            m = jnp.maximum(m, pltpu.roll(m, 127, 1))
            h = m.astype(BF16)
            hrow.append(h)
            lrow.append((m - h.astype(F32)).astype(BF16))
        highs.append(jnp.concatenate(hrow, axis=0))
        lows.append(jnp.concatenate(lrow, axis=0))
    pooled = jnp.dot(jnp.concatenate(highs, axis=1), pick, preferred_element_type=F32)
    pooled = pooled + jnp.dot(jnp.concatenate(lows, axis=1), pick, preferred_element_type=F32)
    hi = jnp.full((32, 128), -jnp.inf, F32)
    lo = jnp.full((32, 128), jnp.inf, F32)
    for yp in range(4):
        blk = pooled[32 * yp : 32 * yp + 32]
        p3[yp] = blk
        put_raw(blk, yp + 1, h3, z3s)
        hi = jnp.maximum(hi, blk)
        lo = jnp.minimum(lo, blk)
    halo_done(1, x2r, range(12))
    coarse_send(2, h3, z3s, z3r)
    group_forward(0)
    group_forward(1)

    got = stat_wait(1)
    cols = to_cols(jnp.sum(got[:, 0:1, :], axis=0))
    aff2 = fine_affine(cols, 1)
    b2 = bound_of(2)
    coarse_settle(2, h3, z3s, z3r, c3, c3z, aff2, b2)

    cfirst, clast = (lane & 63) == 0, (lane & 63) == 63

    def coarse_conv(buf, zbuf, w):
        strips = []
        mids = [buf[y] for y in range(6)]
        pairs = [[], mids, []]
        half = buf.shape[1] // 2
        for y in range(6):
            own = pltpu.roll(mids[y].astype(F32), 64, 1)
            prev = zbuf[0, y].astype(F32)
            nxt = zbuf[1, y].astype(F32)
            a = jnp.where(lower, prev, own[:half])
            b = jnp.where(lower, pltpu.roll(prev, 64, 1), own[half:])
            pairs[0].append(jnp.concatenate([a, b], axis=0).astype(BF16))
            a = jnp.where(lower, own[:half], pltpu.roll(nxt, 64, 1))
            b = jnp.where(lower, own[half:], nxt)
            pairs[2].append(jnp.concatenate([a, b], axis=0).astype(BF16))
        for zt in range(3):
            for yt in range(3):
                strips.append(jnp.concatenate(pairs[zt][yt : yt + 4], axis=1))
        got = jnp.dot(w, jnp.concatenate(strips, axis=0), preferred_element_type=F32)
        outs = []
        for y in range(4):
            blk = got[:, 128 * y : 128 * y + 128]
            parts = []
            for g in range(4):
                t = blk[48 * g : 48 * g + 48]
                parts.append(combine(t[0:16], t[16:32], t[32:48], cfirst, clast))
            outs.append(jnp.concatenate(parts, axis=0))
        return outs

    group_wait(0)
    for yp in range(4):
        c3[yp + 1] = settle(p3[yp], aff2, b2)
    outs = coarse_conv(c3, c3z, wg3[...].reshape(192, 288))
    zero64 = jnp.zeros((64, 128), F32)
    acc = (zero64, zero64, jnp.full((64, 128), -jnp.inf, F32), jnp.full((64, 128), jnp.inf, F32))
    acc = gather_stats(acc, outs, True)

    def extreme_row(cols, split):
        t = to_rows(jnp.concatenate(cols, axis=0))
        return jnp.where(split, jnp.max(t, axis=0, keepdims=True), jnp.min(t, axis=0, keepdims=True))

    stat_send(2, [sum_row(acc[0:2]), extreme_row(acc[2:4], lower), extreme_row((hi, hi, lo, lo), lower)])
    for y in range(4):
        put_raw(outs[y], y + 1, h4, z4s)
        r4i[y] = outs[y]
    coarse_done(2, h3, z3s, z3r)
    coarse_send(3, h4, z4s, z4r)

    outof = onehot(jnp.logical_and((ci & 31) == (ri >> 3), (ci >> 5) == (ri & 7)))
    for zp in range(2):
        parts = []
        for z in (2 * zp, 2 * zp + 1):
            parts.append(jnp.concatenate([act(r2[z, y], aff2).astype(BF16) for y in range(8)], axis=0))
        moved = jnp.dot(outof, jnp.concatenate(parts, axis=1), preferred_element_type=F32)
        for k in range(2):
            z = 2 * zp + k
            skip[z] = moved[:, 128 * k : 128 * k + 128].reshape(32, 8, 128).astype(BF16)

    gall = jnp.transpose(jnp.concatenate([st[0, sz * ny + g, 2:4] for g in range(ny)], axis=0))

    def gathered(k):
        parts = [gall[0:16, 2 * g + k : 2 * g + k + 1] for g in range(ny)]
        return jnp.broadcast_to(jnp.concatenate(parts, axis=0), (64, 128))

    got = stat_wait(2)
    cols = to_cols(jnp.sum(got[:, 0:1, :], axis=0))
    aff3 = affine(cols[0:64], cols[64:128], coarse_cells, gathered(0), gathered(1))
    b3 = bound_of(3)

    def cross(src, dst, dev):
        return pltpu.make_async_remote_copy(
            src_ref=am.at[src], dst_ref=am.at[dst], send_sem=xs.at[0], recv_sem=xs.at[1],
            device_id=dev, device_id_type=MESH,
        )

    def cross_all():
        return cross(pl.ds(0, ns - 1), pl.ds(0, ns - 1), other_sample(1)[1])

    coarse_settle(3, h4, z4s, z4r, c4, c4z, aff3, b3)
    group_wait(1)
    for y in range(4):
        c4[y + 1] = settle(r4i[y], aff3, b3)

    high = jnp.max(got[:, 1:3, :], axis=0)
    low = jnp.min(got[:, 1:3, :], axis=0)
    ext = jnp.where(lower, high, low)
    pext, ext = to_cols(ext[1:2]), to_cols(ext[0:1])
    peak2 = peak_of(pext[0:32], pext[64:96], aff2)
    peak3 = peak_of(ext[0:64], ext[64:128], aff3)
    peaks = jnp.where(lane == 0, peak0, jnp.where(lane == 1, peak1, jnp.where(lane == 2, peak2, peak3)))

    greeted(2)
    am[smp] = peaks
    for d in range(1, ns):
        cross(smp, smp, other_sample(d)[1]).start()


    outs = coarse_conv(c4, c4z, wg4[...].reshape(192, 576))
    acc = gather_stats((zero64, zero64, None, None), outs, False)
    def swap(src, dst, q):
        return pltpu.make_async_remote_copy(
            src_ref=a2s.at[src], dst_ref=a2a.at[dst], send_sem=bs.at[0], recv_sem=bs.at[1],
            device_id={"sy": q}, device_id_type=MESH,
        )

    stat_send(3, [sum_row(acc[0:2])])
    for g in range(4):
        for y in range(4):
            a2s[g, y] = outs[y][16 * g : 16 * g + 16].astype(BF16)

    for d in range(1, ny):
        q = lax.rem(sy + d, ny)
        swap(q, sy, q).start()
    swap_all = swap(pl.ds(0, ny - 1), pl.ds(0, ny - 1), mate)
    a2a[sy] = a2s[sy]

    coarse_done(3, h4, z4s, z4r)
    for which in range(2):
        group_done(which)
    swap_all.wait_recv()
    got = stat_wait(3)
    rows8b = to_cols(jnp.sum(got[:, 0:1, :], axis=0))
    gs[...] = rows8b
    tot = gs[pl.ds(pl.multiple_of(sy * 16, 8), 16), :]
    totsq = gs[pl.ds(pl.multiple_of(64 + sy * 16, 8), 16), :]
    aff4 = affine(tot, totsq, coarse_cells, gain_col(5, 16), gain_col(7, 16))
    planes = [[], []]
    for g in range(4):
        for yp in range(2):
            u = act(a2a[g, 2 * yp].astype(F32), aff4)
            v = act(a2a[g, 2 * yp + 1].astype(F32), aff4)
            planes[0].append(jnp.where(lower, u, pltpu.roll(v, 64, 1)))
            planes[1].append(jnp.where(lower, pltpu.roll(u, 64, 1), v))
    both = [jnp.concatenate(planes[z], axis=1) for z in range(2)]
    coarse[...] = jnp.stack(both, axis=1).astype(BF16)

    if ns > 1:
        cross_all().wait_recv()
    amax[...] = jnp.max(am[...], axis=0)[:, 0:4]

    stat_all(3).wait_send()
    swap_all.wait_send()
    if ns > 1:
        cross_all().wait_send()


def solution(mesh):
    ny, nz, ns = mesh.shape["sy"], mesh.shape["sz"], mesh.shape["sample"]
    n = ny * nz
    vmem = pl.BlockSpec(memory_space=pltpu.VMEM)
    hbm = pl.BlockSpec(memory_space=pl.ANY)

    def step(volume, hist, w1, w2, w3, w4, gf, sf, gc, sc):
        dma = pltpu.SemaphoreType.DMA
        skip, coarse, amax = pl.pallas_call(
            functools.partial(body_entry, ny, nz, ns),
            out_shape=(
                pltpu.VMEM((4, 32, 8, 128), BF16),
                pltpu.VMEM((16, 2, 1024), BF16),
                pltpu.VMEM((1, 4), F32),
            ),
            in_specs=[hbm] * 10,
            out_specs=(vmem, vmem, vmem),
            scratch_shapes=[
                pltpu.VMEM((4, 16), F32),
                pltpu.VMEM((2, 32), F32),
                pltpu.VMEM((2, 32), F32),
                pltpu.VMEM((2, 16), F32),
                pltpu.VMEM((2, 16), F32),
                pltpu.VMEM((4, 32, 8, 128), BF16),
                pltpu.VMEM((9, 96, 32), BF16),
                pltpu.VMEM((9, 96, 32), BF16),
                pltpu.VMEM((9, 48, 32), BF16),
                pltpu.VMEM((9, 48, 64), BF16),
                pltpu.VMEM((96, 288), BF16),
                pltpu.VMEM((96, 288), BF16),
                pltpu.VMEM((ny, 48, 288), BF16),
                pltpu.VMEM((ny, 48, 576), BF16),
                pltpu.VMEM((6, 10, 32, 128), BF16),
                pltpu.VMEM((4, 8, 32, 128), F32),
                pltpu.VMEM((6, 10, 32, 128), BF16),
                pltpu.VMEM((6, 10, 32, 128), BF16),
                pltpu.VMEM((4, 8, 32, 128), F32),
                pltpu.VMEM((6, 32, 128), BF16),
                pltpu.VMEM((2, 6, 16, 128), BF16),
                pltpu.VMEM((2, 6, 16, 128), BF16),
                pltpu.VMEM((4, 32, 128), F32),
                pltpu.VMEM((6, 32, 128), BF16),
                pltpu.VMEM((2, 6, 16, 128), BF16),
                pltpu.VMEM((6, 64, 128), BF16),
                pltpu.VMEM((2, 6, 32, 128), BF16),
                pltpu.VMEM((2, 6, 32, 128), BF16),
                pltpu.VMEM((4, 64, 128), F32),
                pltpu.VMEM((6, 64, 128), BF16),
                pltpu.VMEM((2, 6, 32, 128), BF16),
                pltpu.VMEM((ny, 4, 16, 128), BF16),
                pltpu.VMEM((ny, 4, 16, 128), BF16),
                pltpu.VMEM((4, n, 4, 128), F32),
                pltpu.VMEM((ns, 1, 128), F32),
                pltpu.VMEM((8, 128), F32),
                pltpu.VMEM((128, 128), F32),
                pltpu.SemaphoreType.REGULAR((3,)),
                dma((11,)),
                dma((12,)),
                dma((2, 12)),
                dma((1,)),
                dma((2,)),
                dma((2, 3)),
                dma((2, 3)),
                dma((2,)),
                dma((2,)),
            ],
            compiler_params=pltpu.CompilerParams(collective_id=0, has_side_effects=True),
            name="encoder",
        )(
            volume.reshape(32, 4, 8, 128), hist, w1.reshape(9, 96, 32), w2.reshape(9, 96, 32),
            w3.reshape(9, 48, 32), w4.reshape(9, 48, 64), gf, sf, gc, sc,
        )
        skip, coarse, amax = pl.pallas_call(
            emit,
            out_shape=(
                jax.ShapeDtypeStruct((32, 4, 8, 128), BF16),
                jax.ShapeDtypeStruct((16, 2, 1024), BF16),
                jax.ShapeDtypeStruct((1, 4), F32),
            ),
            in_specs=[vmem] * 3,
            out_specs=(hbm, hbm, hbm),
            scratch_shapes=[dma((6,))],
            name="emit",
        )(*(pltpu.with_memory_space_constraint(t, pltpu.VMEM) for t in (skip, coarse, amax)))
        return skip.reshape(1, 32, 4, 8, 128), coarse.reshape(1, 16, 2, 1024), amax.reshape(4)

    return jax.shard_map(
        step,
        mesh=mesh,
        in_specs=(
            P("sample", None, "sz", "sy", None), P(), P(), P(),
            P(None, "sy", None), P(None, "sy", None), P(), P(), P(None, "sy"), P(None, "sy"),
        ),
        out_specs=(P("sample", None, "sz", "sy", None), P("sample", "sy", "sz", None), P()),
        check_vma=False,
    )


def body_entry(ny, nz, ns, *refs):
    (
        vol, hist, w1, w2, w3, w4, gf, sf, gc, sc, skip, coarse, amax,
        hist_v, gf_v, sf_v, gc_v, sc_v, vin, w1v, w2v, w3v, w4v, wf1, wf2, wg3, wg4,
        x1, r1, x2r, x2, r2, h3, z3s, z3r, p3, c3, c3z, h4, z4s, z4r, r4i, c4, c4z, a2a, a2s,
        st, am, rows8, tcols,
        rounds, lsem, hs, hr, ss, sr, ws, wr, bs, xs,
    ) = refs
    body(
        ny, nz, ns,
        vol, hist, w1, w2, w3, w4, gf, sf, gc, sc, skip, coarse, amax,
        hist_v, gf_v, sf_v, gc_v, sc_v, vin, w1v, w2v, w3v, w4v, wf1, wf2, wg3, wg4,
        x1, r1, x2r, x2, r2, h3, z3s, z3r, p3, c3, c3z, h4, z4s, z4r, r4i, c4, c4z, a2a, a2s,
        st, am, rows8,
        rounds, lsem, hs, hr, ss, sr, ws, wr, tcols, bs, xs,
    )


def emit(skip_v, coarse_v, amax_v, skip, coarse, amax, sem):
    copies = [pltpu.make_async_copy(skip_v.at[z], skip.at[:, z], sem.at[z]) for z in range(4)]
    copies.append(pltpu.make_async_copy(coarse_v, coarse, sem.at[4]))
    copies.append(pltpu.make_async_copy(amax_v, amax, sem.at[5]))
    for c in copies:
        c.start()
    for c in copies:
        c.wait()
```

```python
import functools

import jax
import jax.numpy as jnp
from jax import lax
from jax.experimental import pallas as pl
from jax.experimental.pallas import tpu as pltpu
from jax.sharding import PartitionSpec as P

MESH = pl.DeviceIdType.MESH
F32 = jnp.float32
BF16 = jnp.bfloat16
EPS = 1e-05
SLOPE = 0.01
PIECES = (
    ((-1, 0, 1, 6), (1, 0, 1, 6), (-1, 0, 7, 2), (1, 0, 7, 2), (-1, -1, 1, 1), (-1, 1, 8, 1), (1, -1, 1, 1), (1, 1, 8, 1),
     (0, -1, 1, 1), (0, 1, 8, 1)),
    ((-1, 0, 2, 4), (1, 0, 2, 4), (-1, 0, 6, 3), (1, 0, 6, 3), (-1, -1, 1, 1), (-1, 1, 8, 1), (1, -1, 1, 1), (1, 1, 8, 1),
     (0, -1, 1, 1), (0, 1, 8, 1), (-1, 0, 1, 1), (1, 0, 1, 1)),
)
DIRS = ((-1, 0), (1, 0), (-1, -1), (-1, 1), (1, -1), (1, 1), (0, -1), (0, 1))


def body(
    ny, nz, ns,
    vol, hist_h, w1, w2, w3, w4, gf_h, sf_h, gc_h, sc_h,
    skip, coarse, amax,
    hist, gf, sf, gc, sc, vin, w1v, w2v, w3v, w4v, wf1, wf2, wg3, wg4,
    x1, r1, x2r, x2, r2, h3, z3s, z3r, p3, c3, c3z, h4, z4s, z4r, r4i, c4, c4z, a2a, a2s,
    st, am, rows8,
    rounds, lsem, hs, hr, ss, sr, ws, wr, gs, bs, xs,
):
    n = ny * nz
    sy = lax.axis_index("sy")
    sz = lax.axis_index("sz")
    smp = lax.axis_index("sample")
    me = sz * ny + sy

    near = [{"sz": lax.rem(sz + d, nz)} for d in sorted({1, nz - 1})]
    near += [{"sy": lax.rem(sy + d, ny)} for d in range(1, ny)]
    if ns > 1:
        sx, sv = lax.rem(smp, 4), lax.div(smp, 4)
        near += [{"sample": sv * 4 + lax.rem(sx + d, 4)} for d in (1, 3)]
        near += [{"sample": lax.rem(sv + d, 4) * 4 + sx} for d in (1, 3)]
    barrier = pltpu.get_barrier_semaphore()
    for dev in near:
        pl.semaphore_signal(barrier, inc=1, device_id=dev, device_id_type=MESH)

    def greet(r):
        for dev in near:
            pl.semaphore_signal(rounds.at[r], inc=1, device_id=dev, device_id_type=MESH)

    def greeted(r):
        pl.semaphore_wait(rounds.at[r], len(near))

    place = {0: 0, 3: 1, 1: 2, 2: 3}
    loads = [pltpu.make_async_copy(vol.at[:, z], vin.at[place[z]], lsem.at[place[z] // 2]) for z in range(4)]
    small = ((hist_h, hist), (w1, w1v), (w2, w2v), (w3, w3v), (w4, w4v), (gf_h, gf), (sf_h, sf), (gc_h, gc), (sc_h, sc))
    for i, (s, d) in enumerate(small):
        loads.append(pltpu.make_async_copy(s, d, lsem.at[2 + i]))
    for i in (4, 0, 3, 1, 2, 5, 6, 7, 8, 9, 10, 11, 12):
        loads[i].start()

    def partner(d):
        p = lax.rem(me + d, n)
        return p, {"sy": lax.rem(p, ny), "sz": lax.div(p, ny)}

    order = sorted(range(1, n), key=lambda d: -min(d, n - d))
    def other_sample(d):
        q = lax.rem(smp + d, ns)
        return q, {"sample": q}

    def exists(dz, dy):
        cond = None
        for idx, cnt, d in ((sz, nz, dz), (sy, ny, dy)):
            if d == 0:
                continue
            c = (idx > 0) if d < 0 else (idx < cnt - 1)
            cond = c if cond is None else jnp.logical_and(cond, c)
        return cond

    lane = lax.broadcasted_iota(jnp.int32, (1, 128), 1)
    lower = lane < 64

    def bound_of(l):
        b = jnp.max(hist[l : l + 1, :], axis=1, keepdims=True)
        return b.astype(BF16).astype(F32)

    def src_z(dz, zl):
        return pl.ds(1, zl) if dz == 0 else (pl.ds(1, 1) if dz < 0 else pl.ds(zl, 1))

    def dst_z(dz, zl):
        return pl.ds(1, zl) if dz == 0 else (pl.ds(zl + 1, 1) if dz < 0 else pl.ds(0, 1))

    def halo(ph, buf, i):
        dz, dy, row, count = PIECES[ph][i]
        return pltpu.make_async_remote_copy(
            src_ref=buf.at[src_z(dz, 4), pl.ds(row, count)],
            dst_ref=buf.at[dst_z(dz, 4), pl.ds(row - 8 * dy, count)],
            send_sem=hs.at[i],
            recv_sem=hr.at[ph % 2, i],
            device_id={"sy": sy + dy, "sz": sz + dz},
            device_id_type=MESH,
        )

    def halo_send(ph, buf, which):
        for i in which:
            @pl.when(exists(*PIECES[ph][i][:2]))
            def _():
                halo(ph, buf, i).start()

    def halo_wait(ph, buf, which):
        for i in which:
            @pl.when(exists(-PIECES[ph][i][0], -PIECES[ph][i][1]))
            def _():
                halo(ph, buf, i).wait_recv()

    def halo_done(ph, buf, which):
        for i in which:
            @pl.when(exists(*PIECES[ph][i][:2]))
            def _():
                halo(ph, buf, i).wait_send()

    def halo_slots(ph, i):
        dz, dy, row, count = PIECES[ph][i]
        return slots(dz, 4), range(row - 8 * dy, row - 8 * dy + count)

    def coarse_halo(ph, own, zs, zr, i):
        dz, dy = DIRS[i]
        if dz == 0:
            src, dst = own.at[src_z(dy, 4)], own.at[dst_z(dy, 4)]
        else:
            up = 1 if dz > 0 else 0
            src, dst = zs.at[up, src_z(dy, 4)], zr.at[1 - up, dst_z(dy, 4)]
        return pltpu.make_async_remote_copy(
            src_ref=src, dst_ref=dst, send_sem=hs.at[i], recv_sem=hr.at[ph % 2, i],
            device_id={"sy": sy + dy, "sz": sz + dz}, device_id_type=MESH,
        )

    def coarse_send(ph, own, zs, zr):
        for i in range(8):
            @pl.when(exists(*DIRS[i]))
            def _():
                coarse_halo(ph, own, zs, zr, i).start()

    def coarse_done(ph, own, zs, zr):
        for i in range(8):
            @pl.when(exists(*DIRS[i]))
            def _():
                coarse_halo(ph, own, zs, zr, i).wait_send()

    def put_raw(blk, y, own, zs):
        half = blk.shape[0] // 2
        top, low = blk[:half], blk[half:]
        own[y] = blk.astype(BF16)
        zs[0, y] = jnp.where(lower, top, pltpu.roll(low, 64, 1)).astype(BF16)
        zs[1, y] = jnp.where(lower, pltpu.roll(top, 64, 1), low).astype(BF16)

    def coarse_settle(ph, own, zs, zr, buf, zbuf, aff, b):
        half = buf.shape[1] // 2
        paff = tuple(jnp.where(lower, t[:half], t[half:]) for t in aff)
        for i in range(8):
            dz, dy = DIRS[i]
            there = exists(-dz, -dy)
            ys = slots(dy, 4)

            @pl.when(there)
            def _():
                coarse_halo(ph, own, zs, zr, i).wait_recv()
                for y in ys:
                    if dz == 0:
                        buf[y] = settle(own[y].astype(F32), aff, b)
                    else:
                        k = 0 if dz > 0 else 1
                        zbuf[k, y] = settle(zr[k, y].astype(F32), paff, b)

            @pl.when(jnp.logical_not(there))
            def _():
                for y in ys:
                    if dz == 0:
                        buf[y] = jnp.zeros(buf.shape[1:], BF16)
                    else:
                        k = 0 if dz > 0 else 1
                        zbuf[k, y] = jnp.zeros(zbuf.shape[2:], BF16)

    def slots(d, length):
        return range(1, length + 1) if d == 0 else ((0,) if d > 0 else (length + 1,))

    def stat_copy(ph, src, dst, dev):
        return pltpu.make_async_remote_copy(
            src_ref=st.at[ph, src], dst_ref=st.at[ph, dst],
            send_sem=ss.at[0], recv_sem=sr.at[ph % 2],
            device_id=dev, device_id_type=MESH,
        )

    def stat_all(ph):
        rest = pl.ds(0, n - 1)
        return stat_copy(ph, rest, rest, partner(1)[1])

    def stat_send(ph, rows):
        if ph > 0:
            stat_all(ph - 1).wait_send()
        st[ph, me] = jnp.concatenate(rows + [rows[0]] * (4 - len(rows)), axis=0)
        for d in order:
            stat_copy(ph, me, me, partner(d)[1]).start()

    def stat_wait(ph):
        stat_all(ph).wait_recv()
        return st[ph]

    def to_rows(cols):
        return jnp.transpose(cols)

    def to_cols(row):
        return jnp.transpose(jnp.broadcast_to(row, (128, 128)))

    def affine(tot, totsq, cells, g, s):
        m = tot / cells
        var = totsq / cells - m * m
        a = lax.rsqrt(var + EPS) * g
        return a, m, s

    def act(v, aff):
        a, m, s = aff
        t = (v - m) * a + s
        return jnp.maximum(t, SLOPE * t)

    ri = lax.broadcasted_iota(jnp.int32, (256, 256), 0)
    ci = lax.broadcasted_iota(jnp.int32, (256, 256), 1)

    def onehot(cond):
        return jnp.where(cond, 1.0, 0.0).astype(BF16)

    into = onehot(jnp.logical_and((ri & 31) == (ci >> 3), (ri >> 5) == (ci & 7)))

    loads[4].wait()
    b0 = bound_of(0)
    peaks0 = []

    def take(zp):
        parts = []
        pair = pl.ds(place[zp[0]], 2)
        pltpu.make_async_copy(vin.at[pair], vin.at[pair], lsem.at[place[zp[0]] // 2]).wait()
        for z in zp:
            v = vin[place[z]].astype(F32).reshape(256, 128)
            peaks0.append(jnp.abs(v))
            parts.append(v.astype(BF16))
        moved = jnp.dot(into, jnp.concatenate(parts, axis=1), preferred_element_type=F32)
        moved = jnp.clip(moved, -b0, b0).astype(BF16)
        for k in range(2):
            for y in range(8):
                x1[1 + zp[k], 1 + y] = moved[32 * y : 32 * y + 32, 128 * k : 128 * k + 128]

    take((0, 3))
    pl.semaphore_wait(barrier, len(near))
    greet(0)
    halo_send(0, x1, (0, 1))
    take((1, 2))
    halo_send(0, x1, (8, 9, 2, 3))
    peak0 = jnp.maximum(jnp.maximum(peaks0[0], peaks0[1]), jnp.maximum(peaks0[2], peaks0[3]))
    peak0 = jnp.max(jnp.max(peak0, axis=0, keepdims=True), axis=1, keepdims=True)

    for i in range(5, 13):
        loads[i].wait()
    rows8[...] = jnp.zeros_like(rows8)
    rows8[0:2, 0:32] = gf[...]
    rows8[2:4, 0:32] = sf[...]
    rows8[4:6, 0:16] = gc[...]
    rows8[6:8, 0:16] = sc[...]
    gcols = jnp.transpose(rows8[...])

    def gain_col(j, count):
        return jnp.broadcast_to(gcols[0:count, j : j + 1], (count, 128))


    def lanes_of(w):
        return jnp.concatenate([w[k] for k in range(9)], axis=1)

    wf1[...] = lanes_of(w1v)
    wf2[...] = lanes_of(w2v)
    wg3[sy] = lanes_of(w3v)
    wg4[sy] = lanes_of(w4v)

    for i in range(len(PIECES[0])):
        @pl.when(jnp.logical_not(exists(-PIECES[0][i][0], -PIECES[0][i][1])))
        def _():
            for z in halo_slots(0, i)[0]:
                for y in halo_slots(0, i)[1]:
                    x1[z, y] = jnp.zeros((32, 128), BF16)

    mate = sy + 1 - 2 * lax.rem(sy, 2)
    cross_sy = lax.rem(sy + 2, 4)
    cross_mate = lax.rem(mate + 2, 4)

    def group(which, kind, src):
        buf = (wg3, wg4)[which]
        return pltpu.make_async_remote_copy(
            src_ref=buf.at[src], dst_ref=buf.at[src],
            send_sem=ws.at[which, kind], recv_sem=wr.at[which, kind],
            device_id={"sy": cross_sy if kind == 1 else mate}, device_id_type=MESH,
        )

    def group_send(which):
        group(which, 1, sy).start()
        group(which, 0, sy).start()

    def group_forward(which):
        group(which, 1, cross_sy).wait_recv()
        group(which, 2, cross_sy).start()

    def group_wait(which):
        group(which, 0, mate).wait_recv()
        group(which, 2, cross_mate).wait_recv()

    def group_done(which):
        group(which, 0, sy).wait_send()
        group(which, 1, sy).wait_send()
        group(which, 2, cross_sy).wait_send()

    fine_cells = float(4 * nz * 8 * ny * 128)
    coarse_cells = fine_cells / 8

    def fine_affine(cols, j):
        return affine(cols[0:32], cols[32:64], fine_cells, gain_col(j, 32), gain_col(2 + j, 32))

    def peak_of(high, low, aff):
        v = jnp.maximum(jnp.abs(act(high, aff)), jnp.abs(act(low, aff))).astype(BF16).astype(F32)
        return jnp.max(jnp.max(v, axis=0, keepdims=True), axis=1, keepdims=True)

    greeted(0)
    greet(1)
    halo_send(0, x1, (4, 5, 6, 7))

    first, last = lane == 0, lane == 127

    def combine(p0, p1, p2, lo, hi):
        left = jnp.where(lo, 0.0, pltpu.roll(p0, 1, 1))
        right = jnp.where(hi, 0.0, pltpu.roll(p2, 127, 1))
        return p1 + left + right

    def fine_conv(buf, w, z, rows=range(8)):
        strips = []
        for zt in range(3):
            for yt in range(3):
                strips.append(jnp.concatenate([buf[z + zt, y + yt] for y in rows], axis=1))
        got = jnp.dot(w, jnp.concatenate(strips, axis=0), preferred_element_type=F32)
        outs = []
        for k in range(len(rows)):
            blk = got[:, 128 * k : 128 * k + 128]
            outs.append(combine(blk[0:32], blk[32:64], blk[64:96], first, last))
        return outs

    zero = jnp.zeros((32, 128), F32)

    def gather_stats(acc, blocks, extremes):
        s, q, hi, lo = acc
        for b in blocks:
            s = s + b
            q = q + b * b
            if extremes:
                hi = jnp.maximum(hi, b)
                lo = jnp.minimum(lo, b)
        return s, q, hi, lo

    def sum_row(cols):
        cols = jnp.concatenate(cols, axis=0)
        if cols.shape[0] < 128:
            cols = jnp.concatenate([cols, cols], axis=0)
        return jnp.sum(to_rows(cols), axis=0, keepdims=True)

    def mixed_row(cols):
        t = to_rows(cols)
        total = jnp.sum(t, axis=0, keepdims=True)
        high = jnp.max(t, axis=0, keepdims=True)
        low = jnp.min(t, axis=0, keepdims=True)
        return jnp.where(lane < 64, total, jnp.where(lane < 96, high, low))

    def mixed_total(got):
        total = jnp.sum(got[:, 0:1, :], axis=0)
        high = jnp.max(got[:, 0:1, :], axis=0)
        low = jnp.min(got[:, 0:1, :], axis=0)
        return to_cols(jnp.where(lane < 64, total, jnp.where(lane < 96, high, low)))

    wa = wf1[...]
    acc = (zero, zero, jnp.full((32, 128), -jnp.inf, F32), jnp.full((32, 128), jnp.inf, F32))
    def first_rows(z, rows, acc):
        outs = fine_conv(x1, wa, z, rows)
        for k, y in enumerate(rows):
            r1[z, y] = outs[k]
            if z in (0, 3) or y in (0, 7):
                x2r[z + 1, y + 1] = outs[k].astype(BF16)
        return gather_stats(acc, outs, True)

    halo_wait(0, x1, (0, 1))
    for z in (0, 3):
        acc = first_rows(z, (1, 2, 3, 4), acc)
    halo_done(0, x1, (0, 1))
    halo_send(1, x2r, (0, 1))
    halo_wait(0, x1, (8, 9))
    for z in (1, 2):
        acc = first_rows(z, range(8), acc)
    halo_wait(0, x1, range(2, 8))
    greeted(1)
    for z in (0, 3):
        acc = first_rows(z, (0, 5, 6, 7), acc)
    row = mixed_row(jnp.concatenate(acc, axis=0))
    stat_send(0, [row, jnp.broadcast_to(peak0, (1, 128)), rows8[4:5], rows8[6:7]])
    halo_done(0, x1, range(2, 10))
    halo_send(1, x2r, (2, 3, 10, 11, 4, 5, 6, 7, 8, 9))
    group_send(0)
    greet(2)

    got = stat_wait(0)
    group_send(1)
    peak0 = jnp.max(jnp.max(got[:, 1:2, :], axis=0), axis=1, keepdims=True)
    cols = mixed_total(got)
    aff = fine_affine(cols, 0)
    peak1 = peak_of(cols[64:96], cols[96:128], aff)
    b1 = bound_of(1)

    def settle(v, aff, b):
        return jnp.clip(act(v, aff), -b, b).astype(BF16)


    def settle_halo(ph, raw, buf, which, aff, b):
        for i in which:
            dz, dy = PIECES[ph][i][:2]
            there = exists(-dz, -dy)
            zs, ys = halo_slots(ph, i)

            @pl.when(there)
            def _():
                halo(ph, raw, i).wait_recv()
                for z in zs:
                    for y in ys:
                        buf[z, y] = settle(raw[z, y].astype(F32), aff, b)

            @pl.when(jnp.logical_not(there))
            def _():
                for z in zs:
                    for y in ys:
                        buf[z, y] = jnp.zeros(buf.shape[2:], buf.dtype)

    wb = wf2[...]
    acc = (zero, zero, None, None)
    settle_halo(1, x2r, x2, (8, 9), aff, b1)
    for z in range(4):
        for y in range(8):
            x2[z + 1, y + 1] = settle(r1[z, y], aff, b1)
    for z in (1, 2):
        outs = fine_conv(x2, wb, z)
        acc = gather_stats(acc, outs, False)
        for y in range(8):
            r2[z, y] = outs[y]
    settle_halo(1, x2r, x2, (0, 1, 4, 5, 6, 7, 2, 3, 10, 11), aff, b1)

    for z in (0, 3):
        outs = fine_conv(x2, wb, z)
        acc = gather_stats(acc, outs, False)
        for y in range(8):
            r2[z, y] = outs[y]

    stat_send(1, [sum_row(acc[0:2])])
    s_r = lax.broadcasted_iota(jnp.int32, (256, 128), 0)
    s_c = lax.broadcasted_iota(jnp.int32, (256, 128), 1)
    pick = onehot(s_r == jnp.where(s_c < 64, 2 * s_c, 2 * s_c))
    highs, lows = [], []
    for zp in range(2):
        hrow, lrow = [], []
        for yp in range(4):
            m = jnp.maximum(
                jnp.maximum(r2[2 * zp, 2 * yp], r2[2 * zp, 2 * yp + 1]),
                jnp.maximum(r2[2 * zp + 1, 2 * yp], r2[2 * zp + 1, 2 * yp + 1]),
            )
            m = jnp.maximum(m, pltpu.roll(m, 127, 1))
            h = m.astype(BF16)
            hrow.append(h)
            lrow.append((m - h.astype(F32)).astype(BF16))
        highs.append(jnp.concatenate(hrow, axis=0))
        lows.append(jnp.concatenate(lrow, axis=0))
    pooled = jnp.dot(jnp.concatenate(highs, axis=1), pick, preferred_element_type=F32)
    pooled = pooled + jnp.dot(jnp.concatenate(lows, axis=1), pick, preferred_element_type=F32)
    hi = jnp.full((32, 128), -jnp.inf, F32)
    lo = jnp.full((32, 128), jnp.inf, F32)
    for yp in range(4):
        blk = pooled[32 * yp : 32 * yp + 32]
        p3[yp] = blk
        put_raw(blk, yp + 1, h3, z3s)
        hi = jnp.maximum(hi, blk)
        lo = jnp.minimum(lo, blk)
    halo_done(1, x2r, range(12))
    coarse_send(2, h3, z3s, z3r)
    group_forward(0)
    group_forward(1)

    got = stat_wait(1)
    cols = to_cols(jnp.sum(got[:, 0:1, :], axis=0))
    aff2 = fine_affine(cols, 1)
    b2 = bound_of(2)
    coarse_settle(2, h3, z3s, z3r, c3, c3z, aff2, b2)

    cfirst, clast = (lane & 63) == 0, (lane & 63) == 63

    def coarse_conv(buf, zbuf, w):
        strips = []
        mids = [buf[y] for y in range(6)]
        pairs = [[], mids, []]
        half = buf.shape[1] // 2
        for y in range(6):
            own = pltpu.roll(mids[y].astype(F32), 64, 1)
            prev = zbuf[0, y].astype(F32)
            nxt = zbuf[1, y].astype(F32)
            a = jnp.where(lower, prev, own[:half])
            b = jnp.where(lower, pltpu.roll(prev, 64, 1), own[half:])
            pairs[0].append(jnp.concatenate([a, b], axis=0).astype(BF16))
            a = jnp.where(lower, own[:half], pltpu.roll(nxt, 64, 1))
            b = jnp.where(lower, own[half:], nxt)
            pairs[2].append(jnp.concatenate([a, b], axis=0).astype(BF16))
        for zt in range(3):
            for yt in range(3):
                strips.append(jnp.concatenate(pairs[zt][yt : yt + 4], axis=1))
        got = jnp.dot(w, jnp.concatenate(strips, axis=0), preferred_element_type=F32)
        outs = []
        for y in range(4):
            blk = got[:, 128 * y : 128 * y + 128]
            parts = []
            for g in range(4):
                t = blk[48 * g : 48 * g + 48]
                parts.append(combine(t[0:16], t[16:32], t[32:48], cfirst, clast))
            outs.append(jnp.concatenate(parts, axis=0))
        return outs

    group_wait(0)
    for yp in range(4):
        c3[yp + 1] = settle(p3[yp], aff2, b2)
    outs = coarse_conv(c3, c3z, wg3[...].reshape(192, 288))
    zero64 = jnp.zeros((64, 128), F32)
    acc = (zero64, zero64, jnp.full((64, 128), -jnp.inf, F32), jnp.full((64, 128), jnp.inf, F32))
    acc = gather_stats(acc, outs, True)

    def extreme_row(cols, split):
        t = to_rows(jnp.concatenate(cols, axis=0))
        return jnp.where(split, jnp.max(t, axis=0, keepdims=True), jnp.min(t, axis=0, keepdims=True))

    stat_send(2, [sum_row(acc[0:2]), extreme_row(acc[2:4], lower), extreme_row((hi, hi, lo, lo), lower)])
    for y in range(4):
        put_raw(outs[y], y + 1, h4, z4s)
        r4i[y] = outs[y]
    coarse_done(2, h3, z3s, z3r)
    coarse_send(3, h4, z4s, z4r)

    outof = onehot(jnp.logical_and((ci & 31) == (ri >> 3), (ci >> 5) == (ri & 7)))
    for zp in range(2):
        parts = []
        for z in (2 * zp, 2 * zp + 1):
            parts.append(jnp.concatenate([act(r2[z, y], aff2).astype(BF16) for y in range(8)], axis=0))
        moved = jnp.dot(outof, jnp.concatenate(parts, axis=1), preferred_element_type=F32)
        for k in range(2):
            z = 2 * zp + k
            skip[z] = moved[:, 128 * k : 128 * k + 128].reshape(32, 8, 128).astype(BF16)

    gall = jnp.transpose(jnp.concatenate([st[0, sz * ny + g, 2:4] for g in range(ny)], axis=0))

    def gathered(k):
        parts = [gall[0:16, 2 * g + k : 2 * g + k + 1] for g in range(ny)]
        return jnp.broadcast_to(jnp.concatenate(parts, axis=0), (64, 128))

    got = stat_wait(2)
    cols = to_cols(jnp.sum(got[:, 0:1, :], axis=0))
    aff3 = affine(cols[0:64], cols[64:128], coarse_cells, gathered(0), gathered(1))
    b3 = bound_of(3)

    def cross(src, dst, dev):
        return pltpu.make_async_remote_copy(
            src_ref=am.at[src], dst_ref=am.at[dst], send_sem=xs.at[0], recv_sem=xs.at[1],
            device_id=dev, device_id_type=MESH,
        )

    def cross_all():
        return cross(pl.ds(0, ns - 1), pl.ds(0, ns - 1), other_sample(1)[1])

    coarse_settle(3, h4, z4s, z4r, c4, c4z, aff3, b3)
    group_wait(1)
    for y in range(4):
        c4[y + 1] = settle(r4i[y], aff3, b3)

    high = jnp.max(got[:, 1:3, :], axis=0)
    low = jnp.min(got[:, 1:3, :], axis=0)
    ext = jnp.where(lower, high, low)
    pext, ext = to_cols(ext[1:2]), to_cols(ext[0:1])
    peak2 = peak_of(pext[0:32], pext[64:96], aff2)
    peak3 = peak_of(ext[0:64], ext[64:128], aff3)
    peaks = jnp.where(lane == 0, peak0, jnp.where(lane == 1, peak1, jnp.where(lane == 2, peak2, peak3)))

    greeted(2)
    am[smp] = peaks
    for d in range(1, ns):
        cross(smp, smp, other_sample(d)[1]).start()


    outs = coarse_conv(c4, c4z, wg4[...].reshape(192, 576))
    acc = gather_stats((zero64, zero64, None, None), outs, False)
    def swap(src, dst, q):
        return pltpu.make_async_remote_copy(
            src_ref=a2s.at[src], dst_ref=a2a.at[dst], send_sem=bs.at[0], recv_sem=bs.at[1],
            device_id={"sy": q}, device_id_type=MESH,
        )

    stat_send(3, [sum_row(acc[0:2])])
    for g in range(4):
        for y in range(4):
            a2s[g, y] = outs[y][16 * g : 16 * g + 16].astype(BF16)

    for d in range(1, ny):
        q = lax.rem(sy + d, ny)
        swap(q, sy, q).start()
    swap_all = swap(pl.ds(0, ny - 1), pl.ds(0, ny - 1), mate)
    a2a[sy] = a2s[sy]

    coarse_done(3, h4, z4s, z4r)
    for which in range(2):
        group_done(which)
    swap_all.wait_recv()
    got = stat_wait(3)
    rows8b = to_cols(jnp.sum(got[:, 0:1, :], axis=0))
    gs[...] = rows8b
    tot = gs[pl.ds(pl.multiple_of(sy * 16, 8), 16), :]
    totsq = gs[pl.ds(pl.multiple_of(64 + sy * 16, 8), 16), :]
    aff4 = affine(tot, totsq, coarse_cells, gain_col(5, 16), gain_col(7, 16))
    planes = [[], []]
    for g in range(4):
        for yp in range(2):
            u = act(a2a[g, 2 * yp].astype(F32), aff4)
            v = act(a2a[g, 2 * yp + 1].astype(F32), aff4)
            planes[0].append(jnp.where(lower, u, pltpu.roll(v, 64, 1)))
            planes[1].append(jnp.where(lower, pltpu.roll(u, 64, 1), v))
    both = [jnp.concatenate(planes[z], axis=1) for z in range(2)]
    coarse[...] = jnp.stack(both, axis=1).astype(BF16)

    if ns > 1:
        cross_all().wait_recv()
    amax[...] = jnp.max(am[...], axis=0)[:, 0:4]

    stat_all(3).wait_send()
    swap_all.wait_send()
    if ns > 1:
        cross_all().wait_send()


def solution(mesh):
    ny, nz, ns = mesh.shape["sy"], mesh.shape["sz"], mesh.shape["sample"]
    n = ny * nz
    vmem = pl.BlockSpec(memory_space=pltpu.VMEM)
    hbm = pl.BlockSpec(memory_space=pl.ANY)

    def step(volume, hist, w1, w2, w3, w4, gf, sf, gc, sc):
        dma = pltpu.SemaphoreType.DMA
        skip, coarse, amax = pl.pallas_call(
            functools.partial(body_entry, ny, nz, ns),
            out_shape=(
                pltpu.VMEM((4, 32, 8, 128), BF16),
                pltpu.VMEM((16, 2, 1024), BF16),
                pltpu.VMEM((1, 4), F32),
            ),
            in_specs=[hbm] * 10,
            out_specs=(vmem, vmem, vmem),
            scratch_shapes=[
                pltpu.VMEM((4, 16), F32),
                pltpu.VMEM((2, 32), F32),
                pltpu.VMEM((2, 32), F32),
                pltpu.VMEM((2, 16), F32),
                pltpu.VMEM((2, 16), F32),
                pltpu.VMEM((4, 32, 8, 128), BF16),
                pltpu.VMEM((9, 96, 32), BF16),
                pltpu.VMEM((9, 96, 32), BF16),
                pltpu.VMEM((9, 48, 32), BF16),
                pltpu.VMEM((9, 48, 64), BF16),
                pltpu.VMEM((96, 288), BF16),
                pltpu.VMEM((96, 288), BF16),
                pltpu.VMEM((ny, 48, 288), BF16),
                pltpu.VMEM((ny, 48, 576), BF16),
                pltpu.VMEM((6, 10, 32, 128), BF16),
                pltpu.VMEM((4, 8, 32, 128), F32),
                pltpu.VMEM((6, 10, 32, 128), BF16),
                pltpu.VMEM((6, 10, 32, 128), BF16),
                pltpu.VMEM((4, 8, 32, 128), F32),
                pltpu.VMEM((6, 32, 128), BF16),
                pltpu.VMEM((2, 6, 16, 128), BF16),
                pltpu.VMEM((2, 6, 16, 128), BF16),
                pltpu.VMEM((4, 32, 128), F32),
                pltpu.VMEM((6, 32, 128), BF16),
                pltpu.VMEM((2, 6, 16, 128), BF16),
                pltpu.VMEM((6, 64, 128), BF16),
                pltpu.VMEM((2, 6, 32, 128), BF16),
                pltpu.VMEM((2, 6, 32, 128), BF16),
                pltpu.VMEM((4, 64, 128), F32),
                pltpu.VMEM((6, 64, 128), BF16),
                pltpu.VMEM((2, 6, 32, 128), BF16),
                pltpu.VMEM((ny, 4, 16, 128), BF16),
                pltpu.VMEM((ny, 4, 16, 128), BF16),
                pltpu.VMEM((4, n, 4, 128), F32),
                pltpu.VMEM((ns, 1, 128), F32),
                pltpu.VMEM((8, 128), F32),
                pltpu.VMEM((128, 128), F32),
                pltpu.SemaphoreType.REGULAR((3,)),
                dma((11,)),
                dma((12,)),
                dma((2, 12)),
                dma((1,)),
                dma((2,)),
                dma((2, 3)),
                dma((2, 3)),
                dma((2,)),
                dma((2,)),
            ],
            compiler_params=pltpu.CompilerParams(collective_id=0, has_side_effects=True),
            name="encoder",
        )(
            volume.reshape(32, 4, 8, 128), hist, w1.reshape(9, 96, 32), w2.reshape(9, 96, 32),
            w3.reshape(9, 48, 32), w4.reshape(9, 48, 64), gf, sf, gc, sc,
        )
        skip, coarse, amax = pl.pallas_call(
            emit,
            out_shape=(
                jax.ShapeDtypeStruct((32, 4, 8, 128), BF16),
                jax.ShapeDtypeStruct((16, 2, 1024), BF16),
                jax.ShapeDtypeStruct((1, 4), F32),
            ),
            in_specs=[vmem] * 3,
            out_specs=(hbm, hbm, hbm),
            scratch_shapes=[dma((6,))],
            name="emit",
        )(*(pltpu.with_memory_space_constraint(t, pltpu.VMEM) for t in (skip, coarse, amax)))
        return skip.reshape(1, 32, 4, 8, 128), coarse.reshape(1, 16, 2, 1024), amax.reshape(4)

    return jax.shard_map(
        step,
        mesh=mesh,
        in_specs=(
            P("sample", None, "sz", "sy", None), P(), P(), P(),
            P(None, "sy", None), P(None, "sy", None), P(), P(), P(None, "sy"), P(None, "sy"),
        ),
        out_specs=(P("sample", None, "sz", "sy", None), P("sample", "sy", "sz", None), P()),
        check_vma=False,
    )


def body_entry(ny, nz, ns, *refs):
    (
        vol, hist, w1, w2, w3, w4, gf, sf, gc, sc, skip, coarse, amax,
        hist_v, gf_v, sf_v, gc_v, sc_v, vin, w1v, w2v, w3v, w4v, wf1, wf2, wg3, wg4,
        x1, r1, x2r, x2, r2, h3, z3s, z3r, p3, c3, c3z, h4, z4s, z4r, r4i, c4, c4z, a2a, a2s,
        st, am, rows8, tcols,
        rounds, lsem, hs, hr, ss, sr, ws, wr, bs, xs,
    ) = refs
    body(
        ny, nz, ns,
        vol, hist, w1, w2, w3, w4, gf, sf, gc, sc, skip, coarse, amax,
        hist_v, gf_v, sf_v, gc_v, sc_v, vin, w1v, w2v, w3v, w4v, wf1, wf2, wg3, wg4,
        x1, r1, x2r, x2, r2, h3, z3s, z3r, p3, c3, c3z, h4, z4s, z4r, r4i, c4, c4z, a2a, a2s,
        st, am, rows8,
        rounds, lsem, hs, hr, ss, sr, ws, wr, tcols, bs, xs,
    )


def emit(skip_v, coarse_v, amax_v, skip, coarse, amax, sem):
    copies = [pltpu.make_async_copy(skip_v.at[z], skip.at[:, z], sem.at[z]) for z in range(4)]
    copies.append(pltpu.make_async_copy(coarse_v, coarse, sem.at[4]))
    copies.append(pltpu.make_async_copy(amax_v, amax, sem.at[5]))
    for c in copies:
        c.start()
    for c in copies:
        c.wait()
```
